32 devices in a mesh: data: 1 (over z), model: 32 (over y, x, core).
Axes of the slice: x: 4, y: 4, z: 1, core: 2. Of those that a mesh axis runs over, the one named last changes fastest.
The devices are a block of a 4x4x8 slice.
Arguments:
- x_in: bfloat16 [32, 256, 2048], P('data')
- seg_ids: int32 [32, 256], P('data')
- ln_gain: bfloat16 [2048], replicated
- w_qkv: bfloat16 [2048, 32, 3, 64], P(None, 'model')
- w_out: bfloat16 [32, 64, 2048], P('model')
- w_up: bfloat16 [2048, 8192], P(None, 'model')
- w_down: bfloat16 [8192, 2048], P('model')
- dy_in: bfloat16 [32, 256, 2048], P('data')
Outputs:
- output 1: bfloat16 [32, 256, 2048], P('data')
- output 2: bfloat16 [32, 256, 2048], P('data')
- output 3: bfloat16 [2048], P('data')
- output 4: bfloat16 [2048, 32, 3, 64], P('data', 'model')
- output 5: bfloat16 [32, 64, 2048], P(('data', 'model'))
- output 6: bfloat16 [2048, 8192], P('data', 'model')
- output 7: bfloat16 [8192, 2048], P(('data', 'model'))
All inputs are finite; a program needn't handle non-finite values.
Results may differ from the reference program's by a relative error of at most 0.0183751.
Values are sent between devices in bfloat16 or wider.
A program may use at most 768 MiB of HBM per device.

```python
import jax
import jax.numpy as jnp
from jax import lax

GROUP_ROWS = 32
SEQ_LEN = 256
HIDDEN = 2048
NUM_HEADS = 32
HEAD_DIM = 64
FFN_DIM = 8192
LN_EPS = 1e-5


def setup_inputs(seed: int = 0, part: int = 0) -> dict:
    part_key = jax.random.fold_in(jax.random.key(seed), part)
    key_x, key_seg, key_dy = jax.random.split(part_key, 3)
    key_gain, key_qkv, key_out, key_up, key_down = jax.random.split(jax.random.key(seed + 1), 5)
    attn_width = NUM_HEADS * HEAD_DIM
    cuts = jax.random.randint(key_seg, (GROUP_ROWS, 3), 1, SEQ_LEN)
    positions = jnp.arange(SEQ_LEN)
    seg_ids = jnp.sum(positions[None, :, None] >= cuts[:, None, :], axis=-1).astype(jnp.int32)
    x_in = jax.random.normal(key_x, (GROUP_ROWS, SEQ_LEN, HIDDEN), jnp.float32)
    ln_gain = 1.0 + 0.3 * jax.random.normal(key_gain, (HIDDEN,), jnp.float32)
    w_qkv = jax.random.normal(key_qkv, (HIDDEN, NUM_HEADS, 3, HEAD_DIM), jnp.float32) * HIDDEN ** -0.5
    w_out = jax.random.normal(key_out, (NUM_HEADS, HEAD_DIM, HIDDEN), jnp.float32) * (3.0 * attn_width ** -0.5)
    w_up = jax.random.normal(key_up, (HIDDEN, FFN_DIM), jnp.float32) * HIDDEN ** -0.5
    w_down = jax.random.normal(key_down, (FFN_DIM, HIDDEN), jnp.float32) * FFN_DIM ** -0.5
    dy_in = jax.random.normal(key_dy, (GROUP_ROWS, SEQ_LEN, HIDDEN), jnp.float32)
    return {
        'x_in': x_in.astype(jnp.bfloat16),
        'seg_ids': seg_ids,
        'ln_gain': ln_gain.astype(jnp.bfloat16),
        'w_qkv': w_qkv.astype(jnp.bfloat16),
        'w_out': w_out.astype(jnp.bfloat16),
        'w_up': w_up.astype(jnp.bfloat16),
        'w_down': w_down.astype(jnp.bfloat16),
        'dy_in': dy_in.astype(jnp.bfloat16),
    }


def layer_norm(x_f32, ln_gain):
    mean_val = jnp.mean(x_f32, axis=-1, keepdims=True)
    centered = x_f32 - mean_val
    var_val = jnp.mean(centered * centered, axis=-1, keepdims=True)
    normed = centered * lax.rsqrt(var_val + LN_EPS)
    return (normed * ln_gain.astype(jnp.float32)).astype(jnp.bfloat16)


def head_attention(head_args):
    qkv_head, seg_row = head_args
    query = qkv_head[0]
    keys = qkv_head[1]
    values = qkv_head[2]
    scores = jnp.dot(query, keys.T, preferred_element_type=jnp.float32) * (HEAD_DIM ** -0.5)
    positions = jnp.arange(SEQ_LEN)
    allowed = (positions[None, :] <= positions[:, None]) & (seg_row[None, :] == seg_row[:, None])
    attn_probs = jax.nn.softmax(jnp.where(allowed, scores, -1e30), axis=-1).astype(jnp.bfloat16)
    return jnp.dot(attn_probs, values, preferred_element_type=jnp.float32).astype(jnp.bfloat16)


def layer_forward(x_in, ln_gain, w_qkv, w_out, w_up, w_down, seg_ids):
    rows = x_in.shape[0]
    x_f32 = x_in.astype(jnp.float32)
    normed = layer_norm(x_f32, ln_gain)
    flat = normed.reshape(rows * SEQ_LEN, HIDDEN)
    qkv_proj = jnp.dot(flat, w_qkv.reshape(HIDDEN, NUM_HEADS * 3 * HEAD_DIM), preferred_element_type=jnp.float32).astype(jnp.bfloat16)
    qkv_heads = qkv_proj.reshape(rows, SEQ_LEN, NUM_HEADS, 3, HEAD_DIM).transpose(0, 2, 3, 1, 4).reshape(rows * NUM_HEADS, 3, SEQ_LEN, HEAD_DIM)
    seg_rep = jnp.repeat(seg_ids, NUM_HEADS, axis=0)
    attn_out = lax.map(jax.checkpoint(head_attention), (qkv_heads, seg_rep))
    attn_flat = attn_out.reshape(rows, NUM_HEADS, SEQ_LEN, HEAD_DIM).transpose(0, 2, 1, 3).reshape(rows * SEQ_LEN, NUM_HEADS * HEAD_DIM)
    up_proj = jnp.dot(flat, w_up, preferred_element_type=jnp.float32).astype(jnp.bfloat16)
    hidden_act = jax.nn.gelu(up_proj.astype(jnp.float32), approximate=False).astype(jnp.bfloat16)
    share_sum = jnp.dot(attn_flat, w_out.reshape(NUM_HEADS * HEAD_DIM, HIDDEN), preferred_element_type=jnp.float32) + jnp.dot(hidden_act, w_down, preferred_element_type=jnp.float32)
    mixed = share_sum.astype(jnp.bfloat16).reshape(rows, SEQ_LEN, HIDDEN)
    return (x_f32 + mixed.astype(jnp.float32)).astype(jnp.bfloat16)


def reference(x_in, seg_ids, ln_gain, w_qkv, w_out, w_up, w_down, dy_in):
    def forward_fn(x_val, gain_val, qkv_val, out_val, up_val, down_val):
        return layer_forward(x_val, gain_val, qkv_val, out_val, up_val, down_val, seg_ids)
    y_out, vjp_fn = jax.vjp(forward_fn, x_in, ln_gain, w_qkv, w_out, w_up, w_down)
    dx_out, d_gain, d_wqkv, d_wout, d_wup, d_wdown = vjp_fn(dy_in)
    return (y_out, dx_out, d_gain, d_wqkv, d_wout, d_wup, d_wdown)
```

```python
import functools

import jax
import jax.numpy as jnp
from jax import lax
from jax.experimental import pallas as pl
from jax.experimental.pallas import tpu as pltpu
from jax.sharding import PartitionSpec as P

LN_EPS = 1e-5
PAIR = 2
NT = (((1,), (1,)), ((), ()))
NN = (((1,), (0,)), ((), ()))
TN = (((0,), (0,)), ((), ()))


def dot(lhs, rhs, dims):
    return lax.dot_general(lhs, rhs, dims, preferred_element_type=jnp.float32)


def norm_rows(x_f32):
    mean_val = jnp.mean(x_f32, axis=-1, keepdims=True)
    centered = x_f32 - mean_val
    inv_std = lax.rsqrt(jnp.mean(centered * centered, axis=-1, keepdims=True) + LN_EPS)
    return centered * inv_std, inv_std


def rows_kernel(first, x_ref, dy_ref, seg_ref, gain_ref, wqkv_ref, wo_ref, w1_ref, w2_ref, *refs):
    if first:
        md_ref, acc_in, acc_out, a_scr = refs
    else:
        prev_in, prev_out, md_ref, acc_in, acc_out, a_scr = refs
    seqs, seq_len, hidden = x_ref.shape
    head_dim = wo_ref.shape[0]
    tokens = seqs * seq_len

    @pl.when(pl.program_id(0) == 0)
    def _():
        if first:
            acc_in[...] = jnp.zeros_like(acc_in)
            acc_out[...] = jnp.zeros_like(acc_out)
        else:
            acc_in[...] = prev_in[...]
            acc_out[...] = prev_out[...]

    gain = gain_ref[...].astype(jnp.float32)
    sub = 64
    for t in range(0, tokens, sub):
        s, o = t // seq_len, t % seq_len
        normed, _ = norm_rows(x_ref[s, o:o + sub, :].astype(jnp.float32))
        a_scr[t:t + sub, :] = (normed * gain).astype(jnp.bfloat16)

    a_all = a_scr[...]
    dy_all = dy_ref[...].reshape(tokens, hidden)
    qkv = dot(a_all, wqkv_ref[...], NT).astype(jnp.bfloat16)
    up = dot(a_all, w1_ref[...], NN).astype(jnp.bfloat16).astype(jnp.float32)
    d_attn = dot(dy_all, wo_ref[...], NT).astype(jnp.bfloat16)
    d_hid = dot(dy_all, w2_ref[...], NT).astype(jnp.bfloat16).astype(jnp.float32)
    cdf = 0.5 * (1.0 + lax.erf(up * (0.5 ** 0.5)))
    hid = (up * cdf).astype(jnp.bfloat16)
    slope = cdf + up * (jnp.exp(-0.5 * up * up) * 0.3989422804014327)
    d_up = (d_hid * slope).astype(jnp.bfloat16)

    scale = head_dim ** -0.5
    rows_id = lax.broadcasted_iota(jnp.int32, (seq_len, seq_len), 0)
    cols_id = lax.broadcasted_iota(jnp.int32, (seq_len, seq_len), 1)
    causal = cols_id <= rows_id
    outs, d_qkvs = [], []
    for s in range(seqs):
        lo, hi = s * seq_len, (s + 1) * seq_len
        query = qkv[lo:hi, :head_dim]
        keys = qkv[lo:hi, head_dim:2 * head_dim]
        values = qkv[lo:hi, 2 * head_dim:]
        d_o = d_attn[lo:hi]
        seg_cols = jnp.broadcast_to(seg_ref[s], (seq_len, seq_len))
        allowed = causal & (seg_cols == seg_cols.T)
        scores = jnp.where(allowed, dot(query, keys, NT) * scale, -1e30)
        expd = jnp.exp(scores - jnp.max(scores, axis=-1, keepdims=True))
        probs = expd / jnp.sum(expd, axis=-1, keepdims=True)
        probs_b = probs.astype(jnp.bfloat16)
        outs.append(dot(probs_b, values, NN).astype(jnp.bfloat16))
        d_p = dot(d_o, values, NT)
        d_s = (probs * (d_p - jnp.sum(d_p * probs, axis=-1, keepdims=True)) * scale).astype(jnp.bfloat16)
        d_q = dot(d_s, keys, NN).astype(jnp.bfloat16)
        d_k = dot(d_s, query, TN).astype(jnp.bfloat16)
        d_v = dot(probs_b, d_o, TN).astype(jnp.bfloat16)
        d_qkvs.append(jnp.concatenate([d_q, d_k, d_v], axis=-1))
    attn = jnp.concatenate(outs, axis=0)
    d_qkv = jnp.concatenate(d_qkvs, axis=0)

    devs, _, per, _ = md_ref.shape
    width_qkv = d_qkv.shape[1]
    step = 512
    for h in range(0, hidden, step):
        cols = slice(h, h + step)
        share = dot(attn, wo_ref[:, cols], NN) + dot(hid, w2_ref[:, cols], NN)
        md_ref[:, 0, :, cols] = share.astype(jnp.bfloat16).reshape(devs, per, step)
        d_share = dot(d_qkv, wqkv_ref[:, cols], NN) + dot(d_up, w1_ref[cols, :], NT)
        md_ref[:, 1, :, cols] = d_share.astype(jnp.bfloat16).reshape(devs, per, step)
        a_cols = a_scr[:, cols]
        dy_cols = dy_ref[:, :, cols].reshape(tokens, step)
        acc_in[:width_qkv, cols] += dot(d_qkv, a_cols, TN)
        acc_in[width_qkv:, cols] += dot(d_up, a_cols, TN)
        acc_out[:head_dim, cols] += dot(attn, dy_cols, TN)
        acc_out[head_dim:, cols] += dot(hid, dy_cols, TN)


def rows_call(start, count, devices, x_in, dy_in, seg, gain, wqkv, wo, w1, w2, prev):
    _, seq_len, hidden = x_in.shape
    per = count * seq_len // devices
    tokens = PAIR * seq_len
    base = start // PAIR
    width_in = wqkv.shape[0] + w1.shape[1]
    width_out = wo.shape[0] + w2.shape[0]
    row_spec = pl.BlockSpec((PAIR, seq_len, hidden), lambda i: (base + i, 0, 0))
    whole = lambda shape: pl.BlockSpec(shape, lambda i: (0,) * len(shape), pipeline_mode=pl.Buffered(1))
    acc_specs = [whole((width_in, hidden)), whole((width_out, hidden))]
    acc_shapes = [jax.ShapeDtypeStruct((width_in, hidden), jnp.float32), jax.ShapeDtypeStruct((width_out, hidden), jnp.float32)]
    args = [x_in, dy_in, seg, gain, wqkv, wo, w1, w2]
    in_specs = [row_spec, row_spec, pl.BlockSpec((PAIR, 1, seq_len), lambda i: (base + i, 0, 0)),
                whole(gain.shape), whole(wqkv.shape), whole(wo.shape), whole(w1.shape), whole(w2.shape)]
    aliases = {}
    if prev is not None:
        args += list(prev)
        in_specs += acc_specs
        aliases = {8: 1, 9: 2}
    flops = 2 * count * seq_len * hidden * (width_in * 3 + width_out * 3)
    return pl.pallas_call(
        functools.partial(rows_kernel, prev is None),
        grid=(count // PAIR,),
        in_specs=in_specs,
        out_specs=[pl.BlockSpec((tokens // per, 2, per, hidden), lambda i: (i, 0, 0, 0))] + acc_specs,
        out_shape=[jax.ShapeDtypeStruct((devices, 2, per, hidden), jnp.bfloat16)] + acc_shapes,
        input_output_aliases=aliases,
        scratch_shapes=[pltpu.VMEM((tokens, hidden), jnp.bfloat16)],
        cost_estimate=pl.CostEstimate(flops=flops, bytes_accessed=count * seq_len * hidden * 8, transcendentals=0),
        compiler_params=pltpu.CompilerParams(vmem_limit_bytes=60 * 2 ** 20),
        name=f"rows_{start}",
    )(*args)


def place_kernel(y_part, dx_part, *refs):
    y_out, dx_out = refs[-2:]
    y_out[...] = y_part[...].reshape(y_out.shape)
    dx_out[...] = dx_part[...].reshape(dx_out.shape)


def place_call(start, count, gathered, shape, dtype, prev):
    rows, seq_len, hidden = shape
    _, _, per, _ = gathered.shape
    spread = seq_len // per
    out_spec = pl.BlockSpec((1, seq_len, hidden), lambda i: (start + i, 0, 0))
    args = [gathered, gathered]
    in_specs = [pl.BlockSpec((spread, 1, per, hidden), lambda i: (i, 0, 0, 0)), pl.BlockSpec((spread, 1, per, hidden), lambda i: (i, 1, 0, 0))]
    aliases = {}
    if prev is not None:
        args += list(prev)
        in_specs += [pl.BlockSpec(memory_space=pl.ANY)] * 2
        aliases = {2: 0, 3: 1}
    return pl.pallas_call(
        place_kernel,
        grid=(count,),
        in_specs=in_specs,
        out_specs=[out_spec, out_spec],
        out_shape=[jax.ShapeDtypeStruct(shape, dtype)] * 2,
        input_output_aliases=aliases,
        cost_estimate=pl.CostEstimate(flops=count * seq_len * hidden * 64, bytes_accessed=count * seq_len * hidden * 8, transcendentals=0),
        name=f"place_{start}",
    )(*args)


def chunk_sizes(rows):
    return [rows // 8, rows // 8, rows // 4, rows // 4, rows // 4]


def solution(mesh):
    devices = mesh.shape['model']

    def body(x_in, seg_ids, ln_gain, w_qkv, w_out, w_up, w_down, dy_in):
        rows, seq_len, hidden = x_in.shape
        wqkv = w_qkv.transpose(1, 2, 3, 0).reshape(-1, hidden)
        wo = w_out.reshape(-1, hidden)
        seg = seg_ids.reshape(rows, 1, seq_len)
        gain = ln_gain.reshape(1, hidden)
        gain_f32 = ln_gain.astype(jnp.float32)
        me = lax.axis_index('model')
        x_flat = x_in.reshape(rows * seq_len, hidden)
        dy_flat = dy_in.reshape(rows * seq_len, hidden)

        acc, start, parts = None, 0, []
        for count in chunk_sizes(rows):
            shares, *acc = rows_call(start, count, devices, x_in, dy_in, seg, gain, wqkv, wo, w_up, w_down, acc)
            parts.append((start, count, lax.psum_scatter(shares, 'model', scatter_dimension=0, tiled=False)))
            start += count

        d_gain = jnp.zeros((hidden,), jnp.float32)
        local = []
        for start, count, summed in parts:
            per = summed.shape[1]
            at = start * seq_len + me * per
            x_f32 = lax.dynamic_slice_in_dim(x_flat, at, per, 0).astype(jnp.float32)
            dy_f32 = lax.dynamic_slice_in_dim(dy_flat, at, per, 0).astype(jnp.float32)
            normed, inv_std = norm_rows(x_f32)
            y_loc = (x_f32 + summed[0].astype(jnp.float32)).astype(jnp.bfloat16)
            grad = summed[1].astype(jnp.float32)
            d_gain += jnp.sum(grad * normed, axis=0)
            d_hat = grad * gain_f32
            d_x = inv_std * (d_hat - jnp.mean(d_hat, axis=-1, keepdims=True) - normed * jnp.mean(d_hat * normed, axis=-1, keepdims=True))
            dx_loc = (dy_f32 + d_x).astype(jnp.bfloat16)
            local.append((start, count, jnp.stack([y_loc, dx_loc])))
        out = None
        for start, count, pair in reversed(local):
            gathered = lax.all_gather(pair, 'model', axis=0, tiled=False)
            out = place_call(start, count, gathered, x_in.shape, x_in.dtype, out)
        d_gain = lax.psum(d_gain, 'model').astype(jnp.bfloat16)
        acc_in, acc_out = acc
        n_qkv = wqkv.shape[0]
        d_wqkv = acc_in[:n_qkv].astype(jnp.bfloat16).reshape(w_qkv.shape[1:] + (hidden,)).transpose(3, 0, 1, 2)
        d_wup = acc_in[n_qkv:].astype(jnp.bfloat16).T
        n_o = wo.shape[0]
        d_wout = acc_out[:n_o].astype(jnp.bfloat16).reshape(w_out.shape)
        d_wdown = acc_out[n_o:].astype(jnp.bfloat16)
        return out[0], out[1], d_gain, d_wqkv, d_wout, d_wup, d_wdown

    in_specs = (P('data'), P('data'), P(), P(None, 'model'), P('model'), P(None, 'model'), P('model'), P('data'))
    out_specs = (P('data'), P('data'), P('data'), P('data', 'model'), P(('data', 'model')), P('data', 'model'), P(('data', 'model')))
    return jax.shard_map(body, mesh=mesh, in_specs=in_specs, out_specs=out_specs, check_vma=False)
```

```python
import functools
import math

import jax
import jax.numpy as jnp
from jax import lax
from jax.experimental import pallas as pl
from jax.experimental.pallas import tpu as pltpu
from jax.sharding import PartitionSpec as P

LN_EPS = 1e-5
RING = 4
STAGES = 3
MESH = pl.DeviceIdType.MESH
NT = (((1,), (1,)), ((), ()))
NN = (((1,), (0,)), ((), ()))
TN = (((0,), (0,)), ((), ()))
ORDER = ((2, 2), (2, 1), (1, 2), (2, 3), (3, 2), (1, 1), (3, 3), (1, 3), (3, 1),
         (2, 0), (0, 2), (1, 0), (0, 1), (3, 0), (0, 3), (0, 0))
VMEM_LIMIT = 62 * 2 ** 20


def dot(lhs, rhs, dims):
    return lax.dot_general(lhs, rhs, dims, preferred_element_type=jnp.float32)


def norm_rows(x_f32):
    mean_val = jnp.mean(x_f32, axis=-1, keepdims=True)
    centered = x_f32 - mean_val
    inv_std = lax.rsqrt(jnp.mean(centered * centered, axis=-1, keepdims=True) + LN_EPS)
    return centered * inv_std, inv_std


class Place:
    def __init__(self):
        me = lax.axis_index('model')
        self.core = me % 2
        self.x = (me // 2) % RING
        self.y = me // (2 * RING)
        self.me = me

    def index(self, d_y, d_x, core=None):
        core = self.core if core is None else core
        return (((self.y + d_y) % RING) * RING + (self.x + d_x) % RING) * 2 + core

    def peer(self, axis, offset):
        return self.index(offset % RING, 0) if axis == 'y' else self.index(0, offset % RING)

    def sibling(self):
        return self.index(0, 0, 1 - self.core)


def remote(src, dst, send_sem, recv_sem, device):
    return pltpu.make_async_remote_copy(src_ref=src, dst_ref=dst, send_sem=send_sem, recv_sem=recv_sem,
                                        device_id={'model': device}, device_id_type=MESH)


def enter(peers):
    barrier = pltpu.get_barrier_semaphore()
    for peer in peers:
        pl.semaphore_signal(barrier, inc=1, device_id={'model': peer}, device_id_type=MESH)
    pl.semaphore_wait(barrier, len(peers))


def pick(step, values):
    out = jnp.int32(0)
    for n, value in enumerate(values):
        out = jnp.where(step == n, value, out)
    return out


def add_into(dst, *sources):
    rows = dst.shape[0]
    tile = min(rows, 32)

    def tile_add(n, carry):
        at = pl.ds(pl.multiple_of(n * tile, tile), tile)
        total = dst[at, :].astype(jnp.float32)
        for source in sources:
            total += source[at, :].astype(jnp.float32)
        dst[at, :] = total.astype(dst.dtype)
        return carry

    lax.fori_loop(0, rows // tile, tile_add, 0)


def reduce_kernel(x_hbm, dy_hbm, seg_ref, gain_ref, wqkv_hbm, w1t_hbm, wo_hbm, w2_hbm,
                  y_own, dx_own, dgain_ref, g_own, g_sib, full,
                  w_in, w_out, acc_in, acc_out, x_buf, dy_buf, a_scr, h_scr, d_scr, stage, half, tmp,
                  row_sem, w_sem, ws_sem, wr_sem, send_sem, half_sem, full_sem, tmp_sem, out_sem):
    place = Place()
    core = place.core
    _, seq_len, hidden = x_buf.shape
    mid = seq_len // 2
    n_qkv, n_up, n_o, n_dn = wqkv_hbm.shape[0], w1t_hbm.shape[0], wo_hbm.shape[0], w2_hbm.shape[0]
    head_dim = n_o
    steps = len(ORDER)

    def row_of(step):
        d_y = pick(step, [o[0] for o in ORDER])
        d_x = pick(step, [o[1] for o in ORDER])
        return place.index(d_y, d_x)

    def row_copies(step):
        row, buf = row_of(step), step % 2
        return (pltpu.make_async_copy(x_hbm.at[row], x_buf.at[buf], row_sem.at[buf, 0]),
                pltpu.make_async_copy(dy_hbm.at[row], dy_buf.at[buf], row_sem.at[buf, 1]))

    def weight_spots(side):
        return ((wqkv_hbm, w_in.at[pl.ds(pl.multiple_of(side * n_qkv, 16), n_qkv)]),
                (w1t_hbm, w_in.at[pl.ds(pl.multiple_of(2 * n_qkv + side * n_up, 16), n_up)]),
                (wo_hbm, w_out.at[pl.ds(pl.multiple_of(side * n_o, 16), n_o)]),
                (w2_hbm, w_out.at[pl.ds(pl.multiple_of(2 * n_o + side * n_dn, 16), n_dn)]))

    for copy in row_copies(0):
        copy.start()
    mine = [pltpu.make_async_copy(src, dst, w_sem.at[n]) for n, (src, dst) in enumerate(weight_spots(core))]
    for copy in mine:
        copy.start()
    enter([place.peer('x', 1), place.peer('x', -1), place.peer('y', 1), place.peer('y', -1), place.sibling()])
    swaps = [remote(src, dst, ws_sem.at[n], wr_sem.at[n], place.sibling()) for n, (src, dst) in enumerate(weight_spots(core))]
    for copy in swaps:
        copy.start()
    acc_in[...] = jnp.zeros_like(acc_in)
    acc_out[...] = jnp.zeros_like(acc_out)
    for copy in mine:
        copy.wait()
    for copy in swaps:
        copy.wait()

    gain = gain_ref[...].astype(jnp.float32)
    scale = head_dim ** -0.5
    sub = min(seq_len, 64)
    cols_step = min(hidden, 512)

    def slot_sends(slot):
        return [pltpu.make_async_copy(stage.at[slot, t, pl.ds(piece * mid, mid)], stage.at[slot, t, pl.ds(piece * mid, mid)],
                                      send_sem.at[slot, t, piece]) for t in range(2) for piece in range(2)]

    def send(slot, t, piece, dst, recv_sem, device):
        remote(stage.at[slot, t, pl.ds(piece * mid, mid)], dst, send_sem.at[slot, t, piece], recv_sem, device).start()

    def hop(slot, t, axis, offset, line):
        ahead, behind = place.peer(axis, 1), place.peer(axis, -1)
        spot = stage.at[slot, t]
        if offset == 2:
            send(slot, t, 0, half.at[t, line, 0], half_sem.at[t, line, 0], ahead)
            send(slot, t, 1, half.at[t, line, 1], half_sem.at[t, line, 1], behind)
            return
        if offset in (1, 3):
            piece = 0 if offset == 1 else 1
            came = half.at[t, line, piece]
            pltpu.make_async_copy(came, came, half_sem.at[t, line, piece]).wait()
            add_into(spot.at[pl.ds(piece * mid, mid)], came)
            for n in range(2):
                send(slot, t, n, full.at[t, line, piece, pl.ds(n * mid, mid)], full_sem.at[t, line, piece, n],
                     ahead if offset == 1 else behind)
            return
        loads = []
        for side in range(2):
            for n in range(2):
                came = full.at[t, line, side, pl.ds(n * mid, mid)]
                pltpu.make_async_copy(came, came, full_sem.at[t, line, side, n]).wait()
            load = pltpu.make_async_copy(full.at[t, line, side], tmp.at[side], tmp_sem.at[side])
            load.start()
            loads.append(load)
        for load in loads:
            load.wait()
        add_into(spot, tmp.at[0], tmp.at[1])

    def row_step(step, carry):
        buf = step % 2
        slot = step % STAGES
        for copy in row_copies(step):
            copy.wait()

        @pl.when(step + 1 < steps)
        def _():
            for copy in row_copies(step + 1):
                copy.start()

        for t in range(0, seq_len, sub):
            normed, _ = norm_rows(x_buf[buf, t:t + sub, :].astype(jnp.float32))
            a_scr[t:t + sub, :] = (normed * gain).astype(jnp.bfloat16)

        proj = dot(w_in[...], a_scr[...], NT)
        qkv = proj[:2 * n_qkv].astype(jnp.bfloat16)
        up = proj[2 * n_qkv:].astype(jnp.bfloat16).astype(jnp.float32)
        d_proj = dot(w_out[...], dy_buf[buf], NT).astype(jnp.bfloat16)
        d_attn = d_proj[:2 * n_o]
        d_hid = d_proj[2 * n_o:].astype(jnp.float32)
        cdf = 0.5 * (1.0 + lax.erf(up * (0.5 ** 0.5)))
        h_scr[2 * n_o:, :] = (up * cdf).astype(jnp.bfloat16)
        slope = cdf + up * (jnp.exp(-0.5 * up * up) * 0.3989422804014327)
        d_scr[2 * n_qkv:, :] = (d_hid * slope).astype(jnp.bfloat16)

        seg_row = seg_ref[row_of(step)]
        classes = lax.broadcasted_iota(jnp.int32, (16, seq_len), 0)
        one_hot = (classes == jnp.broadcast_to(seg_row, (16, seq_len))).astype(jnp.bfloat16)
        same = dot(one_hot, one_hot, TN) > 0.5
        key_id = lax.broadcasted_iota(jnp.int32, (seq_len, seq_len), 0)
        query_id = lax.broadcasted_iota(jnp.int32, (seq_len, seq_len), 1)
        allowed = (key_id <= query_id) & same
        for head in range(2):
            at = head * n_qkv
            query = qkv[at:at + head_dim]
            keys = qkv[at + head_dim:at + 2 * head_dim]
            values = qkv[at + 2 * head_dim:at + 3 * head_dim]
            d_o = d_attn[head * head_dim:(head + 1) * head_dim]
            scores = jnp.where(allowed, dot(keys, query, TN) * scale, -1e30)
            expd = jnp.exp(scores - jnp.max(scores, axis=0, keepdims=True))
            probs = expd / jnp.sum(expd, axis=0, keepdims=True)
            probs_b = probs.astype(jnp.bfloat16)
            h_scr[head * head_dim:(head + 1) * head_dim, :] = dot(values, probs_b, NN).astype(jnp.bfloat16)
            d_p = dot(values, d_o, TN)
            d_s = (probs * (d_p - jnp.sum(d_p * probs, axis=0, keepdims=True)) * scale).astype(jnp.bfloat16)
            d_scr[at:at + head_dim, :] = dot(keys, d_s, NN).astype(jnp.bfloat16)
            d_scr[at + head_dim:at + 2 * head_dim, :] = dot(query, d_s, NT).astype(jnp.bfloat16)
            d_scr[at + 2 * head_dim:at + 3 * head_dim, :] = dot(d_o, probs_b, NT).astype(jnp.bfloat16)

        @pl.when(step >= STAGES)
        def _():
            for copy in slot_sends(slot):
                copy.wait()

        for h in range(0, hidden, cols_step):
            cols = slice(h, h + cols_step)
            stage[slot, 0, :, cols] = dot(h_scr[...], w_out[:, cols], TN).astype(jnp.bfloat16)
            stage[slot, 1, :, cols] = dot(d_scr[...], w_in[:, cols], TN).astype(jnp.bfloat16)
            acc_in[:, cols] += dot(d_scr[...], a_scr[:, cols], NN)
            acc_out[:, cols] += dot(h_scr[...], dy_buf[buf, :, cols], NN)

        for n, (d_y, d_x) in enumerate(ORDER):
            @pl.when(step == n)
            def _():
                at = n % STAGES
                for t, first, second in ((0, ('x', d_x), ('y', d_y)), (1, ('y', d_y), ('x', d_x))):
                    hop(at, t, *first, second[1])
                    if first[1] == 0:
                        hop(at, t, *second, RING)
        return carry

    lax.fori_loop(0, steps, row_step, 0)

    outs = []
    for n, (side, dst) in enumerate(((core, g_own), (1 - core, g_sib))):
        to = 0
        for m, (acc, at, count) in enumerate(((acc_in, side * n_qkv, n_qkv), (acc_in, 2 * n_qkv + side * n_up, n_up),
                                              (acc_out, side * n_o, n_o), (acc_out, 2 * n_o + side * n_dn, n_dn))):
            outs.append(pltpu.make_async_copy(acc.at[pl.ds(pl.multiple_of(at, 16), count)], dst.at[pl.ds(to, count)], out_sem.at[4 * n + m]))
            to += count
    for copy in outs:
        copy.start()
    for n in range(max(0, steps - STAGES), steps - 1):
        for copy in slot_sends(n % STAGES):
            copy.wait()

    last, buf = (steps - 1) % STAGES, (steps - 1) % 2
    d_gain = jnp.zeros((1, hidden), jnp.float32)
    fine = min(seq_len, 32)

    def finish(n, d_gain):
        at = pl.ds(pl.multiple_of(n * fine, fine), fine)
        x_f32 = x_buf[buf, at, :].astype(jnp.float32)
        normed, inv_std = norm_rows(x_f32)
        grad = stage[last, 1, at, :].astype(jnp.float32)
        stage[last, 0, at, :] = (x_f32 + stage[last, 0, at, :].astype(jnp.float32)).astype(jnp.bfloat16)
        d_hat = grad * gain
        d_x = inv_std * (d_hat - jnp.mean(d_hat, axis=-1, keepdims=True) - normed * jnp.mean(d_hat * normed, axis=-1, keepdims=True))
        stage[last, 1, at, :] = (dy_buf[buf, at, :].astype(jnp.float32) + d_x).astype(jnp.bfloat16)
        return d_gain + jnp.sum(grad * normed, axis=0, keepdims=True)

    dgain_ref[...] = lax.fori_loop(0, seq_len // fine, finish, d_gain)
    ends = [pltpu.make_async_copy(stage.at[last, t], dst, tmp_sem.at[t]) for t, dst in ((0, y_own), (1, dx_own))]
    for copy in ends:
        copy.start()
    for copy in ends + outs:
        copy.wait()


def gather_kernel(y_own, dx_own, dgain_ref, g_sib, y_all, dx_all, g_recv, dgain_out, gain_scr,
                  send_sem, link_sem, pair_sem, pair_recv, own_sem, g_sem, dg_send, dg_recv):
    place = Place()
    seq_len = y_all.shape[1]
    mid = seq_len // 2
    outs = (y_all, dx_all)
    owns = (y_own, dx_own)
    links = (('x', 1), ('x', -1), ('y', 1), ('y', -1))
    enter([place.peer(a, o) for a in ('x', 'y') for o in (1, 2, 3)] + [place.sibling()])

    issued = {link: [] for link in links}
    sends = []

    def row_index(t, d_1, d_2):
        return place.index(d_1, d_2) if t == 0 else place.index(d_2, d_1)

    def issue(link, t, d_1, d_2, piece):
        n = len(issued[link])
        row = row_index(t, d_1 % RING, d_2 % RING)
        spot = outs[t].at[row, pl.ds(piece * mid, mid)]
        src = owns[t].at[pl.ds(piece * mid, mid)] if (d_1, d_2) == (0, 0) else spot
        which = links.index(link)
        copy = remote(src, spot, send_sem.at[which, n], link_sem.at[which, n], place.peer(*link))
        copy.start()
        sends.append(copy)
        issued[link].append((t, d_1, d_2, piece))

    def pair(t, d_1, d_2, piece):
        row = row_index(t, d_1 % RING, d_2 % RING)
        spot = outs[t].at[row, pl.ds(piece * mid, mid)]
        src = owns[t].at[pl.ds(piece * mid, mid)] if (d_1, d_2) == (0, 0) else spot
        slot = ((d_1 % RING) * RING + d_2 % RING) * 2 + piece
        copy = remote(src, spot, pair_sem.at[t, slot], pair_recv.at[t], place.sibling())
        copy.start()
        sends.append(copy)

    axes = (('y', 'x'), ('x', 'y'))
    for piece in range(2):
        for t in range(2):
            for way in (1, -1):
                issue((axes[t][0], way), t, 0, 0, piece)
    for piece in range(2):
        for t in range(2):
            for way in (1, -1):
                issue((axes[t][1], way), t, 0, 0, piece)
    locals_ = []
    for t in range(2):
        for piece in range(2):
            pair(t, 0, 0, piece)
        copy = pltpu.make_async_copy(owns[t], outs[t].at[place.me], own_sem.at[t])
        copy.start()
        locals_.append(copy)
    g_copy = remote(g_sib, g_recv, g_sem.at[0], g_sem.at[1], place.sibling())
    g_copy.start()

    total = dgain_ref[...]
    for n, (axis, offsets) in enumerate((('core', (1,)), ('x', (1, 2, 3)), ('y', (1, 2, 3)))):
        spot = {'core': place.core, 'x': place.x, 'y': place.y}[axis]
        gain_scr[n, spot] = total
        copies = []
        for m, offset in enumerate(offsets):
            device = place.sibling() if axis == 'core' else place.peer(axis, offset)
            copies.append(remote(gain_scr.at[n, spot], gain_scr.at[n, spot], dg_send.at[n, m], dg_recv.at[n, m], device))
        for copy in copies:
            copy.start()
        for copy in copies:
            copy.wait()
        total = gain_scr[n, 0]
        for m in range(1, len(offsets) + 1):
            total = total + gain_scr[n, m]
    dgain_out[...] = total.astype(dgain_out.dtype)

    rounds = 4 * (RING * RING - 1) // 4
    for n in range(rounds):
        for link in links:
            t, d_1, d_2, piece = issued[link][n]
            axis, way = link
            on_first = axis == axes[t][0]
            d_1, d_2 = (d_1 - way, d_2) if on_first else (d_1, d_2 - way)
            row = row_index(t, d_1 % RING, d_2 % RING)
            spot = outs[t].at[row, pl.ds(piece * mid, mid)]
            pltpu.make_async_copy(spot, spot, link_sem.at[links.index(link), n]).wait()
            along = d_1 if on_first else d_2
            if abs(along) == 1 and piece == (0 if way == 1 else 1):
                issue(link, t, d_1, d_2, piece)
            if on_first:
                for other in (1, -1):
                    issue((axes[t][1], other), t, d_1, d_2, piece)
            pair(t, d_1, d_2, piece)

    for t in range(2):
        theirs = outs[t].at[pl.ds(0, RING * RING)]
        pltpu.make_async_copy(theirs, theirs, pair_recv.at[t]).wait()
    for copy in sends:
        copy.wait_send()
    for copy in locals_:
        copy.wait()
    g_copy.wait()


def solution(mesh):
    devices = mesh.shape['model']
    assert devices == 2 * RING * RING and math.isqrt(devices // 2) == RING

    def body(x_in, seg_ids, ln_gain, w_qkv, w_out, w_up, w_down, dy_in):
        rows, seq_len, hidden = x_in.shape
        assert rows == devices
        wqkv = w_qkv.transpose(1, 2, 3, 0).reshape(-1, hidden)
        w1t = w_up.T
        wo = w_out.reshape(-1, hidden)
        n_qkv, n_up, n_o, n_dn = wqkv.shape[0], w1t.shape[0], wo.shape[0], w_down.shape[0]
        n_in, n_out = n_qkv + n_up, n_o + n_dn
        bf16, f32 = jnp.bfloat16, jnp.float32
        vmem, anywhere = pl.BlockSpec(memory_space=pltpu.VMEM), pl.BlockSpec(memory_space=pl.ANY)
        dma = pltpu.SemaphoreType.DMA
        shape = jax.ShapeDtypeStruct
        mid = seq_len // 2
        y_own, dx_own, d_gain, g_own, g_sib, _ = pl.pallas_call(
            reduce_kernel,
            in_specs=[anywhere, anywhere, vmem, vmem] + [anywhere] * 4,
            out_specs=[anywhere, anywhere, vmem, anywhere, anywhere, anywhere],
            out_shape=[shape((seq_len, hidden), bf16), shape((seq_len, hidden), bf16), shape((1, hidden), f32),
                       shape((n_in + n_out, hidden), f32), shape((n_in + n_out, hidden), f32),
                       shape((2, RING + 1, 2, seq_len, hidden), bf16)],
            scratch_shapes=[
                pltpu.VMEM((2 * n_in, hidden), bf16), pltpu.VMEM((2 * n_out, hidden), bf16),
                pltpu.VMEM((2 * n_in, hidden), f32), pltpu.VMEM((2 * n_out, hidden), f32),
                pltpu.VMEM((2, seq_len, hidden), bf16), pltpu.VMEM((2, seq_len, hidden), bf16),
                pltpu.VMEM((seq_len, hidden), bf16),
                pltpu.VMEM((2 * n_out, seq_len), bf16), pltpu.VMEM((2 * n_in, seq_len), bf16),
                pltpu.VMEM((STAGES, 2, seq_len, hidden), bf16),
                pltpu.VMEM((2, RING + 1, 2, mid, hidden), bf16),
                pltpu.VMEM((2, seq_len, hidden), bf16),
                dma((2, 2)), dma((4,)), dma((4,)), dma((4,)), dma((STAGES, 2, 2)),
                dma((2, RING + 1, 2)), dma((2, RING + 1, 2, 2)), dma((2,)), dma((8,)),
            ],
            compiler_params=pltpu.CompilerParams(collective_id=0, has_side_effects=True, vmem_limit_bytes=VMEM_LIMIT),
            name="rows_reduce",
        )(x_in, dy_in, seg_ids.reshape(rows, 1, seq_len), ln_gain.reshape(1, hidden), wqkv, w1t, wo, w_down)

        per_link = RING * RING - 1
        y_out, dx_out, g_recv, d_gain = pl.pallas_call(
            gather_kernel,
            in_specs=[anywhere, anywhere, vmem, anywhere],
            out_specs=[anywhere, anywhere, anywhere, vmem],
            out_shape=[shape(x_in.shape, bf16), shape(x_in.shape, bf16), shape(g_sib.shape, f32), shape((1, hidden), bf16)],
            scratch_shapes=[
                pltpu.VMEM((3, RING, 1, hidden), f32),
                dma((4, per_link)), dma((4, per_link)), dma((2, 2 * RING * RING)), dma((2,)), dma((2,)), dma((2,)),
                dma((3, 3)), dma((3, 3)),
            ],
            compiler_params=pltpu.CompilerParams(collective_id=1, has_side_effects=True, vmem_limit_bytes=VMEM_LIMIT),
            name="rows_gather",
        )(y_own, dx_own, d_gain, g_sib)

        grads = (g_own + g_recv).astype(bf16)
        d_wqkv = grads[:n_qkv].reshape(w_qkv.shape[1:] + (hidden,)).transpose(3, 0, 1, 2)
        d_wup = grads[n_qkv:n_in].T
        d_wout = grads[n_in:n_in + n_o].reshape(w_out.shape)
        d_wdown = grads[n_in + n_o:]
        return y_out, dx_out, d_gain.reshape(hidden), d_wqkv, d_wout, d_wup, d_wdown

    in_specs = (P('data'), P('data'), P(), P(None, 'model'), P('model'), P(None, 'model'), P('model'), P('data'))
    out_specs = (P('data'), P('data'), P('data'), P('data', 'model'), P(('data', 'model')), P('data', 'model'), P(('data', 'model')))
    return jax.shard_map(body, mesh=mesh, in_specs=in_specs, out_specs=out_specs, check_vma=False)
```

```python
import functools
import math

import jax
import jax.numpy as jnp
from jax import lax
from jax.experimental import pallas as pl
from jax.experimental.pallas import tpu as pltpu
from jax.sharding import PartitionSpec as P

LN_EPS = 1e-5
RING = 4
MESH = pl.DeviceIdType.MESH
NT = (((1,), (1,)), ((), ()))
NN = (((1,), (0,)), ((), ()))
TN = (((0,), (0,)), ((), ()))
ORDER = ((2, 2), (1, 2), (2, 3), (3, 2), (2, 1), (0, 1), (1, 1), (3, 3),
         (2, 0), (0, 2), (3, 0), (1, 3), (3, 1), (0, 3), (1, 0), (0, 0))
SLOT = (0, 1, 2, 3, 4, 0, 1, 2, 3, 4, 2, 1, 3, 4, 1, 3)
SLOTS = max(SLOT) + 1
EVENTS = (
    ((0, 0, 0, 1), (0, 0, 1, 1), (0, 1, 0, 1), (0, 1, 1, 1)),
    ((1, 0, 0, 1), (1, 0, 1, 1), (1, 1, 1, 1)),
    ((2, 0, 0, 1), (2, 1, 0, 1), (2, 1, 1, 1), (1, 1, 0, 1), (2, 0, 1, 1)),
    ((3, 0, 0, 1), (3, 0, 1, 1), (3, 1, 0, 1), (3, 1, 1, 1)),
    ((4, 0, 1, 1), (4, 1, 0, 1), (4, 1, 1, 1), (4, 0, 0, 1)),
    ((5, 0, 1, 1),),
    ((6, 0, 1, 1), (6, 1, 1, 1), (6, 0, 0, 1)),
    ((7, 0, 0, 1), (7, 1, 0, 1), (7, 1, 1, 1)),
    ((8, 1, 0, 1), (8, 1, 1, 1), (8, 0, 1, 1), (8, 0, 1, 2), (6, 1, 0, 1), (7, 0, 1, 1), (8, 0, 0, 1), (8, 0, 0, 2)),
    ((9, 0, 0, 1), (9, 0, 1, 1), (9, 1, 0, 1), (9, 1, 0, 2), (9, 1, 1, 1), (9, 1, 1, 2)),
    ((10, 1, 0, 1),),
    ((11, 0, 0, 1), (11, 1, 1, 1), (11, 0, 1, 1), (11, 1, 0, 1), (10, 1, 1, 1)),
    ((12, 0, 1, 1), (12, 1, 0, 1), (12, 0, 0, 1), (12, 1, 1, 1), (5, 0, 0, 1)),
    ((13, 0, 0, 1), (13, 0, 1, 1), (13, 1, 1, 1), (13, 1, 1, 2)),
    ((14, 1, 1, 1), (14, 1, 0, 1), (14, 0, 0, 1), (14, 0, 0, 2), (10, 0, 1, 1), (10, 0, 1, 2), (13, 1, 0, 1), (13, 1, 0, 2), (14, 0, 1, 1), (14, 0, 1, 2), (10, 0, 0, 1), (10, 0, 0, 2), (5, 1, 0, 1), (5, 1, 0, 2)),
    ((15, 1, 1, 1), (15, 0, 0, 1), (15, 0, 1, 1), (5, 1, 1, 1), (5, 1, 1, 2), (15, 1, 0, 1), (15, 1, 0, 2), (15, 1, 1, 2), (15, 0, 0, 2), (15, 0, 1, 2)),
)
VMEM_LIMIT = 62 * 2 ** 20


def dot(lhs, rhs, dims):
    return lax.dot_general(lhs, rhs, dims, preferred_element_type=jnp.float32)


def norm_rows(x_f32):
    mean_val = jnp.mean(x_f32, axis=-1, keepdims=True)
    centered = x_f32 - mean_val
    inv_std = lax.rsqrt(jnp.mean(centered * centered, axis=-1, keepdims=True) + LN_EPS)
    return centered * inv_std, inv_std


class Place:
    def __init__(self):
        me = lax.axis_index('model')
        self.core = me % 2
        self.x = (me // 2) % RING
        self.y = me // (2 * RING)
        self.me = me

    def index(self, d_y, d_x, core=None):
        core = self.core if core is None else core
        return (((self.y + d_y) % RING) * RING + (self.x + d_x) % RING) * 2 + core

    def peer(self, axis, offset):
        return self.index(offset % RING, 0) if axis == 'y' else self.index(0, offset % RING)

    def sibling(self):
        return self.index(0, 0, 1 - self.core)


def remote(src, dst, send_sem, recv_sem, device):
    return pltpu.make_async_remote_copy(src_ref=src, dst_ref=dst, send_sem=send_sem, recv_sem=recv_sem,
                                        device_id={'model': device}, device_id_type=MESH)


def enter(peers):
    barrier = pltpu.get_barrier_semaphore()
    for peer in peers:
        pl.semaphore_signal(barrier, inc=1, device_id={'model': peer}, device_id_type=MESH)
    pl.semaphore_wait(barrier, len(peers))


def pick(step, values):
    out = jnp.int32(0)
    for n, value in enumerate(values):
        out = jnp.where(step == n, value, out)
    return out


def add_into(dst, *sources):
    rows = dst.shape[0]
    tile = min(rows, 32)

    def tile_add(n, carry):
        at = pl.ds(pl.multiple_of(n * tile, tile), tile)
        total = dst[at, :].astype(jnp.float32)
        for source in sources:
            total += source[at, :].astype(jnp.float32)
        dst[at, :] = total.astype(dst.dtype)
        return carry

    lax.fori_loop(0, rows // tile, tile_add, 0)


def reduce_kernel(x_hbm, dy_hbm, seg_ref, gain_ref, wqkv_hbm, w1_hbm, wo_hbm, w2_hbm,
                  y_own, dx_own, dgain_ref, g_own, g_sib, full,
                  w_in, w_out, w1_raw, acc_in, acc_out, x_buf, dy_buf, a_scr, h_scr, d_scr, stage, half, last_full, tmp,
                  row_sem, w_sem, ws_sem, wr_sem, send_sem, half_sem, full_sem, tmp_sem, out_sem):
    place = Place()
    core = place.core
    _, seq_len, hidden = x_buf.shape
    mid = seq_len // 2
    n_qkv, n_up, n_o, n_dn = wqkv_hbm.shape[0], w1_hbm.shape[1], wo_hbm.shape[0], w2_hbm.shape[0]
    head_dim = n_o
    steps = len(ORDER)

    def row_of(step):
        d_y = pick(step, [o[0] for o in ORDER])
        d_x = pick(step, [o[1] for o in ORDER])
        return place.index(d_y, d_x)

    def row_copies(step):
        row, buf = row_of(step), step % 2
        return (pltpu.make_async_copy(x_hbm.at[row], x_buf.at[buf], row_sem.at[buf, 0]),
                pltpu.make_async_copy(dy_hbm.at[row], dy_buf.at[buf], row_sem.at[buf, 1]))

    def rows_at(ref, at, count):
        return ref.at[pl.ds(pl.multiple_of(at, 16), count)]

    up_spot = rows_at(w_in, 2 * n_qkv + core * n_up, n_up)
    spots = ((wqkv_hbm, rows_at(w_in, core * n_qkv, n_qkv)), (wo_hbm, rows_at(w_out, core * n_o, n_o)),
             (w2_hbm, rows_at(w_out, 2 * n_o + core * n_dn, n_dn)))

    raw = pltpu.make_async_copy(w1_hbm, w1_raw, w_sem.at[3])
    raw.start()
    for copy in row_copies(0):
        copy.start()
    mine = [pltpu.make_async_copy(src, dst, w_sem.at[n]) for n, (src, dst) in enumerate(spots)]
    for copy in mine:
        copy.start()
    enter([place.peer('x', 1), place.peer('x', -1), place.peer('y', 1), place.peer('y', -1), place.sibling()])
    swaps = [remote(src, dst, ws_sem.at[n], wr_sem.at[n], place.sibling()) for n, (src, dst) in enumerate(spots)]
    for copy in swaps:
        copy.start()
    raw.wait()
    turn = min(hidden, 256)
    for h in range(0, hidden, turn):
        up_spot[:, h:h + turn] = w1_raw[h:h + turn, :].T
    acc_in[...] = jnp.zeros_like(acc_in)
    acc_out[...] = jnp.zeros_like(acc_out)
    swaps.append(remote(up_spot, up_spot, ws_sem.at[3], wr_sem.at[3], place.sibling()))
    swaps[3].start()
    for copy in mine:
        copy.wait()
    for copy in swaps:
        copy.wait()

    gain = gain_ref[...].astype(jnp.float32)
    scale = head_dim ** -0.5
    sub = min(seq_len, 64)
    cols_step = min(hidden, 512)

    def piece_of(ref, piece):
        return ref.at[pl.ds(piece * mid, mid)]

    def landed(ref, sem):
        pltpu.make_async_copy(ref, ref, sem).wait()

    def slot_sends(slot):
        return [pltpu.make_async_copy(piece_of(stage.at[slot, t], piece), piece_of(stage.at[slot, t], piece),
                                      send_sem.at[slot, t, piece]) for t in range(2) for piece in range(2)]

    def event(n, t, piece, ring):
        d_y, d_x = ORDER[n]
        first, second = (('x', d_x), ('y', d_y)) if t == 0 else (('y', d_y), ('x', d_x))
        (axis, offset), line = (first, second[1]) if ring == 1 else (second, RING)
        ahead, behind = place.peer(axis, 1), place.peer(axis, -1)
        spot = piece_of(stage.at[SLOT[n], t], piece)

        def arrival(side):
            return piece_of(last_full.at[t, side] if line == RING else full.at[t, line, side], piece)

        def send(dst, recv_sem, device):
            remote(spot, dst, send_sem.at[SLOT[n], t, piece], recv_sem, device).start()

        if offset == 2:
            send(half.at[t, line, piece], half_sem.at[t, line, piece], ahead if piece == 0 else behind)
        elif offset in (1, 3):
            side = 0 if offset == 1 else 1
            if side == piece:
                landed(half.at[t, line, piece], half_sem.at[t, line, piece])
                add_into(spot, half.at[t, line, piece])
            send(arrival(side), full_sem.at[t, line, side, piece], ahead if side == 0 else behind)
        elif line == RING:
            for side in range(2):
                landed(arrival(side), full_sem.at[t, line, side, piece])
            add_into(spot, arrival(0), arrival(1))
        else:
            loads = [pltpu.make_async_copy(arrival(side), tmp.at[piece, side], tmp_sem.at[piece, side]) for side in range(2)]
            for side in range(2):
                landed(arrival(side), full_sem.at[t, line, side, piece])
                loads[side].start()
            for load in loads:
                load.wait()
            add_into(spot, tmp.at[piece, 0], tmp.at[piece, 1])

    def grad_copies():
        copies = []
        for n, (side, dst) in enumerate(((core, g_own), (1 - core, g_sib))):
            to = 0
            for m, (acc, at, count) in enumerate(((acc_in, side * n_qkv, n_qkv), (acc_in, 2 * n_qkv + side * n_up, n_up),
                                                  (acc_out, side * n_o, n_o), (acc_out, 2 * n_o + side * n_dn, n_dn))):
                copies.append(pltpu.make_async_copy(rows_at(acc, at, count), dst.at[pl.ds(to, count)], out_sem.at[4 * n + m]))
                to += count
        return copies

    def row_step(step, carry):
        buf = step % 2
        slot = pick(step, SLOT)
        for copy in row_copies(step):
            copy.wait()

        @pl.when(step + 1 < steps)
        def _():
            for copy in row_copies(step + 1):
                copy.start()

        for t in range(0, seq_len, sub):
            normed, _ = norm_rows(x_buf[buf, t:t + sub, :].astype(jnp.float32))
            a_scr[t:t + sub, :] = (normed * gain).astype(jnp.bfloat16)

        proj = dot(w_in[...], a_scr[...], NT)
        qkv = proj[:2 * n_qkv].astype(jnp.bfloat16)
        up = proj[2 * n_qkv:].astype(jnp.bfloat16).astype(jnp.float32)
        d_proj = dot(w_out[...], dy_buf[buf], NT).astype(jnp.bfloat16)
        d_attn = d_proj[:2 * n_o]
        d_hid = d_proj[2 * n_o:].astype(jnp.float32)
        cdf = 0.5 * (1.0 + lax.erf(up * (0.5 ** 0.5)))
        h_scr[2 * n_o:, :] = (up * cdf).astype(jnp.bfloat16)
        slope = cdf + up * (jnp.exp(-0.5 * up * up) * 0.3989422804014327)
        d_scr[2 * n_qkv:, :] = (d_hid * slope).astype(jnp.bfloat16)

        seg_row = seg_ref[pl.ds(row_of(step), 1), :]
        classes = lax.broadcasted_iota(jnp.int32, (16, seq_len), 0)
        one_hot = (classes == jnp.broadcast_to(seg_row, (16, seq_len))).astype(jnp.bfloat16)
        same = dot(one_hot, one_hot, TN) > 0.5
        key_id = lax.broadcasted_iota(jnp.int32, (seq_len, seq_len), 0)
        query_id = lax.broadcasted_iota(jnp.int32, (seq_len, seq_len), 1)
        allowed = (key_id <= query_id) & same
        for head in range(2):
            at = head * n_qkv
            query = qkv[at:at + head_dim]
            keys = qkv[at + head_dim:at + 2 * head_dim]
            values = qkv[at + 2 * head_dim:at + 3 * head_dim]
            d_o = d_attn[head * head_dim:(head + 1) * head_dim]
            scores = jnp.where(allowed, dot(keys, query, TN) * scale, -1e30)
            expd = jnp.exp(scores - jnp.max(scores, axis=0, keepdims=True))
            probs = expd / jnp.sum(expd, axis=0, keepdims=True)
            probs_b = probs.astype(jnp.bfloat16)
            h_scr[head * head_dim:(head + 1) * head_dim, :] = dot(values, probs_b, NN).astype(jnp.bfloat16)
            d_p = dot(values, d_o, TN)
            d_s = (probs * (d_p - jnp.sum(d_p * probs, axis=0, keepdims=True)) * scale).astype(jnp.bfloat16)
            d_scr[at:at + head_dim, :] = dot(keys, d_s, NN).astype(jnp.bfloat16)
            d_scr[at + head_dim:at + 2 * head_dim, :] = dot(query, d_s, NT).astype(jnp.bfloat16)
            d_scr[at + 2 * head_dim:at + 3 * head_dim, :] = dot(d_o, probs_b, NT).astype(jnp.bfloat16)

        @pl.when(pick(step, [int(SLOT[n] in SLOT[:n]) for n in range(steps)]) == 1)
        def _():
            for copy in slot_sends(slot):
                copy.wait()

        for h in range(0, hidden, cols_step):
            cols = slice(h, h + cols_step)
            stage[slot, 0, :, cols] = dot(h_scr[...], w_out[:, cols], TN).astype(jnp.bfloat16)
            stage[slot, 1, :, cols] = dot(d_scr[...], w_in[:, cols], TN).astype(jnp.bfloat16)
            acc_in[:, cols] += dot(d_scr[...], a_scr[:, cols], NN)
            acc_out[:, cols] += dot(h_scr[...], dy_buf[buf, :, cols], NN)

        for n in range(steps):
            @pl.when(step == n)
            def _():
                if n == steps - 1:
                    for copy in grad_copies():
                        copy.start()
                for work in EVENTS[n]:
                    event(*work)
        return carry

    lax.fori_loop(0, steps, row_step, 0)
    last, buf = SLOT[-1], (steps - 1) % 2
    for slot in range(SLOTS):
        if slot != last:
            for copy in slot_sends(slot):
                copy.wait()

    fine = min(seq_len, 32)

    def finish(n, d_gain):
        at = pl.ds(pl.multiple_of(n * fine, fine), fine)
        x_f32 = x_buf[buf, at, :].astype(jnp.float32)
        normed, inv_std = norm_rows(x_f32)
        grad = stage[last, 1, at, :].astype(jnp.float32)
        stage[last, 0, at, :] = (x_f32 + stage[last, 0, at, :].astype(jnp.float32)).astype(jnp.bfloat16)
        d_hat = grad * gain
        d_x = inv_std * (d_hat - jnp.mean(d_hat, axis=-1, keepdims=True) - normed * jnp.mean(d_hat * normed, axis=-1, keepdims=True))
        stage[last, 1, at, :] = (dy_buf[buf, at, :].astype(jnp.float32) + d_x).astype(jnp.bfloat16)
        return d_gain + jnp.sum(grad * normed, axis=0, keepdims=True)

    dgain_ref[...] = lax.fori_loop(0, seq_len // fine, finish, jnp.zeros((1, hidden), jnp.float32))
    ends = [pltpu.make_async_copy(stage.at[last, t], dst, tmp_sem.at[0, t]) for t, dst in ((0, y_own), (1, dx_own))]
    for copy in ends:
        copy.start()
    for copy in ends + grad_copies():
        copy.wait()


def gather_kernel(y_own, dx_own, dgain_ref, g_own, g_sib, y_lo, y_hi, dx_all, g_recv, dgain_out, grads, d_up,
                  gain_scr, g_buf, t_buf, send_sem, link_sem, pair_sem, pair_recv, own_sem, g_sem, gb_sem, dg_send, dg_recv):
    place = Place()
    _, seq_len, hidden = dx_all.shape
    mid = seq_len // 2
    links = (('x', 1), ('x', -1), ('y', 1), ('y', -1))
    enter([place.peer(a, o) for a in ('x', 'y') for o in (1, 2, 3)] + [place.sibling()])

    issued = {link: [] for link in links}
    sends = []

    def row_index(t, d_1, d_2):
        return place.index(d_1 % RING, d_2 % RING) if t == 0 else place.index(d_2 % RING, d_1 % RING)

    def spot_of(t, row, piece):
        if t == 1:
            return dx_all.at[row, pl.ds(piece * mid, mid)]
        return (y_lo, y_hi)[piece].at[row]

    def source(t, d_1, d_2, piece):
        if (d_1, d_2) == (0, 0):
            return (y_own, dx_own)[t].at[pl.ds(piece * mid, mid)]
        return spot_of(t, row_index(t, d_1, d_2), piece)

    def issue(link, t, d_1, d_2, piece):
        n = len(issued[link])
        which = links.index(link)
        copy = remote(source(t, d_1, d_2, piece), spot_of(t, row_index(t, d_1, d_2), piece),
                      send_sem.at[which, n], link_sem.at[which, n], place.peer(*link))
        copy.start()
        sends.append(copy)
        issued[link].append((t, d_1, d_2, piece))

    def pair(t, d_1, d_2, piece):
        slot = ((d_1 % RING) * RING + d_2 % RING) * 2 + piece
        copy = remote(source(t, d_1, d_2, piece), spot_of(t, row_index(t, d_1, d_2), piece),
                      pair_sem.at[t, slot], pair_recv.at[t, piece], place.sibling())
        copy.start()
        sends.append(copy)

    axes = (('y', 'x'), ('x', 'y'))
    for ring in range(2):
        for piece in range(2):
            for t in range(2):
                for way in (1, -1):
                    issue((axes[t][ring], way), t, 0, 0, piece)
    locals_ = []
    for t in range(2):
        for piece in range(2):
            pair(t, 0, 0, piece)
            copy = pltpu.make_async_copy(source(t, 0, 0, piece), spot_of(t, place.me, piece), own_sem.at[t, piece])
            copy.start()
            locals_.append(copy)
    g_copy = remote(g_sib, g_recv, g_sem.at[0], g_sem.at[1], place.sibling())
    g_copy.start()

    total = dgain_ref[...]
    for n, (axis, offsets) in enumerate((('core', (1,)), ('x', (1, 2, 3)), ('y', (1, 2, 3)))):
        spot = {'core': place.core, 'x': place.x, 'y': place.y}[axis]
        gain_scr[n, spot] = total
        copies = []
        for m, offset in enumerate(offsets):
            device = place.sibling() if axis == 'core' else place.peer(axis, offset)
            copies.append(remote(gain_scr.at[n, spot], gain_scr.at[n, spot], dg_send.at[n, m], dg_recv.at[n, m], device))
        for copy in copies:
            copy.start()
        for copy in copies:
            copy.wait()
        total = gain_scr[n, 0]
        for m in range(1, len(offsets) + 1):
            total = total + gain_scr[n, m]
    dgain_out[...] = total.astype(dgain_out.dtype)

    tile, turn = g_buf.shape[1], t_buf.shape[2]
    n_up = d_up.shape[1]
    n_qkv = 3 * tile

    def grad_tile(at, to):
        loads = [pltpu.make_async_copy(g.at[pl.ds(at, tile)], g_buf.at[n], gb_sem.at[n]) for n, g in enumerate((g_own, g_recv))]
        for load in loads:
            load.start()
        for load in loads:
            load.wait()
        grads[to:to + tile, :] = (g_buf[0] + g_buf[1]).astype(grads.dtype)

    def up_tile(h):
        loads = [pltpu.make_async_copy(g.at[pl.ds(n_qkv, n_up), pl.ds(h, turn)], t_buf.at[n], gb_sem.at[n]) for n, g in enumerate((g_own, g_recv))]
        for load in loads:
            load.start()
        for load in loads:
            load.wait()
        d_up[h:h + turn, :] = (t_buf[0] + t_buf[1]).T.astype(d_up.dtype)

    jobs = [functools.partial(grad_tile, at, at) for at in range(0, n_qkv, tile)]
    jobs += [functools.partial(grad_tile, at, at - n_up) for at in range(n_qkv + n_up, g_own.shape[0], tile)]
    jobs += [functools.partial(up_tile, h) for h in range(0, hidden, turn)]

    rounds = RING * RING - 1
    for n in range(rounds):
        for link in links:
            t, d_1, d_2, piece = issued[link][n]
            axis, way = link
            on_first = axis == axes[t][0]
            d_1, d_2 = (d_1 - way, d_2) if on_first else (d_1, d_2 - way)
            spot = spot_of(t, row_index(t, d_1, d_2), piece)
            pltpu.make_async_copy(spot, spot, link_sem.at[links.index(link), n]).wait()
            along = d_1 if on_first else d_2
            if abs(along) == 1 and piece == (0 if way == 1 else 1):
                issue(link, t, d_1, d_2, piece)
            if on_first:
                for other in (1, -1):
                    issue((axes[t][1], other), t, d_1, d_2, piece)
            pair(t, d_1, d_2, piece)
        if n == 2:
            g_copy.wait()
        if n >= 2:
            for job in jobs[(n - 2) * len(jobs) // (rounds - 2):(n - 1) * len(jobs) // (rounds - 2)]:
                job()

    for t in range(2):
        for piece in range(2):
            theirs = dx_all.at[pl.ds(0, RING * RING), pl.ds(piece * mid, mid)] if t else (y_lo, y_hi)[piece].at[pl.ds(0, RING * RING)]
            pltpu.make_async_copy(theirs, theirs, pair_recv.at[t, piece]).wait()
    for copy in sends:
        copy.wait_send()
    for copy in locals_:
        copy.wait()


def place_kernel(y_lo, y_hi, dx_all, grads, d_up, y_out, dx_out, d_wqkv, d_wout, d_wdown, d_wup, bounce, in_sem, out_sem, sem):
    rows, mid, _ = y_lo.shape
    n_qkv, n_o, n_dn = d_wqkv.shape[0], d_wout.shape[0], d_wdown.shape[0]
    bufs, per = bounce.shape[0], bounce.shape[1]
    count = rows // per
    loads = [pltpu.make_async_copy(y_hi.at[pl.ds(n * per, per)], bounce.at[n % bufs], in_sem.at[n % bufs]) for n in range(count)]
    stores = [pltpu.make_async_copy(bounce.at[n % bufs], y_out.at[pl.ds(n * per, per), pl.ds(mid, mid)], out_sem.at[n % bufs]) for n in range(count)]
    for n in range(min(bufs, count)):
        loads[n].start()
    direct = [(y_lo, y_out.at[:, pl.ds(0, mid)]), (dx_all, dx_out), (grads.at[pl.ds(0, n_qkv)], d_wqkv),
              (grads.at[pl.ds(n_qkv, n_o)], d_wout), (grads.at[pl.ds(n_qkv + n_o, n_dn)], d_wdown), (d_up, d_wup)]
    copies = [pltpu.make_async_copy(src, dst, sem.at[n]) for n, (src, dst) in enumerate(direct)]
    for copy in copies:
        copy.start()
    for n in range(count):
        loads[n].wait()
        stores[n].start()
        if n >= 1 and n - 1 + bufs < count:
            stores[n - 1].wait()
            loads[n - 1 + bufs].start()
    for n in range(max(0, count - bufs), count):
        stores[n].wait()
    for copy in copies:
        copy.wait()


def solution(mesh):
    devices = mesh.shape['model']
    assert devices == 2 * RING * RING and math.isqrt(devices // 2) == RING

    def body(x_in, seg_ids, ln_gain, w_qkv, w_out, w_up, w_down, dy_in):
        rows, seq_len, hidden = x_in.shape
        assert rows == devices
        wqkv = w_qkv.transpose(1, 2, 3, 0).reshape(-1, hidden)
        wo = w_out.reshape(-1, hidden)
        n_qkv, n_up, n_o, n_dn = wqkv.shape[0], w_up.shape[1], wo.shape[0], w_down.shape[0]
        n_in, n_out = n_qkv + n_up, n_o + n_dn
        bf16, f32 = jnp.bfloat16, jnp.float32
        vmem, anywhere = pl.BlockSpec(memory_space=pltpu.VMEM), pl.BlockSpec(memory_space=pl.ANY)
        dma = pltpu.SemaphoreType.DMA
        shape = jax.ShapeDtypeStruct
        mid = seq_len // 2
        y_own, dx_own, d_gain, g_own, g_sib, _ = pl.pallas_call(
            reduce_kernel,
            in_specs=[anywhere, anywhere, vmem, vmem] + [anywhere] * 4,
            out_specs=[anywhere, anywhere, vmem, anywhere, anywhere, anywhere],
            out_shape=[shape((seq_len, hidden), bf16), shape((seq_len, hidden), bf16), shape((1, hidden), f32),
                       shape((n_in + n_out, hidden), f32), shape((n_in + n_out, hidden), f32),
                       shape((2, RING, 2, seq_len, hidden), bf16)],
            scratch_shapes=[
                pltpu.VMEM((2 * n_in, hidden), bf16), pltpu.VMEM((2 * n_out, hidden), bf16), pltpu.VMEM((hidden, n_up), bf16),
                pltpu.VMEM((2 * n_in, hidden), f32), pltpu.VMEM((2 * n_out, hidden), f32),
                pltpu.VMEM((2, seq_len, hidden), bf16), pltpu.VMEM((2, seq_len, hidden), bf16),
                pltpu.VMEM((seq_len, hidden), bf16),
                pltpu.VMEM((2 * n_out, seq_len), bf16), pltpu.VMEM((2 * n_in, seq_len), bf16),
                pltpu.VMEM((SLOTS, 2, seq_len, hidden), bf16),
                pltpu.VMEM((2, RING + 1, 2, mid, hidden), bf16),
                pltpu.VMEM((2, 2, seq_len, hidden), bf16),
                pltpu.VMEM((2, 2, mid, hidden), bf16),
                dma((2, 2)), dma((4,)), dma((4,)), dma((4,)), dma((SLOTS, 2, 2)),
                dma((2, RING + 1, 2)), dma((2, RING + 1, 2, 2)), dma((2, 2)), dma((8,)),
            ],
            compiler_params=pltpu.CompilerParams(collective_id=0, has_side_effects=True, vmem_limit_bytes=VMEM_LIMIT),
            name="rows_reduce",
        )(x_in, dy_in, seg_ids, ln_gain.reshape(1, hidden), wqkv, w_up, wo, w_down)

        per_link = RING * RING - 1
        y_lo, y_hi, dx_all, _, d_gain, grads, d_up = pl.pallas_call(
            gather_kernel,
            in_specs=[anywhere, anywhere, vmem, anywhere, anywhere],
            out_specs=[vmem, anywhere, vmem, anywhere, vmem, vmem, vmem],
            out_shape=[pltpu.VMEM((rows, mid, hidden), bf16), shape((rows, mid, hidden), bf16), pltpu.VMEM((rows, seq_len, hidden), bf16),
                       shape(g_sib.shape, f32), shape((1, hidden), bf16),
                       pltpu.VMEM((n_qkv + n_out, hidden), bf16), pltpu.VMEM((hidden, n_up), bf16)],
            scratch_shapes=[
                pltpu.VMEM((3, RING, 1, hidden), f32), pltpu.VMEM((2, n_o, hidden), f32), pltpu.VMEM((2, n_up, min(hidden, 256)), f32),
                dma((4, per_link)), dma((4, per_link)), dma((2, 2 * RING * RING)), dma((2, 2)), dma((2, 2)), dma((2,)), dma((2,)),
                dma((3, 3)), dma((3, 3)),
            ],
            compiler_params=pltpu.CompilerParams(collective_id=1, has_side_effects=True, vmem_limit_bytes=6 * 2 ** 20),
            name="rows_gather",
        )(y_own, dx_own, d_gain, g_own, g_sib)

        bufs = 4
        fixed = lambda array: pltpu.with_memory_space_constraint(array, pltpu.VMEM)
        y_out, dx_out, d_wqkv, d_wout, d_wdown, d_wup = pl.pallas_call(
            place_kernel,
            in_specs=[vmem, anywhere, vmem, vmem, vmem],
            out_specs=[anywhere] * 6,
            out_shape=[shape(x_in.shape, bf16), shape(x_in.shape, bf16), shape(wqkv.shape, bf16), shape(wo.shape, bf16),
                       shape(w_down.shape, bf16), shape(w_up.shape, bf16)],
            scratch_shapes=[pltpu.VMEM((bufs, 2, mid, hidden), bf16), dma((bufs,)), dma((bufs,)), dma((6,))],
            compiler_params=pltpu.CompilerParams(vmem_limit_bytes=6 * 2 ** 20),
            name="rows_place",
        )(fixed(y_lo), pltpu.with_memory_space_constraint(y_hi, pltpu.HBM), fixed(dx_all), fixed(grads), fixed(d_up))
        d_wqkv = d_wqkv.reshape(w_qkv.shape[1:] + (hidden,)).transpose(3, 0, 1, 2)
        return y_out, dx_out, d_gain.reshape(hidden), d_wqkv, d_wout.reshape(w_out.shape), d_wup, d_wdown

    in_specs = (P('data'), P('data'), P(), P(None, 'model'), P('model'), P(None, 'model'), P('model'), P('data'))
    out_specs = (P('data'), P('data'), P('data'), P('data', 'model'), P(('data', 'model')), P('data', 'model'), P(('data', 'model')))
    return jax.shard_map(body, mesh=mesh, in_specs=in_specs, out_specs=out_specs, check_vma=False)
```

```python
import functools
import math

import jax
import jax.numpy as jnp
from jax import lax
from jax.experimental import pallas as pl
from jax.experimental.pallas import tpu as pltpu
from jax.sharding import PartitionSpec as P

LN_EPS = 1e-5
RING = 4
MESH = pl.DeviceIdType.MESH
NT = (((1,), (1,)), ((), ()))
NN = (((1,), (0,)), ((), ()))
TN = (((0,), (0,)), ((), ()))
ORDER = ((2, 2), (3, 2), (2, 1), (2, 3), (1, 2), (0, 2), (2, 0), (3, 3),
         (1, 1), (3, 1), (0, 3), (1, 3), (1, 0), (3, 0), (0, 1), (0, 0))
SLOT = (0, 1, 2, 3, 4, 0, 1, 2, 3, 4, 0, 1, 2, 3, 4, 1)
SLOTS = max(SLOT) + 1
EVENTS = (
    (((0, 0, 0, 1), (0, 0, 1, 1), (0, 1, 0, 1), (0, 1, 1, 1)), ()),
    (((1, 0, 0, 1), (1, 0, 1, 1), (1, 1, 0, 1)), ()),
    (((2, 0, 1, 1), (2, 1, 0, 1), (2, 1, 1, 1), (1, 1, 1, 1), (2, 0, 0, 1)), ()),
    (((3, 0, 0, 1), (3, 1, 0, 1), (3, 1, 1, 1), (3, 0, 1, 1)), ()),
    (((4, 0, 0, 1), (4, 0, 1, 1), (4, 1, 1, 1), (4, 1, 0, 1)), ()),
    (((5, 0, 0, 1), (5, 0, 1, 1)), ()),
    (((6, 1, 0, 1), (6, 1, 1, 1), (6, 0, 0, 1), (6, 0, 0, 2), (6, 0, 1, 1), (6, 0, 1, 2)), ((5, 1, 1, 1), (5, 1, 1, 2))),
    (((7, 0, 0, 1), (7, 1, 0, 1), (7, 0, 1, 1), (7, 1, 1, 1)), ((5, 1, 0, 1), (5, 1, 0, 2))),
    (((8, 0, 1, 1), (8, 1, 1, 1), (8, 1, 0, 1), (8, 0, 0, 1)), ()),
    (((9, 0, 1, 1), (9, 1, 0, 1), (9, 0, 0, 1), (9, 1, 1, 1)), ()),
    (((10, 0, 0, 1), (10, 0, 1, 1)), ()),
    (((11, 0, 0, 1), (11, 1, 1, 1), (11, 1, 0, 1), (11, 0, 1, 1)), ()),
    (((12, 1, 1, 1), (12, 1, 0, 1)), ()),
    (((13, 1, 0, 1), (13, 1, 1, 1), (13, 0, 1, 1), (13, 0, 1, 2)), ((10, 1, 1, 1), (10, 1, 1, 2))),
    (((14, 0, 1, 1), (14, 0, 0, 1), (14, 1, 0, 1), (14, 1, 0, 2), (13, 0, 0, 1), (13, 0, 0, 2), (14, 1, 1, 1), (14, 1, 1, 2), (10, 1, 0, 1), (10, 1, 0, 2)), ((12, 0, 0, 1), (12, 0, 0, 2))),
    ((), ((15, 0, 1, 1), (15, 1, 1, 1), (12, 0, 1, 1), (12, 0, 1, 2), (15, 0, 0, 1), (15, 1, 0, 1), (15, 0, 0, 2), (15, 1, 0, 2), (15, 1, 1, 2), (15, 0, 1, 2))),
)
VMEM_LIMIT = 60 * 2 ** 20


def dot(lhs, rhs, dims):
    return lax.dot_general(lhs, rhs, dims, preferred_element_type=jnp.float32)


def norm_rows(x_f32):
    mean_val = jnp.mean(x_f32, axis=-1, keepdims=True)
    centered = x_f32 - mean_val
    inv_std = lax.rsqrt(jnp.mean(centered * centered, axis=-1, keepdims=True) + LN_EPS)
    return centered * inv_std, inv_std


class Place:
    def __init__(self):
        me = lax.axis_index('model')
        self.core = me % 2
        self.x = (me // 2) % RING
        self.y = me // (2 * RING)
        self.me = me

    def index(self, d_y, d_x, core=None):
        core = self.core if core is None else core
        return (((self.y + d_y) % RING) * RING + (self.x + d_x) % RING) * 2 + core

    def peer(self, axis, offset):
        return self.index(offset % RING, 0) if axis == 'y' else self.index(0, offset % RING)

    def sibling(self):
        return self.index(0, 0, 1 - self.core)


def remote(src, dst, send_sem, recv_sem, device):
    return pltpu.make_async_remote_copy(src_ref=src, dst_ref=dst, send_sem=send_sem, recv_sem=recv_sem,
                                        device_id={'model': device}, device_id_type=MESH)


def enter(peers):
    barrier = pltpu.get_barrier_semaphore()
    for peer in peers:
        pl.semaphore_signal(barrier, inc=1, device_id={'model': peer}, device_id_type=MESH)
    pl.semaphore_wait(barrier, len(peers))


def pick(step, values):
    out = jnp.int32(0)
    for n, value in enumerate(values):
        out = jnp.where(step == n, value, out)
    return out


def add_into(dst, *sources):
    rows = dst.shape[0]
    tile = min(rows, 32)

    def tile_add(n, carry):
        at = pl.ds(pl.multiple_of(n * tile, tile), tile)
        total = dst[at, :].astype(jnp.float32)
        for source in sources:
            total += source[at, :].astype(jnp.float32)
        dst[at, :] = total.astype(dst.dtype)
        return carry

    lax.fori_loop(0, rows // tile, tile_add, 0)


def reduce_kernel(x_hbm, dy_hbm, seg_ref, gain_ref, wqkv_hbm, w1_hbm, wo_hbm, w2_hbm,
                  y_own, dx_own, dgain_ref, g_own, g_sib, full,
                  w_in, w_out, w1_raw, acc_in, acc_out, x_buf, dy_buf, a_scr, h_scr, d_scr, stage, half, last_full, tmp,
                  row_sem, w_sem, ws_sem, wr_sem, send_sem, half_sem, full_sem, tmp_sem, out_sem):
    place = Place()
    core = place.core
    _, seq_len, hidden = x_buf.shape
    mid = seq_len // 2
    n_qkv, n_up, n_o, n_dn = wqkv_hbm.shape[0], w1_hbm.shape[1], wo_hbm.shape[0], w2_hbm.shape[0]
    head_dim = n_o
    steps = len(ORDER)

    def row_of(step):
        d_y = pick(step, [o[0] for o in ORDER])
        d_x = pick(step, [o[1] for o in ORDER])
        return place.index(d_y, d_x)

    def row_copy(step, buf, n):
        return pltpu.make_async_copy((x_hbm, dy_hbm)[n].at[row_of(step)], (x_buf, dy_buf)[n].at[buf], row_sem.at[buf, n])

    def rows_at(ref, at, count):
        return ref.at[pl.ds(pl.multiple_of(at, 16), count)]

    up_spot = rows_at(w_in, 2 * n_qkv + core * n_up, n_up)
    spots = ((wqkv_hbm, rows_at(w_in, core * n_qkv, n_qkv)), (wo_hbm, rows_at(w_out, core * n_o, n_o)),
             (w2_hbm, rows_at(w_out, 2 * n_o + core * n_dn, n_dn)))

    gain = gain_ref[...].astype(jnp.float32)[None, :]
    sub = min(seq_len, 16)

    def norm_row(buf):
        for t in range(0, seq_len, sub):
            normed, _ = norm_rows(x_buf[buf, t:t + sub, :].astype(jnp.float32))
            a_scr[t:t + sub, :] = (normed * gain).astype(jnp.bfloat16)

    peers = [place.peer('x', 1), place.peer('x', -1), place.peer('y', 1), place.peer('y', -1), place.sibling()]
    barrier = pltpu.get_barrier_semaphore()
    for peer in peers:
        pl.semaphore_signal(barrier, inc=1, device_id={'model': peer}, device_id_type=MESH)
    raw = pltpu.make_async_copy(w1_hbm, w1_raw, w_sem.at[3])
    raw.start()
    for n in range(2):
        row_copy(0, 0, n).start()
    mine = [pltpu.make_async_copy(src, dst, w_sem.at[n]) for n, (src, dst) in enumerate(spots)]
    for copy in mine:
        copy.start()
    raw.wait()
    turn = min(hidden, 256)
    for h in range(0, hidden, turn):
        up_spot[:, h:h + turn] = w1_raw[h:h + turn, :].T
    pl.semaphore_wait(barrier, len(peers))
    swaps = [remote(src, dst, ws_sem.at[n], wr_sem.at[n], place.sibling()) for n, (src, dst) in enumerate(spots)]
    swaps.append(remote(up_spot, up_spot, ws_sem.at[3], wr_sem.at[3], place.sibling()))
    for n in (0, 3, 1, 2):
        swaps[n].start()
    row_copy(0, 0, 0).wait()
    norm_row(0)
    acc_in[...] = jnp.zeros_like(acc_in)
    acc_out[...] = jnp.zeros_like(acc_out)
    mine[0].wait()
    for n in (0, 3):
        swaps[n].wait()

    scale = head_dim ** -0.5
    cols_step = min(hidden, 512)

    def piece_of(ref, piece):
        return ref.at[pl.ds(piece * mid, mid)]

    def landed(ref, sem):
        pltpu.make_async_copy(ref, ref, sem).wait()

    def slot_sends(slot):
        return [pltpu.make_async_copy(piece_of(stage.at[slot, t], piece), piece_of(stage.at[slot, t], piece),
                                      send_sem.at[slot, t, piece]) for t in range(2) for piece in range(2)]

    def event(n, t, piece, ring):
        d_y, d_x = ORDER[n]
        first, second = (('x', d_x), ('y', d_y)) if t == 0 else (('y', d_y), ('x', d_x))
        (axis, offset), line = (first, second[1]) if ring == 1 else (second, RING)
        ahead, behind = place.peer(axis, 1), place.peer(axis, -1)
        spot = piece_of(stage.at[SLOT[n], t], piece)

        def arrival(side):
            return piece_of(last_full.at[t, side] if line == RING else full.at[t, line, side], piece)

        def send(dst, recv_sem, device):
            remote(spot, dst, send_sem.at[SLOT[n], t, piece], recv_sem, device).start()

        if offset == 2:
            send(half.at[t, line, piece], half_sem.at[t, line, piece], ahead if piece == 0 else behind)
        elif offset in (1, 3):
            side = 0 if offset == 1 else 1
            if side == piece:
                landed(half.at[t, line, piece], half_sem.at[t, line, piece])
                add_into(spot, half.at[t, line, piece])
            send(arrival(side), full_sem.at[t, line, side, piece], ahead if side == 0 else behind)
        elif line == RING:
            for side in range(2):
                landed(arrival(side), full_sem.at[t, line, side, piece])
            add_into(spot, arrival(0), arrival(1))
        else:
            loads = [pltpu.make_async_copy(arrival(side), tmp.at[piece, side], tmp_sem.at[piece, side]) for side in range(2)]
            for side in range(2):
                landed(arrival(side), full_sem.at[t, line, side, piece])
                loads[side].start()
            for load in loads:
                load.wait()
            add_into(spot, tmp.at[piece, 0], tmp.at[piece, 1])

    def grad_copies():
        copies = []
        for n, (side, dst) in enumerate(((core, g_own), (1 - core, g_sib))):
            to = 0
            for m, (acc, at, count) in enumerate(((acc_in, side * n_qkv, n_qkv), (acc_in, 2 * n_qkv + side * n_up, n_up),
                                                  (acc_out, side * n_o, n_o), (acc_out, 2 * n_o + side * n_dn, n_dn))):
                copies.append(pltpu.make_async_copy(rows_at(acc, at, count), dst.at[pl.ds(to, count)], out_sem.at[4 * n + m]))
                to += count
        return copies

    def grad_cols(buf, h):
        cols = slice(h, h + cols_step)
        acc_in[:, cols] += dot(d_scr[...], a_scr[:, cols], NN)
        acc_out[:, cols] += dot(h_scr[...], dy_buf[buf, :, cols], NN)

    def attend(head, qkv, d_attn, allowed):
        at = head * n_qkv
        query = qkv[at:at + head_dim]
        keys = qkv[at + head_dim:at + 2 * head_dim]
        values = qkv[at + 2 * head_dim:at + 3 * head_dim]
        d_o = d_attn[head * head_dim:(head + 1) * head_dim]
        scores = jnp.where(allowed, dot(keys, query, TN) * scale, -1e30)
        expd = jnp.exp(scores - jnp.max(scores, axis=0, keepdims=True))
        probs = expd / jnp.sum(expd, axis=0, keepdims=True)
        probs_b = probs.astype(jnp.bfloat16)
        h_scr[head * head_dim:(head + 1) * head_dim, :] = dot(values, probs_b, NN).astype(jnp.bfloat16)
        d_p = dot(values, d_o, TN)
        d_s = (probs * (d_p - jnp.sum(d_p * probs, axis=0, keepdims=True)) * scale).astype(jnp.bfloat16)
        d_scr[at:at + head_dim, :] = dot(keys, d_s, NN).astype(jnp.bfloat16)
        d_scr[at + head_dim:at + 2 * head_dim, :] = dot(query, d_s, NT).astype(jnp.bfloat16)
        d_scr[at + 2 * head_dim:at + 3 * head_dim, :] = dot(d_o, probs_b, NT).astype(jnp.bfloat16)

    def row_step(step, carry):
        buf = step % 2
        slot = pick(step, SLOT)
        tiles = range(0, hidden, cols_step)

        @pl.when(step > 0)
        def _():
            row_copy(step, buf, 0).wait()
            norm_row(buf)

        row_copy(step, buf, 1).wait()

        @pl.when(step + 1 < steps)
        def _():
            for n in range(2):
                row_copy(step + 1, 1 - buf, n).start()

        @pl.when(step == 0)
        def _():
            for copy in mine[1:] + swaps[1:3]:
                copy.wait()

        proj = dot(w_in[...], a_scr[...], NT)
        d_proj = dot(w_out[...], dy_buf[buf], NT).astype(jnp.bfloat16)
        qkv = proj[:2 * n_qkv].astype(jnp.bfloat16)
        up = proj[2 * n_qkv:].astype(jnp.bfloat16).astype(jnp.float32)
        d_attn = d_proj[:2 * n_o]
        d_hid = d_proj[2 * n_o:].astype(jnp.float32)
        cdf = 0.5 * (1.0 + lax.erf(up * (0.5 ** 0.5)))
        h_scr[2 * n_o:, :] = (up * cdf).astype(jnp.bfloat16)
        slope = cdf + up * (jnp.exp(-0.5 * up * up) * 0.3989422804014327)
        d_scr[2 * n_qkv:, :] = (d_hid * slope).astype(jnp.bfloat16)

        seg_row = seg_ref[pl.ds(row_of(step), 1), :]
        classes = lax.broadcasted_iota(jnp.int32, (16, seq_len), 0)
        one_hot = (classes == jnp.broadcast_to(seg_row, (16, seq_len))).astype(jnp.bfloat16)
        same = dot(one_hot, one_hot, TN) > 0.5
        key_id = lax.broadcasted_iota(jnp.int32, (seq_len, seq_len), 0)
        query_id = lax.broadcasted_iota(jnp.int32, (seq_len, seq_len), 1)
        allowed = (key_id <= query_id) & same
        for head in range(2):
            attend(head, qkv, d_attn, allowed)

        @pl.when(pick(step, [int(SLOT[n] in SLOT[:n]) for n in range(steps)]) == 1)
        def _():
            for copy in slot_sends(slot):
                copy.wait()

        for h in tiles:
            cols = slice(h, h + cols_step)
            stage[slot, 0, :, cols] = dot(h_scr[...], w_out[:, cols], TN).astype(jnp.bfloat16)
            stage[slot, 1, :, cols] = dot(d_scr[...], w_in[:, cols], TN).astype(jnp.bfloat16)

        def pass_on(when):
            for n in range(steps - 1):
                if EVENTS[n][when]:
                    @pl.when(step == n)
                    def _():
                        for work in EVENTS[n][when]:
                            event(*work)

        pass_on(0)
        for h in tiles:
            grad_cols(buf, h)
        pass_on(1)
        return carry

    lax.fori_loop(0, steps, row_step, 0)
    last, buf = SLOT[-1], (steps - 1) % 2
    for copy in grad_copies():
        copy.start()
    dgain_ref[...] = jnp.zeros_like(dgain_ref)
    fine = min(mid, 32)

    def finish(piece):
        def tile(n, d_gain):
            at = pl.ds(pl.multiple_of(piece * mid + n * fine, fine), fine)
            x_f32 = x_buf[buf, at, :].astype(jnp.float32)
            normed, inv_std = norm_rows(x_f32)
            grad = stage[last, 1, at, :].astype(jnp.float32)
            stage[last, 0, at, :] = (x_f32 + stage[last, 0, at, :].astype(jnp.float32)).astype(jnp.bfloat16)
            d_hat = grad * gain
            d_x = inv_std * (d_hat - jnp.mean(d_hat, axis=-1, keepdims=True) - normed * jnp.mean(d_hat * normed, axis=-1, keepdims=True))
            stage[last, 1, at, :] = (dy_buf[buf, at, :].astype(jnp.float32) + d_x).astype(jnp.bfloat16)
            return d_gain + jnp.sum(grad * normed, axis=0, keepdims=True)

        dgain_ref[...] += lax.fori_loop(0, mid // fine, tile, jnp.zeros((1, hidden), jnp.float32))
        for t, dst in ((0, y_own), (1, dx_own)):
            ends.append(pltpu.make_async_copy(piece_of(stage.at[last, t], piece), piece_of(dst, piece), tmp_sem.at[piece, t]))
            ends[-1].start()

    ends = []
    ended = {0: 0, 1: 0}
    for work in EVENTS[-1][1]:
        event(*work)
        n, _, piece, ring = work
        if n == steps - 1 and ring == 2:
            ended[piece] += 1
            if ended[piece] == 2:
                finish(piece)
    for slot in range(SLOTS):
        if slot != last:
            for copy in slot_sends(slot):
                copy.wait()
    for copy in ends + grad_copies():
        copy.wait()


def gather_kernel(y_own, dx_own, dgain_ref, g_own, g_sib, y_lo, y_hi, dx_all, g_recv, dgain_out, grads, d_up,
                  gain_scr, g_buf, t_buf, send_sem, link_sem, pair_sem, pair_recv, own_sem, g_sem, gb_sem, dg_send, dg_recv):
    place = Place()
    _, seq_len, hidden = dx_all.shape
    mid = seq_len // 2
    links = (('x', 1), ('x', -1), ('y', 1), ('y', -1))
    enter([place.peer(a, o) for a in ('x', 'y') for o in (1, 2, 3)] + [place.sibling()])

    issued = {link: [] for link in links}
    sends = []

    def row_index(t, d_1, d_2):
        return place.index(d_1 % RING, d_2 % RING) if t == 0 else place.index(d_2 % RING, d_1 % RING)

    def spot_of(t, row, piece):
        if t == 1:
            return dx_all.at[row, pl.ds(piece * mid, mid)]
        return (y_lo, y_hi)[piece].at[row]

    def source(t, d_1, d_2, piece):
        if (d_1, d_2) == (0, 0):
            return (y_own, dx_own)[t].at[pl.ds(piece * mid, mid)]
        return spot_of(t, row_index(t, d_1, d_2), piece)

    def issue(link, t, d_1, d_2, piece):
        n = len(issued[link])
        which = links.index(link)
        copy = remote(source(t, d_1, d_2, piece), spot_of(t, row_index(t, d_1, d_2), piece),
                      send_sem.at[which, n], link_sem.at[which, n], place.peer(*link))
        copy.start()
        sends.append(copy)
        issued[link].append((t, d_1, d_2, piece))

    def pair(t, d_1, d_2, piece):
        slot = ((d_1 % RING) * RING + d_2 % RING) * 2 + piece
        copy = remote(source(t, d_1, d_2, piece), spot_of(t, row_index(t, d_1, d_2), piece),
                      pair_sem.at[t, slot], pair_recv.at[t, piece], place.sibling())
        copy.start()
        sends.append(copy)

    axes = (('y', 'x'), ('x', 'y'))
    for ring in range(2):
        for piece in range(2):
            for t in range(2):
                for way in (1, -1):
                    issue((axes[t][ring], way), t, 0, 0, piece)
    locals_ = []
    for t in range(2):
        for piece in range(2):
            pair(t, 0, 0, piece)
            copy = pltpu.make_async_copy(source(t, 0, 0, piece), spot_of(t, place.me, piece), own_sem.at[t, piece])
            copy.start()
            locals_.append(copy)
    g_copy = remote(g_sib, g_recv, g_sem.at[0], g_sem.at[1], place.sibling())
    g_copy.start()

    total = dgain_ref[...]
    for n, (axis, offsets) in enumerate((('core', (1,)), ('x', (1, 2, 3)), ('y', (1, 2, 3)))):
        spot = {'core': place.core, 'x': place.x, 'y': place.y}[axis]
        gain_scr[n, spot] = total
        copies = []
        for m, offset in enumerate(offsets):
            device = place.sibling() if axis == 'core' else place.peer(axis, offset)
            copies.append(remote(gain_scr.at[n, spot], gain_scr.at[n, spot], dg_send.at[n, m], dg_recv.at[n, m], device))
        for copy in copies:
            copy.start()
        for copy in copies:
            copy.wait()
        total = gain_scr[n, 0]
        for m in range(1, len(offsets) + 1):
            total = total + gain_scr[n, m]
    dgain_out[...] = jnp.sum(total, axis=0).astype(dgain_out.dtype)

    tile, turn = g_buf.shape[1], t_buf.shape[2]
    n_up = d_up.shape[1]
    n_qkv = 3 * tile

    def grad_tile(at, to):
        loads = [pltpu.make_async_copy(g.at[pl.ds(at, tile)], g_buf.at[n], gb_sem.at[n]) for n, g in enumerate((g_own, g_recv))]
        for load in loads:
            load.start()
        for load in loads:
            load.wait()
        grads[to:to + tile, :] = (g_buf[0] + g_buf[1]).astype(grads.dtype)

    def up_tile(h):
        loads = [pltpu.make_async_copy(g.at[pl.ds(n_qkv, n_up), pl.ds(h, turn)], t_buf.at[n], gb_sem.at[n]) for n, g in enumerate((g_own, g_recv))]
        for load in loads:
            load.start()
        for load in loads:
            load.wait()
        d_up[h:h + turn, :] = (t_buf[0] + t_buf[1]).T.astype(d_up.dtype)

    jobs = [functools.partial(grad_tile, at, at) for at in range(0, n_qkv, tile)]
    jobs += [functools.partial(grad_tile, at, at - n_up) for at in range(n_qkv + n_up, g_own.shape[0], tile)]
    jobs += [functools.partial(up_tile, h) for h in range(0, hidden, turn)]

    rounds = RING * RING - 1
    for n in range(rounds):
        for link in links:
            t, d_1, d_2, piece = issued[link][n]
            axis, way = link
            on_first = axis == axes[t][0]
            d_1, d_2 = (d_1 - way, d_2) if on_first else (d_1, d_2 - way)
            spot = spot_of(t, row_index(t, d_1, d_2), piece)
            pltpu.make_async_copy(spot, spot, link_sem.at[links.index(link), n]).wait()
            along = d_1 if on_first else d_2
            if abs(along) == 1 and piece == (0 if way == 1 else 1):
                issue(link, t, d_1, d_2, piece)
            if on_first:
                for other in (1, -1):
                    issue((axes[t][1], other), t, d_1, d_2, piece)
            pair(t, d_1, d_2, piece)
        if n == 2:
            g_copy.wait()
        if n >= 2:
            for job in jobs[2 * (n - 2):2 * (n - 1)]:
                job()

    for t in range(2):
        for piece in range(2):
            theirs = dx_all.at[pl.ds(0, RING * RING), pl.ds(piece * mid, mid)] if t else (y_lo, y_hi)[piece].at[pl.ds(0, RING * RING)]
            pltpu.make_async_copy(theirs, theirs, pair_recv.at[t, piece]).wait()
    for copy in sends:
        copy.wait_send()
    for copy in locals_:
        copy.wait()


def place_kernel(y_lo, y_hi, dx_all, grads, d_up, dgain, y_out, dx_out, d_wqkv, d_wout, d_wdown, d_wup, dgain_out, bounce, in_sem, out_sem, sem):
    rows, mid, _ = y_lo.shape
    n_qkv, n_o, n_dn = d_wqkv.shape[0], d_wout.shape[0], d_wdown.shape[0]
    bufs, per = bounce.shape[0], bounce.shape[1]
    count = rows // per
    loads = [pltpu.make_async_copy(y_hi.at[pl.ds(n * per, per)], bounce.at[n % bufs], in_sem.at[n % bufs]) for n in range(count)]
    stores = [pltpu.make_async_copy(bounce.at[n % bufs], y_out.at[pl.ds(n * per, per), pl.ds(mid, mid)], out_sem.at[n % bufs]) for n in range(count)]
    for n in range(min(bufs, count)):
        loads[n].start()
    direct = [(y_lo, y_out.at[:, pl.ds(0, mid)]), (dx_all, dx_out), (grads.at[pl.ds(0, n_qkv)], d_wqkv),
              (grads.at[pl.ds(n_qkv, n_o)], d_wout), (grads.at[pl.ds(n_qkv + n_o, n_dn)], d_wdown), (d_up, d_wup)]
    copies = [pltpu.make_async_copy(src, dst, sem.at[n]) for n, (src, dst) in enumerate(direct)]
    for copy in copies:
        copy.start()
    dgain_out[...] = dgain[...]
    for n in range(count):
        loads[n].wait()
        stores[n].start()
        if n >= 1 and n - 1 + bufs < count:
            stores[n - 1].wait()
            loads[n - 1 + bufs].start()
    for n in range(max(0, count - bufs), count):
        stores[n].wait()
    for copy in copies:
        copy.wait()


def solution(mesh):
    devices = mesh.shape['model']
    assert devices == 2 * RING * RING and math.isqrt(devices // 2) == RING

    def body(x_in, seg_ids, ln_gain, w_qkv, w_out, w_up, w_down, dy_in):
        rows, seq_len, hidden = x_in.shape
        assert rows == devices
        wqkv = w_qkv.transpose(1, 2, 3, 0).reshape(-1, hidden)
        wo = w_out.reshape(-1, hidden)
        n_qkv, n_up, n_o, n_dn = wqkv.shape[0], w_up.shape[1], wo.shape[0], w_down.shape[0]
        n_in, n_out = n_qkv + n_up, n_o + n_dn
        bf16, f32 = jnp.bfloat16, jnp.float32
        vmem, anywhere = pl.BlockSpec(memory_space=pltpu.VMEM), pl.BlockSpec(memory_space=pl.ANY)
        dma = pltpu.SemaphoreType.DMA
        shape = jax.ShapeDtypeStruct
        mid = seq_len // 2
        fixed = lambda array: pltpu.with_memory_space_constraint(array, pltpu.VMEM)
        y_own, dx_own, d_gain, g_own, g_sib, _ = pl.pallas_call(
            reduce_kernel,
            in_specs=[anywhere, anywhere, vmem, vmem] + [anywhere] * 4,
            out_specs=[anywhere, anywhere, vmem, anywhere, anywhere, anywhere],
            out_shape=[shape((seq_len, hidden), bf16), shape((seq_len, hidden), bf16), shape((1, hidden), f32),
                       shape((n_in + n_out, hidden), f32), shape((n_in + n_out, hidden), f32),
                       shape((2, RING, 2, seq_len, hidden), bf16)],
            scratch_shapes=[
                pltpu.VMEM((2 * n_in, hidden), bf16), pltpu.VMEM((2 * n_out, hidden), bf16), pltpu.VMEM((hidden, n_up), bf16),
                pltpu.VMEM((2 * n_in, hidden), f32), pltpu.VMEM((2 * n_out, hidden), f32),
                pltpu.VMEM((2, seq_len, hidden), bf16), pltpu.VMEM((2, seq_len, hidden), bf16),
                pltpu.VMEM((seq_len, hidden), bf16),
                pltpu.VMEM((2 * n_out, seq_len), bf16), pltpu.VMEM((2 * n_in, seq_len), bf16),
                pltpu.VMEM((SLOTS, 2, seq_len, hidden), bf16),
                pltpu.VMEM((2, RING + 1, 2, mid, hidden), bf16),
                pltpu.VMEM((2, 2, seq_len, hidden), bf16),
                pltpu.VMEM((2, 2, mid, hidden), bf16),
                dma((2, 2)), dma((4,)), dma((4,)), dma((4,)), dma((SLOTS, 2, 2)),
                dma((2, RING + 1, 2)), dma((2, RING + 1, 2, 2)), dma((2, 2)), dma((8,)),
            ],
            compiler_params=pltpu.CompilerParams(collective_id=0, has_side_effects=True, vmem_limit_bytes=VMEM_LIMIT),
            name="rows_reduce",
        )(x_in, dy_in, seg_ids, ln_gain, wqkv, w_up, wo, w_down)

        per_link = RING * RING - 1
        y_lo, y_hi, dx_all, _, d_gain, grads, d_up = pl.pallas_call(
            gather_kernel,
            in_specs=[anywhere, anywhere, vmem, anywhere, anywhere],
            out_specs=[vmem, anywhere, vmem, anywhere, vmem, vmem, vmem],
            out_shape=[pltpu.VMEM((rows, mid, hidden), bf16), shape((rows, mid, hidden), bf16), pltpu.VMEM((rows, seq_len, hidden), bf16),
                       shape(g_sib.shape, f32), pltpu.VMEM((hidden,), bf16),
                       pltpu.VMEM((n_qkv + n_out, hidden), bf16), pltpu.VMEM((hidden, n_up), bf16)],
            scratch_shapes=[
                pltpu.VMEM((3, RING, 1, hidden), f32), pltpu.VMEM((2, n_o, hidden), f32), pltpu.VMEM((2, n_up, min(hidden, 256)), f32),
                dma((4, per_link)), dma((4, per_link)), dma((2, 2 * RING * RING)), dma((2, 2)), dma((2, 2)), dma((2,)), dma((2,)),
                dma((3, 3)), dma((3, 3)),
            ],
            compiler_params=pltpu.CompilerParams(collective_id=1, has_side_effects=True, vmem_limit_bytes=6 * 2 ** 20),
            name="rows_gather",
        )(y_own, dx_own, d_gain, g_own, g_sib)

        bufs = 4
        y_out, dx_out, d_wqkv, d_wout, d_wdown, d_wup, d_gain = pl.pallas_call(
            place_kernel,
            in_specs=[vmem, anywhere, vmem, vmem, vmem, vmem],
            out_specs=[anywhere] * 6 + [vmem],
            out_shape=[shape(x_in.shape, bf16), shape(x_in.shape, bf16), shape(wqkv.shape, bf16), shape(wo.shape, bf16),
                       shape(w_down.shape, bf16), shape(w_up.shape, bf16), shape((hidden,), bf16)],
            scratch_shapes=[pltpu.VMEM((bufs, 2, mid, hidden), bf16), dma((bufs,)), dma((bufs,)), dma((6,))],
            compiler_params=pltpu.CompilerParams(vmem_limit_bytes=6 * 2 ** 20),
            name="rows_place",
        )(fixed(y_lo), pltpu.with_memory_space_constraint(y_hi, pltpu.HBM), fixed(dx_all), fixed(grads), fixed(d_up), fixed(d_gain))
        d_wqkv = d_wqkv.reshape(w_qkv.shape[1:] + (hidden,)).transpose(3, 0, 1, 2)
        return y_out, dx_out, d_gain, d_wqkv, d_wout.reshape(w_out.shape), d_wup, d_wdown

    in_specs = (P('data'), P('data'), P(), P(None, 'model'), P('model'), P(None, 'model'), P('model'), P('data'))
    out_specs = (P('data'), P('data'), P('data'), P('data', 'model'), P(('data', 'model')), P('data', 'model'), P(('data', 'model')))
    return jax.shard_map(body, mesh=mesh, in_specs=in_specs, out_specs=out_specs, check_vma=False)
```

```python
import jax
import jax.numpy as jnp
from jax import lax
from jax.experimental import pallas as pl
from jax.experimental.pallas import tpu as pltpu
from jax.sharding import PartitionSpec as P

LN_EPS = 1e-5
RING = 4
MESH = pl.DeviceIdType.MESH
NT = (((1,), (1,)), ((), ()))
NN = (((1,), (0,)), ((), ()))
TN = (((0,), (0,)), ((), ()))
ORDER = ((2, 2), (1, 2), (2, 3), (3, 2), (1, 1), (3, 3), (2, 1), (2, 0),
         (0, 2), (3, 1), (1, 3), (3, 0), (0, 3), (1, 0), (0, 1), (0, 0))
SLOT = (0, 1, 2, 3, 4, 0, 1, 3, 2, 0, 1, 4, 2, 3, 1, 0)
SLOTS = max(SLOT) + 1
EVENTS = (
    ((0, 0, 0, 1), (0, 0, 1, 1), (0, 1, 0, 1), (0, 1, 1, 1)),
    ((1, 0, 0, 1), (1, 0, 1, 1), (1, 1, 1, 1)),
    ((2, 0, 0, 1), (2, 1, 0, 1), (2, 1, 1, 1)),
    ((3, 0, 0, 1), (3, 0, 1, 1), (3, 1, 0, 1), (1, 1, 0, 1), (2, 0, 1, 1), (3, 1, 1, 1)),
    ((4, 0, 1, 1), (4, 1, 1, 1), (4, 0, 0, 1)),
    ((5, 0, 0, 1), (5, 1, 0, 1), (5, 1, 1, 1)),
    ((6, 0, 1, 1), (6, 1, 0, 1), (6, 1, 1, 1), (6, 0, 0, 1), (5, 0, 1, 1)),
    ((7, 1, 0, 1), (7, 1, 1, 1)),
    ((8, 0, 0, 1), (8, 0, 1, 1), (8, 1, 0, 1), (8, 1, 0, 2), (8, 1, 1, 1), (8, 1, 1, 2), (4, 1, 0, 1), (7, 0, 1, 1), (7, 0, 1, 2)),
    ((9, 0, 1, 1), (9, 1, 0, 1), (9, 0, 0, 1), (7, 0, 0, 1), (7, 0, 0, 2), (9, 1, 1, 1)),
    ((10, 0, 0, 1), (10, 1, 1, 1), (10, 0, 1, 1), (10, 1, 0, 1)),
    ((11, 1, 0, 1), (11, 1, 1, 1)),
    ((12, 0, 0, 1), (12, 0, 1, 1)),
    ((13, 1, 1, 1), (13, 1, 0, 1), (11, 0, 1, 1), (11, 0, 1, 2), (12, 1, 1, 1), (12, 1, 1, 2), (13, 0, 0, 1), (13, 0, 0, 2)),
    ((14, 0, 1, 1), (14, 0, 0, 1), (14, 1, 0, 1), (14, 1, 0, 2), (11, 0, 0, 1), (11, 0, 0, 2), (12, 1, 0, 1), (12, 1, 0, 2), (13, 0, 1, 1), (13, 0, 1, 2), (14, 1, 1, 1), (14, 1, 1, 2)),
    ((15, 0, 1, 1), (15, 1, 0, 1), (15, 1, 1, 1), (15, 0, 0, 1), (15, 0, 1, 2), (15, 1, 0, 2), (15, 0, 0, 2), (15, 1, 1, 2)),
)
VMEM_LIMIT = 60 * 2 ** 20
LANDING_LIMIT = 8 * 2 ** 20


def dot(lhs, rhs, dims):
    return lax.dot_general(lhs, rhs, dims, preferred_element_type=jnp.float32)


def norm_rows(x_f32):
    mean_val = jnp.mean(x_f32, axis=-1, keepdims=True)
    centered = x_f32 - mean_val
    inv_std = lax.rsqrt(jnp.mean(centered * centered, axis=-1, keepdims=True) + LN_EPS)
    return centered * inv_std, inv_std


class Place:
    def __init__(self):
        me = lax.axis_index('model')
        self.core = me % 2
        self.x = (me // 2) % RING
        self.y = me // (2 * RING)
        self.me = me

    def index(self, d_y, d_x, core=None):
        core = self.core if core is None else core
        return (((self.y + d_y) % RING) * RING + (self.x + d_x) % RING) * 2 + core

    def peer(self, axis, offset):
        return self.index(offset % RING, 0) if axis == 'y' else self.index(0, offset % RING)

    def sibling(self):
        return self.index(0, 0, 1 - self.core)


def remote(src, dst, send_sem, recv_sem, device):
    return pltpu.make_async_remote_copy(src_ref=src, dst_ref=dst, send_sem=send_sem, recv_sem=recv_sem,
                                        device_id={'model': device}, device_id_type=MESH)


def greet(peers):
    barrier = pltpu.get_barrier_semaphore()
    for peer in peers:
        pl.semaphore_signal(barrier, inc=1, device_id={'model': peer}, device_id_type=MESH)
    return barrier


def pick(step, values):
    out = jnp.int32(0)
    for n, value in enumerate(values):
        out = jnp.where(step == n, value, out)
    return out


def rows_at(ref, at, count):
    return ref.at[pl.ds(pl.multiple_of(at, 16), count)]


def landed(ref, sem):
    pltpu.make_async_copy(ref, ref, sem).wait()


def add_into(dst, *sources):
    rows = dst.shape[0]
    tile = min(rows, 32)

    def tile_add(n, carry):
        at = pl.ds(pl.multiple_of(n * tile, tile), tile)
        total = dst[at, :].astype(jnp.float32)
        for source in sources:
            total += source[at, :].astype(jnp.float32)
        dst[at, :] = total.astype(dst.dtype)
        return carry

    lax.fori_loop(0, rows // tile, tile_add, 0)


def reduce_kernel(x_hbm, dy_hbm, seg_ref, gain_ref, wqkv_hbm, w1_hbm, wo_hbm, w2_hbm,
                  y_own, dx_own, dgain_ref, a_all, hd_all,
                  w_in, w_out, w1_raw, x_buf, dy_buf, a_scr, hd_scr, stage, half, full,
                  row_sem, w_sem, ws_sem, wr_sem, send_sem, half_sem, full_sem, end_sem, save_sem):
    place = Place()
    core = place.core
    _, seq_len, hidden = x_buf.shape
    mid = seq_len // 2
    n_qkv, n_up, n_o, n_dn = wqkv_hbm.shape[0], w1_hbm.shape[1], wo_hbm.shape[0], w2_hbm.shape[0]
    n_d = 2 * (n_qkv + n_up)
    steps = len(ORDER)

    def row_of(step):
        return place.index(pick(step, [o[0] for o in ORDER]), pick(step, [o[1] for o in ORDER]))

    def row_copy(step, buf, n):
        return pltpu.make_async_copy((x_hbm, dy_hbm)[n].at[row_of(step)], (x_buf, dy_buf)[n].at[buf], row_sem.at[buf, n])

    def save(step, n):
        return pltpu.make_async_copy((a_scr, hd_scr)[n], (a_all, hd_all)[n].at[row_of(step) // 2], save_sem.at[n])

    up_spot = rows_at(w_in, 2 * n_qkv + core * n_up, n_up)
    spots = ((wqkv_hbm, rows_at(w_in, core * n_qkv, n_qkv)), (wo_hbm, rows_at(w_out, core * n_o, n_o)),
             (w2_hbm, rows_at(w_out, 2 * n_o + core * n_dn, n_dn)))

    gain = gain_ref[...].astype(jnp.float32)[None, :]
    sub = min(seq_len, 16)

    def norm_row(buf):
        for t in range(0, seq_len, sub):
            normed, _ = norm_rows(x_buf[buf, t:t + sub, :].astype(jnp.float32))
            a_scr[t:t + sub, :] = (normed * gain).astype(jnp.bfloat16)

    peers = [place.peer('x', 1), place.peer('x', -1), place.peer('y', 1), place.peer('y', -1), place.sibling()]
    barrier = greet(peers)
    raw = pltpu.make_async_copy(w1_hbm, w1_raw, w_sem.at[3])
    raw.start()
    for n in range(2):
        row_copy(0, 0, n).start()
    mine = [pltpu.make_async_copy(src, dst, w_sem.at[n]) for n, (src, dst) in enumerate(spots)]
    for copy in mine:
        copy.start()
    raw.wait()
    turn = min(hidden, 256)
    for h in range(0, hidden, turn):
        up_spot[:, h:h + turn] = w1_raw[h:h + turn, :].T
    pl.semaphore_wait(barrier, len(peers))
    swaps = [remote(src, dst, ws_sem.at[n], wr_sem.at[n], place.sibling()) for n, (src, dst) in enumerate(spots)]
    swaps.append(remote(up_spot, up_spot, ws_sem.at[3], wr_sem.at[3], place.sibling()))
    for n in (0, 3, 1, 2):
        swaps[n].start()
    row_copy(0, 0, 0).wait()
    norm_row(0)
    mine[0].wait()
    for n in (0, 3):
        swaps[n].wait()

    scale = n_o ** -0.5
    cols_step = min(hidden, 512)

    def piece_of(ref, piece):
        return ref.at[pl.ds(piece * mid, mid)]

    def slot_sends(slot):
        return [pltpu.make_async_copy(piece_of(stage.at[slot, t], piece), piece_of(stage.at[slot, t], piece),
                                      send_sem.at[slot, t, piece]) for t in range(2) for piece in range(2)]

    def event(n, t, piece, ring):
        d_y, d_x = ORDER[n]
        first, second = (('x', d_x), ('y', d_y)) if t == 0 else (('y', d_y), ('x', d_x))
        (axis, offset), line = (first, second[1]) if ring == 1 else (second, RING)
        ahead, behind = place.peer(axis, 1), place.peer(axis, -1)
        spot = piece_of(stage.at[SLOT[n], t], piece)

        def send(dst, recv_sem, device):
            remote(spot, dst, send_sem.at[SLOT[n], t, piece], recv_sem, device).start()

        if offset == 2:
            send(half.at[t, line, piece], half_sem.at[t, line, piece], ahead if piece == 0 else behind)
        elif offset in (1, 3):
            side = 0 if offset == 1 else 1
            if side == piece:
                landed(half.at[t, line, piece], half_sem.at[t, line, piece])
                add_into(spot, half.at[t, line, piece])
            send(piece_of(full.at[t, line, side], piece), full_sem.at[t, line, side, piece], ahead if side == 0 else behind)
        else:
            came = [piece_of(full.at[t, line, side], piece) for side in range(2)]
            for side in range(2):
                landed(came[side], full_sem.at[t, line, side, piece])
            add_into(spot, *came)

    def attend(head, qkv, d_attn, allowed):
        at = head * n_qkv
        query, keys, values = qkv[at:at + n_o], qkv[at + n_o:at + 2 * n_o], qkv[at + 2 * n_o:at + 3 * n_o]
        d_o = d_attn[head * n_o:(head + 1) * n_o]
        scores = jnp.where(allowed, dot(keys, query, TN) * scale, -1e30)
        expd = jnp.exp(scores - jnp.max(scores, axis=0, keepdims=True))
        probs = expd / jnp.sum(expd, axis=0, keepdims=True)
        probs_b = probs.astype(jnp.bfloat16)
        hd_scr[n_d + head * n_o:n_d + (head + 1) * n_o, :] = dot(values, probs_b, NN).astype(jnp.bfloat16)
        d_p = dot(values, d_o, TN)
        d_s = (probs * (d_p - jnp.sum(d_p * probs, axis=0, keepdims=True)) * scale).astype(jnp.bfloat16)
        hd_scr[at:at + n_o, :] = dot(keys, d_s, NN).astype(jnp.bfloat16)
        hd_scr[at + n_o:at + 2 * n_o, :] = dot(query, d_s, NT).astype(jnp.bfloat16)
        hd_scr[at + 2 * n_o:at + 3 * n_o, :] = dot(d_o, probs_b, NT).astype(jnp.bfloat16)

    def row_step(step, carry):
        buf = step % 2
        slot = pick(step, SLOT)

        @pl.when(step > 0)
        def _():
            for n in range(2):
                save(step - 1, n).wait()
            row_copy(step, buf, 0).wait()
            norm_row(buf)

        row_copy(step, buf, 1).wait()
        save(step, 0).start()

        @pl.when(step + 1 < steps)
        def _():
            for n in range(2):
                row_copy(step + 1, 1 - buf, n).start()

        @pl.when(step == 0)
        def _():
            for copy in mine[1:] + swaps[1:3]:
                copy.wait()

        proj = dot(w_in[...], a_scr[...], NT)
        d_proj = dot(w_out[...], dy_buf[buf], NT).astype(jnp.bfloat16)
        qkv = proj[:2 * n_qkv].astype(jnp.bfloat16)
        up = proj[2 * n_qkv:].astype(jnp.bfloat16).astype(jnp.float32)
        d_attn = d_proj[:2 * n_o]
        d_hid = d_proj[2 * n_o:].astype(jnp.float32)
        cdf = 0.5 * (1.0 + lax.erf(up * (0.5 ** 0.5)))
        hd_scr[n_d + 2 * n_o:, :] = (up * cdf).astype(jnp.bfloat16)
        slope = cdf + up * (jnp.exp(-0.5 * up * up) * 0.3989422804014327)
        hd_scr[2 * n_qkv:n_d, :] = (d_hid * slope).astype(jnp.bfloat16)

        seg_row = seg_ref[pl.ds(row_of(step), 1), :]
        classes = lax.broadcasted_iota(jnp.int32, (16, seq_len), 0)
        one_hot = (classes == jnp.broadcast_to(seg_row, (16, seq_len))).astype(jnp.bfloat16)
        same = dot(one_hot, one_hot, TN) > 0.5
        key_id = lax.broadcasted_iota(jnp.int32, (seq_len, seq_len), 0)
        query_id = lax.broadcasted_iota(jnp.int32, (seq_len, seq_len), 1)
        allowed = (key_id <= query_id) & same
        for head in range(2):
            attend(head, qkv, d_attn, allowed)
        save(step, 1).start()

        @pl.when(pick(step, [int(SLOT[n] in SLOT[:n]) for n in range(steps)]) == 1)
        def _():
            for copy in slot_sends(slot):
                copy.wait()

        for h in range(0, hidden, cols_step):
            cols = slice(h, h + cols_step)
            stage[slot, 0, :, cols] = dot(hd_scr[n_d:, :], w_out[:, cols], TN).astype(jnp.bfloat16)
            stage[slot, 1, :, cols] = dot(hd_scr[:n_d, :], w_in[:, cols], TN).astype(jnp.bfloat16)

        for n in range(steps - 1):
            @pl.when(step == n)
            def _():
                for work in EVENTS[n]:
                    event(*work)
        return carry

    lax.fori_loop(0, steps, row_step, 0)
    last, buf = SLOT[-1], (steps - 1) % 2
    dgain_ref[...] = jnp.zeros_like(dgain_ref)
    fine = min(mid, 32)

    def finish(piece):
        def tile(n, d_gain):
            at = pl.ds(pl.multiple_of(piece * mid + n * fine, fine), fine)
            x_f32 = x_buf[buf, at, :].astype(jnp.float32)
            normed, inv_std = norm_rows(x_f32)
            grad = stage[last, 1, at, :].astype(jnp.float32)
            stage[last, 0, at, :] = (x_f32 + stage[last, 0, at, :].astype(jnp.float32)).astype(jnp.bfloat16)
            d_hat = grad * gain
            d_x = inv_std * (d_hat - jnp.mean(d_hat, axis=-1, keepdims=True) - normed * jnp.mean(d_hat * normed, axis=-1, keepdims=True))
            stage[last, 1, at, :] = (dy_buf[buf, at, :].astype(jnp.float32) + d_x).astype(jnp.bfloat16)
            return d_gain + jnp.sum(grad * normed, axis=0, keepdims=True)

        dgain_ref[...] += lax.fori_loop(0, mid // fine, tile, jnp.zeros((1, hidden), jnp.float32))
        copies = [pltpu.make_async_copy(piece_of(stage.at[last, t], piece), piece_of(dst, piece), end_sem.at[piece, t])
                  for t, dst in ((0, y_own), (1, dx_own))]
        for copy in copies:
            copy.start()
        return copies

    ends = []
    ended = {0: 0, 1: 0}
    for work in EVENTS[-1]:
        event(*work)
        n, _, piece, ring = work
        if n == steps - 1 and ring == 2:
            ended[piece] += 1
            if ended[piece] == 2:
                ends += finish(piece)
    for slot in range(SLOTS):
        if slot != last:
            for copy in slot_sends(slot):
                copy.wait()
    for copy in ends + [save(steps - 1, n) for n in range(2)]:
        copy.wait()


def gather_kernel(n_parts, y_own, dx_own, dgain_ref, dy_hbm, a_all, hd_all, y_lo, y_hi, dx_all, dgain_out, grads, d_up,
                  gain_scr, acc, g_recv, a_buf, dy_buf, hd_buf, send_sem, link_sem, pair_sem, pair_recv, own_sem,
                  load_sem, g_send, g_land, dg_send, dg_recv):
    place = Place()
    core = place.core
    _, seq_len, hidden = dx_all.shape
    mid = seq_len // 2
    links = (('x', 1), ('x', -1), ('y', 1), ('y', -1))
    peers = [place.peer(a, o) for a in ('x', 'y') for o in (1, 2, 3)] + [place.sibling()]
    pl.semaphore_wait(greet(peers), len(peers))

    issued = {link: [] for link in links}
    sends = []

    def row_index(t, d_1, d_2):
        return place.index(d_1 % RING, d_2 % RING) if t == 0 else place.index(d_2 % RING, d_1 % RING)

    def spot_of(t, row, piece):
        if t == 1:
            return dx_all.at[row, pl.ds(piece * mid, mid)]
        return (y_lo, y_hi)[piece].at[row]

    def source(t, d_1, d_2, piece):
        if (d_1, d_2) == (0, 0):
            return (y_own, dx_own)[t].at[pl.ds(piece * mid, mid)]
        return spot_of(t, row_index(t, d_1, d_2), piece)

    def issue(link, t, d_1, d_2, piece):
        n = len(issued[link])
        which = links.index(link)
        copy = remote(source(t, d_1, d_2, piece), spot_of(t, row_index(t, d_1, d_2), piece),
                      send_sem.at[which, n], link_sem.at[which, n], place.peer(*link))
        copy.start()
        sends.append(copy)
        issued[link].append((t, d_1, d_2, piece))

    def pair(t, d_1, d_2, piece):
        slot = ((d_1 % RING) * RING + d_2 % RING) * 2 + piece
        copy = remote(source(t, d_1, d_2, piece), spot_of(t, row_index(t, d_1, d_2), piece),
                      pair_sem.at[t, slot], pair_recv.at[t, piece], place.sibling())
        copy.start()
        sends.append(copy)

    axes = (('y', 'x'), ('x', 'y'))
    for ring in range(2):
        for piece in range(2):
            for t in range(2):
                for way in (1, -1):
                    issue((axes[t][ring], way), t, 0, 0, piece)
    locals_ = []
    for t in range(2):
        for piece in range(2):
            pair(t, 0, 0, piece)
            copy = pltpu.make_async_copy(source(t, 0, 0, piece), spot_of(t, place.me, piece), own_sem.at[t, piece])
            copy.start()
            locals_.append(copy)

    depth, _, group = a_buf.shape
    rows = a_all.shape[0]
    n_qkv, n_up, n_o, n_dn = n_parts
    n_d = 2 * (n_qkv + n_up)
    segments, at, to = [], 0, 0
    for size in n_parts:
        segments.append((at, to, size))
        at, to = at + 2 * size, to + size

    def loads(r, h):
        slot = r % depth
        cols = pl.ds(h, group)
        return (pltpu.make_async_copy(a_all.at[r, :, cols], a_buf.at[slot], load_sem.at[slot, 0]),
                pltpu.make_async_copy(dy_hbm.at[2 * r + core, :, cols], dy_buf.at[slot], load_sem.at[slot, 1]),
                pltpu.make_async_copy(hd_all.at[r], hd_buf.at[slot], load_sem.at[slot, 2]))

    def swap_grads(n):
        return [remote(rows_at(acc, at + (1 - core) * size, size), g_recv.at[n % 2, pl.ds(to, size)],
                       g_send.at[m], g_land.at[n % 2, m], place.sibling()) for m, (at, to, size) in enumerate(segments)]

    def sum_rows(n):
        h = n * group
        acc[...] = jnp.zeros_like(acc)
        for r in range(depth - 1):
            for copy in loads(r, h):
                copy.start()

        def add_row(r, carry):
            slot = r % depth
            for copy in loads(r, h):
                copy.wait()

            @pl.when(r + depth - 1 < rows)
            def _():
                for copy in loads(r + depth - 1, h):
                    copy.start()

            acc[:n_d, :] += dot(hd_buf[slot, :n_d, :], a_buf[slot], NN)
            acc[n_d:, :] += dot(hd_buf[slot, n_d:, :], dy_buf[slot], NN)
            return carry

        lax.fori_loop(0, rows, add_row, 0)
        for copy in swap_grads(n):
            copy.start()

    def end_rows(n):
        for copy in swap_grads(n):
            copy.wait()
        for m, (at, to, size) in enumerate(segments):
            total = rows_at(acc, at + core * size, size)[...] + g_recv[n % 2, to:to + size, :]
            if m == 1:
                d_up[n * group:(n + 1) * group, :] = total.T.astype(d_up.dtype)
            else:
                spot = to if m == 0 else to - n_up
                grads[spot:spot + size, n * group:(n + 1) * group] = total.astype(grads.dtype)

    total = dgain_ref[...]
    for n, (axis, offsets) in enumerate((('core', (1,)), ('x', (1, 2, 3)), ('y', (1, 2, 3)))):
        spot = {'core': core, 'x': place.x, 'y': place.y}[axis]
        gain_scr[n, spot] = total
        copies = []
        for m, offset in enumerate(offsets):
            device = place.sibling() if axis == 'core' else place.peer(axis, offset)
            copies.append(remote(gain_scr.at[n, spot], gain_scr.at[n, spot], dg_send.at[n, m], dg_recv.at[n, m], device))
        for copy in copies:
            copy.start()
        for copy in copies:
            copy.wait()
        total = gain_scr[n, 0]
        for m in range(1, len(offsets) + 1):
            total = total + gain_scr[n, m]
    dgain_out[...] = jnp.sum(total, axis=0).astype(dgain_out.dtype)

    groups = hidden // group
    rounds = RING * RING - 1
    assert groups <= rounds
    for n in range(rounds):
        if n < groups:
            sum_rows(n)
        for link in links:
            t, d_1, d_2, piece = issued[link][n]
            axis, way = link
            on_first = axis == axes[t][0]
            d_1, d_2 = (d_1 - way, d_2) if on_first else (d_1, d_2 - way)
            landed(spot_of(t, row_index(t, d_1, d_2), piece), link_sem.at[links.index(link), n])
            along = d_1 if on_first else d_2
            if abs(along) == 1 and piece == (0 if way == 1 else 1):
                issue(link, t, d_1, d_2, piece)
            if on_first:
                for other in (1, -1):
                    issue((axes[t][1], other), t, d_1, d_2, piece)
            pair(t, d_1, d_2, piece)
        if n < groups:
            end_rows(n)

    for t in range(2):
        for piece in range(2):
            theirs = dx_all.at[pl.ds(0, RING * RING), pl.ds(piece * mid, mid)] if t else (y_lo, y_hi)[piece].at[pl.ds(0, RING * RING)]
            landed(theirs, pair_recv.at[t, piece])
    for copy in sends:
        copy.wait_send()
    for copy in locals_:
        copy.wait()


def place_kernel(y_lo, y_hi, dx_all, grads, d_up, dgain, y_out, dx_out, d_wqkv, d_wout, d_wdown, d_wup, dgain_out, bounce, in_sem, out_sem, sem):
    rows, mid, _ = y_lo.shape
    n_qkv, n_o, n_dn = d_wqkv.shape[0], d_wout.shape[0], d_wdown.shape[0]
    bufs, per = bounce.shape[0], bounce.shape[1]
    count = rows // per
    loads = [pltpu.make_async_copy(y_hi.at[pl.ds(n * per, per)], bounce.at[n % bufs], in_sem.at[n % bufs]) for n in range(count)]
    stores = [pltpu.make_async_copy(bounce.at[n % bufs], y_out.at[pl.ds(n * per, per), pl.ds(mid, mid)], out_sem.at[n % bufs]) for n in range(count)]
    for n in range(min(bufs, count)):
        loads[n].start()
    direct = [(y_lo, y_out.at[:, pl.ds(0, mid)]), (dx_all, dx_out), (grads.at[pl.ds(0, n_qkv)], d_wqkv),
              (grads.at[pl.ds(n_qkv, n_o)], d_wout), (grads.at[pl.ds(n_qkv + n_o, n_dn)], d_wdown), (d_up, d_wup)]
    copies = [pltpu.make_async_copy(src, dst, sem.at[n]) for n, (src, dst) in enumerate(direct)]
    for copy in copies:
        copy.start()
    dgain_out[...] = dgain[...]
    for n in range(count):
        loads[n].wait()
        stores[n].start()
        if n >= 1 and n - 1 + bufs < count:
            stores[n - 1].wait()
            loads[n - 1 + bufs].start()
    for n in range(max(0, count - bufs), count):
        stores[n].wait()
    for copy in copies:
        copy.wait()


def solution(mesh):
    devices = mesh.shape['model']
    assert devices == 2 * RING * RING

    def body(x_in, seg_ids, ln_gain, w_qkv, w_out, w_up, w_down, dy_in):
        rows, seq_len, hidden = x_in.shape
        assert rows == devices
        wqkv = w_qkv.transpose(1, 2, 3, 0).reshape(-1, hidden)
        wo = w_out.reshape(-1, hidden)
        n_parts = (wqkv.shape[0], w_up.shape[1], wo.shape[0], w_down.shape[0])
        n_in, n_out = n_parts[0] + n_parts[1], n_parts[2] + n_parts[3]
        n_all, n_up = n_in + n_out, n_parts[1]
        bf16, f32 = jnp.bfloat16, jnp.float32
        vmem, anywhere = pl.BlockSpec(memory_space=pltpu.VMEM), pl.BlockSpec(memory_space=pl.ANY)
        dma = pltpu.SemaphoreType.DMA
        shape = jax.ShapeDtypeStruct
        chips, mid, group = RING * RING, seq_len // 2, hidden // 8
        fixed = lambda array: pltpu.with_memory_space_constraint(array, pltpu.VMEM)
        y_own, dx_own, d_gain, a_all, hd_all = pl.pallas_call(
            reduce_kernel,
            in_specs=[anywhere, anywhere, vmem, vmem] + [anywhere] * 4,
            out_specs=[anywhere, anywhere, vmem, anywhere, anywhere],
            out_shape=[shape((seq_len, hidden), bf16), shape((seq_len, hidden), bf16), shape((1, hidden), f32),
                       shape((chips, seq_len, hidden), bf16), shape((chips, 2 * n_all, seq_len), bf16)],
            scratch_shapes=[
                pltpu.VMEM((2 * n_in, hidden), bf16), pltpu.VMEM((2 * n_out, hidden), bf16), pltpu.VMEM((hidden, n_up), bf16),
                pltpu.VMEM((2, seq_len, hidden), bf16), pltpu.VMEM((2, seq_len, hidden), bf16),
                pltpu.VMEM((seq_len, hidden), bf16), pltpu.VMEM((2 * n_all, seq_len), bf16),
                pltpu.VMEM((SLOTS, 2, seq_len, hidden), bf16),
                pltpu.VMEM((2, RING + 1, 2, mid, hidden), bf16),
                pltpu.VMEM((2, RING + 1, 2, seq_len, hidden), bf16),
                dma((2, 2)), dma((4,)), dma((4,)), dma((4,)), dma((SLOTS, 2, 2)),
                dma((2, RING + 1, 2)), dma((2, RING + 1, 2, 2)), dma((2, 2)), dma((2,)),
            ],
            compiler_params=pltpu.CompilerParams(collective_id=0, has_side_effects=True, vmem_limit_bytes=VMEM_LIMIT),
            name="rows_reduce",
        )(x_in, dy_in, seg_ids, ln_gain, wqkv, w_up, wo, w_down)

        per_link, depth = chips - 1, 4
        y_lo, y_hi, dx_all, d_gain, grads, d_up = pl.pallas_call(
            lambda *refs: gather_kernel(n_parts, *refs),
            in_specs=[anywhere, anywhere, vmem, anywhere, anywhere, anywhere],
            out_specs=[vmem, anywhere, vmem, vmem, vmem, vmem],
            out_shape=[pltpu.VMEM((rows, mid, hidden), bf16), shape((rows, mid, hidden), bf16), pltpu.VMEM((rows, seq_len, hidden), bf16),
                       pltpu.VMEM((hidden,), bf16), pltpu.VMEM((n_all - n_up, hidden), bf16), pltpu.VMEM((hidden, n_up), bf16)],
            scratch_shapes=[
                pltpu.VMEM((3, RING, 1, hidden), f32), pltpu.VMEM((2 * n_all, group), f32), pltpu.VMEM((2, n_all, group), f32),
                pltpu.VMEM((depth, seq_len, group), bf16), pltpu.VMEM((depth, seq_len, group), bf16), pltpu.VMEM((depth, 2 * n_all, seq_len), bf16),
                dma((4, per_link)), dma((4, per_link)), dma((2, 2 * chips)), dma((2, 2)), dma((2, 2)),
                dma((depth, 3)), dma((4,)), dma((2, 4)), dma((3, 3)), dma((3, 3)),
            ],
            compiler_params=pltpu.CompilerParams(collective_id=1, has_side_effects=True, vmem_limit_bytes=LANDING_LIMIT),
            name="rows_gather",
        )(y_own, dx_own, d_gain, dy_in, a_all, hd_all)

        bufs = 6
        y_out, dx_out, d_wqkv, d_wout, d_wdown, d_wup, d_gain = pl.pallas_call(
            place_kernel,
            in_specs=[vmem, anywhere, vmem, vmem, vmem, vmem],
            out_specs=[anywhere] * 6 + [vmem],
            out_shape=[shape(x_in.shape, bf16), shape(x_in.shape, bf16), shape(wqkv.shape, bf16), shape(wo.shape, bf16),
                       shape(w_down.shape, bf16), shape(w_up.shape, bf16), shape((hidden,), bf16)],
            scratch_shapes=[pltpu.VMEM((bufs, 2, mid, hidden), bf16), dma((bufs,)), dma((bufs,)), dma((6,))],
            compiler_params=pltpu.CompilerParams(vmem_limit_bytes=LANDING_LIMIT),
            name="rows_place",
        )(fixed(y_lo), pltpu.with_memory_space_constraint(y_hi, pltpu.HBM), fixed(dx_all), fixed(grads), fixed(d_up), fixed(d_gain))
        d_wqkv = d_wqkv.reshape(w_qkv.shape[1:] + (hidden,)).transpose(3, 0, 1, 2)
        return y_out, dx_out, d_gain, d_wqkv, d_wout.reshape(w_out.shape), d_wup, d_wdown

    in_specs = (P('data'), P('data'), P(), P(None, 'model'), P('model'), P(None, 'model'), P('model'), P('data'))
    out_specs = (P('data'), P('data'), P('data'), P('data', 'model'), P(('data', 'model')), P('data', 'model'), P(('data', 'model')))
    return jax.shard_map(body, mesh=mesh, in_specs=in_specs, out_specs=out_specs, check_vma=False)
```

```python
import jax
import jax.numpy as jnp
from jax import lax
from jax.experimental import pallas as pl
from jax.experimental.pallas import tpu as pltpu
from jax.sharding import PartitionSpec as P

LN_EPS = 1e-5
RING = 4
MESH = pl.DeviceIdType.MESH
NT = (((1,), (1,)), ((), ()))
NN = (((1,), (0,)), ((), ()))
TN = (((0,), (0,)), ((), ()))
ORDER = ((2, 2), (1, 2), (2, 3), (3, 2), (1, 1), (3, 3), (2, 1), (2, 0),
         (0, 2), (3, 1), (1, 3), (3, 0), (0, 3), (1, 0), (0, 1), (0, 0))
SLOT = (0, 1, 2, 3, 4, 0, 1, 3, 2, 0, 1, 4, 2, 3, 1, 0)
SLOTS = max(SLOT) + 1
EVENTS = (
    ((0, 0, 0, 1), (0, 0, 1, 1), (0, 1, 0, 1), (0, 1, 1, 1)),
    ((1, 0, 0, 1), (1, 0, 1, 1), (1, 1, 1, 1)),
    ((2, 0, 0, 1), (2, 1, 0, 1), (2, 1, 1, 1)),
    ((3, 0, 0, 1), (3, 0, 1, 1), (3, 1, 0, 1), (1, 1, 0, 1), (2, 0, 1, 1), (3, 1, 1, 1)),
    ((4, 0, 1, 1), (4, 1, 1, 1), (4, 0, 0, 1)),
    ((5, 0, 0, 1), (5, 1, 0, 1), (5, 1, 1, 1)),
    ((6, 0, 1, 1), (6, 1, 0, 1), (6, 1, 1, 1), (6, 0, 0, 1), (5, 0, 1, 1)),
    ((7, 1, 0, 1), (7, 1, 1, 1)),
    ((8, 0, 0, 1), (8, 0, 1, 1), (8, 1, 0, 1), (8, 1, 0, 2), (8, 1, 1, 1), (8, 1, 1, 2), (4, 1, 0, 1), (7, 0, 1, 1), (7, 0, 1, 2)),
    ((9, 0, 1, 1), (9, 1, 0, 1), (9, 0, 0, 1), (7, 0, 0, 1), (7, 0, 0, 2), (9, 1, 1, 1)),
    ((10, 0, 0, 1), (10, 1, 1, 1), (10, 0, 1, 1), (10, 1, 0, 1)),
    ((11, 1, 0, 1), (11, 1, 1, 1)),
    ((12, 0, 0, 1), (12, 0, 1, 1)),
    ((13, 1, 1, 1), (13, 1, 0, 1), (11, 0, 1, 1), (11, 0, 1, 2), (12, 1, 1, 1), (12, 1, 1, 2), (13, 0, 0, 1), (13, 0, 0, 2)),
    ((14, 0, 1, 1), (14, 0, 0, 1), (14, 1, 0, 1), (14, 1, 0, 2), (11, 0, 0, 1), (11, 0, 0, 2), (12, 1, 0, 1), (12, 1, 0, 2), (13, 0, 1, 1), (13, 0, 1, 2), (14, 1, 1, 1), (14, 1, 1, 2)),
    ((15, 0, 1, 1), (15, 1, 0, 1), (15, 1, 1, 1), (15, 0, 0, 1), (15, 0, 1, 2), (15, 1, 0, 2), (15, 0, 0, 2), (15, 1, 1, 2)),
)
VMEM_LIMIT = 60 * 2 ** 20
LANDING_LIMIT = 8 * 2 ** 20


def dot(lhs, rhs, dims):
    return lax.dot_general(lhs, rhs, dims, preferred_element_type=jnp.float32)


def norm_rows(x_f32):
    mean_val = jnp.mean(x_f32, axis=-1, keepdims=True)
    centered = x_f32 - mean_val
    inv_std = lax.rsqrt(jnp.mean(centered * centered, axis=-1, keepdims=True) + LN_EPS)
    return centered * inv_std, inv_std


class Place:
    def __init__(self):
        me = lax.axis_index('model')
        self.core = me % 2
        self.x = (me // 2) % RING
        self.y = me // (2 * RING)
        self.me = me

    def index(self, d_y, d_x, core=None):
        core = self.core if core is None else core
        return (((self.y + d_y) % RING) * RING + (self.x + d_x) % RING) * 2 + core

    def peer(self, axis, offset):
        return self.index(offset % RING, 0) if axis == 'y' else self.index(0, offset % RING)

    def sibling(self):
        return self.index(0, 0, 1 - self.core)


def remote(src, dst, send_sem, recv_sem, device):
    return pltpu.make_async_remote_copy(src_ref=src, dst_ref=dst, send_sem=send_sem, recv_sem=recv_sem,
                                        device_id={'model': device}, device_id_type=MESH)


def greet(peers):
    barrier = pltpu.get_barrier_semaphore()
    for peer in peers:
        pl.semaphore_signal(barrier, inc=1, device_id={'model': peer}, device_id_type=MESH)
    return barrier


def pick(step, values):
    out = jnp.int32(0)
    for n, value in enumerate(values):
        out = jnp.where(step == n, value, out)
    return out


def rows_at(ref, at, count):
    return ref.at[pl.ds(pl.multiple_of(at, 16), count)]


def landed(ref, sem):
    pltpu.make_async_copy(ref, ref, sem).wait()


def add_into(dst, *sources):
    rows = dst.shape[0]
    tile = min(rows, 32)

    def tile_add(n, carry):
        at = pl.ds(pl.multiple_of(n * tile, tile), tile)
        total = dst[at, :].astype(jnp.float32)
        for source in sources:
            total += source[at, :].astype(jnp.float32)
        dst[at, :] = total.astype(dst.dtype)
        return carry

    lax.fori_loop(0, rows // tile, tile_add, 0)


def reduce_kernel(x_hbm, dy_hbm, seg_ref, gain_ref, wqkv_hbm, w1_hbm, wo_hbm, w2_hbm,
                  y_own, dx_own, dgain_ref, a_all, hd_all,
                  w_in, w_out, w1_raw, x_buf, dy_buf, a_scr, hd_scr, stage, half, full,
                  row_sem, w_sem, ws_sem, wr_sem, send_sem, half_sem, full_sem, end_sem, save_sem):
    place = Place()
    core = place.core
    _, seq_len, hidden = x_buf.shape
    mid = seq_len // 2
    n_qkv, n_up, n_o, n_dn = wqkv_hbm.shape[0], w1_hbm.shape[1], wo_hbm.shape[0], w2_hbm.shape[0]
    n_d = 2 * (n_qkv + n_up)
    steps = len(ORDER)

    def row_of(step):
        return place.index(pick(step, [o[0] for o in ORDER]), pick(step, [o[1] for o in ORDER]))

    def row_copy(step, buf, n):
        return pltpu.make_async_copy((x_hbm, dy_hbm)[n].at[row_of(step)], (x_buf, dy_buf)[n].at[buf], row_sem.at[buf, n])

    def save(step, n):
        return pltpu.make_async_copy((a_scr, hd_scr)[n], (a_all, hd_all)[n].at[row_of(step) // 2], save_sem.at[n])

    up_spot = rows_at(w_in, 2 * n_qkv + core * n_up, n_up)
    spots = ((wqkv_hbm, rows_at(w_in, core * n_qkv, n_qkv)), (wo_hbm, rows_at(w_out, core * n_o, n_o)),
             (w2_hbm, rows_at(w_out, 2 * n_o + core * n_dn, n_dn)))

    gain = gain_ref[...].astype(jnp.float32)[None, :]
    sub = min(seq_len, 16)

    def norm_row(buf):
        for t in range(0, seq_len, sub):
            normed, _ = norm_rows(x_buf[buf, t:t + sub, :].astype(jnp.float32))
            a_scr[t:t + sub, :] = (normed * gain).astype(jnp.bfloat16)

    peers = [place.peer('x', 1), place.peer('x', -1), place.peer('y', 1), place.peer('y', -1), place.sibling()]
    barrier = greet(peers)
    raw = pltpu.make_async_copy(w1_hbm, w1_raw, w_sem.at[3])
    raw.start()
    for n in range(2):
        row_copy(0, 0, n).start()
    mine = [pltpu.make_async_copy(src, dst, w_sem.at[n]) for n, (src, dst) in enumerate(spots)]
    for copy in mine:
        copy.start()
    raw.wait()
    turn = min(hidden, 256)
    for h in range(0, hidden, turn):
        up_spot[:, h:h + turn] = w1_raw[h:h + turn, :].T
    pl.semaphore_wait(barrier, len(peers))
    swaps = [remote(src, dst, ws_sem.at[n], wr_sem.at[n], place.sibling()) for n, (src, dst) in enumerate(spots)]
    swaps.append(remote(up_spot, up_spot, ws_sem.at[3], wr_sem.at[3], place.sibling()))
    for n in (0, 3, 1, 2):
        swaps[n].start()
    row_copy(0, 0, 0).wait()
    norm_row(0)
    mine[0].wait()
    for n in (0, 3):
        swaps[n].wait()

    scale = n_o ** -0.5
    cols_step = min(hidden, 512)

    def piece_of(ref, piece):
        return ref.at[pl.ds(piece * mid, mid)]

    def slot_sends(slot):
        return [pltpu.make_async_copy(piece_of(stage.at[slot, t], piece), piece_of(stage.at[slot, t], piece),
                                      send_sem.at[slot, t, piece]) for t in range(2) for piece in range(2)]

    def event(n, t, piece, ring):
        d_y, d_x = ORDER[n]
        first, second = (('x', d_x), ('y', d_y)) if t == 0 else (('y', d_y), ('x', d_x))
        (axis, offset), line = (first, second[1]) if ring == 1 else (second, RING)
        ahead, behind = place.peer(axis, 1), place.peer(axis, -1)
        spot = piece_of(stage.at[SLOT[n], t], piece)

        def send(dst, recv_sem, device):
            remote(spot, dst, send_sem.at[SLOT[n], t, piece], recv_sem, device).start()

        if offset == 2:
            send(half.at[t, line, piece], half_sem.at[t, line, piece], ahead if piece == 0 else behind)
        elif offset in (1, 3):
            side = 0 if offset == 1 else 1
            if side == piece:
                landed(half.at[t, line, piece], half_sem.at[t, line, piece])
                add_into(spot, half.at[t, line, piece])
            send(piece_of(full.at[t, line, side], piece), full_sem.at[t, line, side, piece], ahead if side == 0 else behind)
        else:
            came = [piece_of(full.at[t, line, side], piece) for side in range(2)]
            for side in range(2):
                landed(came[side], full_sem.at[t, line, side, piece])
            add_into(spot, *came)

    def attend(head, qkv, d_attn, allowed):
        at = head * n_qkv
        query, keys, values = qkv[at:at + n_o], qkv[at + n_o:at + 2 * n_o], qkv[at + 2 * n_o:at + 3 * n_o]
        d_o = d_attn[head * n_o:(head + 1) * n_o]
        scores = jnp.where(allowed, dot(keys, query, TN) * scale, -1e30)
        expd = jnp.exp(scores - jnp.max(scores, axis=0, keepdims=True))
        probs = expd / jnp.sum(expd, axis=0, keepdims=True)
        probs_b = probs.astype(jnp.bfloat16)
        hd_scr[n_d + head * n_o:n_d + (head + 1) * n_o, :] = dot(values, probs_b, NN).astype(jnp.bfloat16)
        d_p = dot(values, d_o, TN)
        d_s = (probs * (d_p - jnp.sum(d_p * probs, axis=0, keepdims=True)) * scale).astype(jnp.bfloat16)
        hd_scr[at:at + n_o, :] = dot(keys, d_s, NN).astype(jnp.bfloat16)
        hd_scr[at + n_o:at + 2 * n_o, :] = dot(query, d_s, NT).astype(jnp.bfloat16)
        hd_scr[at + 2 * n_o:at + 3 * n_o, :] = dot(d_o, probs_b, NT).astype(jnp.bfloat16)

    def row_step(step, carry):
        buf = step % 2
        slot = pick(step, SLOT)

        @pl.when(step > 0)
        def _():
            for n in range(2):
                save(step - 1, n).wait()
            row_copy(step, buf, 0).wait()
            norm_row(buf)

        row_copy(step, buf, 1).wait()
        save(step, 0).start()

        @pl.when(step + 1 < steps)
        def _():
            for n in range(2):
                row_copy(step + 1, 1 - buf, n).start()

        @pl.when(step == 0)
        def _():
            for copy in mine[1:] + swaps[1:3]:
                copy.wait()

        proj = dot(w_in[...], a_scr[...], NT)
        d_proj = dot(w_out[...], dy_buf[buf], NT).astype(jnp.bfloat16)
        qkv = proj[:2 * n_qkv].astype(jnp.bfloat16)
        up = proj[2 * n_qkv:].astype(jnp.bfloat16).astype(jnp.float32)
        d_attn = d_proj[:2 * n_o]
        d_hid = d_proj[2 * n_o:].astype(jnp.float32)
        cdf = 0.5 * (1.0 + lax.erf(up * (0.5 ** 0.5)))
        hd_scr[n_d + 2 * n_o:, :] = (up * cdf).astype(jnp.bfloat16)
        slope = cdf + up * (jnp.exp(-0.5 * up * up) * 0.3989422804014327)
        hd_scr[2 * n_qkv:n_d, :] = (d_hid * slope).astype(jnp.bfloat16)

        seg_row = seg_ref[pl.ds(row_of(step), 1), :]
        classes = lax.broadcasted_iota(jnp.int32, (16, seq_len), 0)
        one_hot = (classes == jnp.broadcast_to(seg_row, (16, seq_len))).astype(jnp.bfloat16)
        same = dot(one_hot, one_hot, TN) > 0.5
        key_id = lax.broadcasted_iota(jnp.int32, (seq_len, seq_len), 0)
        query_id = lax.broadcasted_iota(jnp.int32, (seq_len, seq_len), 1)
        allowed = (key_id <= query_id) & same
        for head in range(2):
            attend(head, qkv, d_attn, allowed)
        save(step, 1).start()

        @pl.when(pick(step, [int(SLOT[n] in SLOT[:n]) for n in range(steps)]) == 1)
        def _():
            for copy in slot_sends(slot):
                copy.wait()

        for h in range(0, hidden, cols_step):
            cols = slice(h, h + cols_step)
            stage[slot, 0, :, cols] = dot(hd_scr[n_d:, :], w_out[:, cols], TN).astype(jnp.bfloat16)
            stage[slot, 1, :, cols] = dot(hd_scr[:n_d, :], w_in[:, cols], TN).astype(jnp.bfloat16)

        for n in range(steps - 1):
            @pl.when(step == n)
            def _():
                for work in EVENTS[n]:
                    event(*work)
        return carry

    lax.fori_loop(0, steps, row_step, 0)
    last, buf = SLOT[-1], (steps - 1) % 2
    dgain_ref[...] = jnp.zeros_like(dgain_ref)
    fine = min(mid, 32)

    def finish(piece):
        def tile(n, d_gain):
            at = pl.ds(pl.multiple_of(piece * mid + n * fine, fine), fine)
            x_f32 = x_buf[buf, at, :].astype(jnp.float32)
            normed, inv_std = norm_rows(x_f32)
            grad = stage[last, 1, at, :].astype(jnp.float32)
            stage[last, 0, at, :] = (x_f32 + stage[last, 0, at, :].astype(jnp.float32)).astype(jnp.bfloat16)
            d_hat = grad * gain
            d_x = inv_std * (d_hat - jnp.mean(d_hat, axis=-1, keepdims=True) - normed * jnp.mean(d_hat * normed, axis=-1, keepdims=True))
            stage[last, 1, at, :] = (dy_buf[buf, at, :].astype(jnp.float32) + d_x).astype(jnp.bfloat16)
            return d_gain + jnp.sum(grad * normed, axis=0, keepdims=True)

        dgain_ref[...] += lax.fori_loop(0, mid // fine, tile, jnp.zeros((1, hidden), jnp.float32))
        copies = [pltpu.make_async_copy(piece_of(stage.at[last, t], piece), piece_of(dst, piece), end_sem.at[piece, t])
                  for t, dst in ((0, y_own), (1, dx_own))]
        for copy in copies:
            copy.start()
        return copies

    ends = []
    ended = {0: 0, 1: 0}
    for work in EVENTS[-1]:
        event(*work)
        n, _, piece, ring = work
        if n == steps - 1 and ring == 2:
            ended[piece] += 1
            if ended[piece] == 2:
                ends += finish(piece)
    for slot in range(SLOTS):
        if slot != last:
            for copy in slot_sends(slot):
                copy.wait()
    for copy in ends + [save(steps - 1, n) for n in range(2)]:
        copy.wait()


def gather_kernel(n_parts, y_own, dx_own, dgain_ref, dy_hbm, a_all, hd_all, y_lo, y_hi, dx_all, dgain_out, grads, d_up,
                  gain_scr, acc, g_recv, a_buf, dy_buf, hd_buf, send_sem, link_sem, pair_sem, pair_recv, own_sem,
                  load_sem, g_send, g_land, dg_send, dg_recv):
    place = Place()
    core = place.core
    _, seq_len, hidden = dx_all.shape
    mid = seq_len // 2
    links = (('x', 1), ('x', -1), ('y', 1), ('y', -1))
    peers = [place.peer(a, o) for a in ('x', 'y') for o in (1, -1)] + [place.sibling()]
    pl.semaphore_wait(greet(peers), len(peers))

    issued = {link: [] for link in links}
    sends = []

    def row_index(t, d_1, d_2):
        return place.index(d_1 % RING, d_2 % RING) if t == 0 else place.index(d_2 % RING, d_1 % RING)

    def spot_of(t, row, piece):
        if t == 1:
            return dx_all.at[row, pl.ds(piece * mid, mid)]
        return (y_lo, y_hi)[piece].at[row]

    def source(t, d_1, d_2, piece):
        if (d_1, d_2) == (0, 0):
            return (y_own, dx_own)[t].at[pl.ds(piece * mid, mid)]
        return spot_of(t, row_index(t, d_1, d_2), piece)

    def issue(link, t, d_1, d_2, piece):
        n = len(issued[link])
        which = links.index(link)
        copy = remote(source(t, d_1, d_2, piece), spot_of(t, row_index(t, d_1, d_2), piece),
                      send_sem.at[which, n], link_sem.at[which, n], place.peer(*link))
        copy.start()
        sends.append(copy)
        issued[link].append((t, d_1, d_2, piece))

    def pair(t, d_1, d_2, piece):
        slot = ((d_1 % RING) * RING + d_2 % RING) * 2 + piece
        copy = remote(source(t, d_1, d_2, piece), spot_of(t, row_index(t, d_1, d_2), piece),
                      pair_sem.at[t, slot], pair_recv.at[t, piece], place.sibling())
        copy.start()
        sends.append(copy)

    axes = (('y', 'x'), ('x', 'y'))
    for ring in range(2):
        for n in range(2):
            for t in range(2):
                for way in (1, -1):
                    issue((axes[t][ring], way), t, 0, 0, n if way == 1 else 1 - n)
    locals_ = []
    for t in range(2):
        for piece in range(2):
            pair(t, 0, 0, piece)
            copy = pltpu.make_async_copy(source(t, 0, 0, piece), spot_of(t, place.me, piece), own_sem.at[t, piece])
            copy.start()
            locals_.append(copy)

    depth, _, _, group = a_buf.shape
    pairs = a_all.shape[0] // 2
    groups = hidden // group
    n_qkv, n_up, n_o, n_dn = n_parts
    n_d = 2 * (n_qkv + n_up)
    segments, at, to = [], 0, 0
    for size in n_parts:
        segments.append((at, to, size))
        at, to = at + 2 * size, to + size

    def loads(count):
        slot = count % depth
        first = 2 * (count % pairs)
        cols = pl.ds(pl.multiple_of(count // pairs * group, group), group)
        copies = []
        for m in range(2):
            r = first + m
            copies += [pltpu.make_async_copy(a_all.at[r, :, cols], a_buf.at[slot, m], load_sem.at[slot, m, 0]),
                       pltpu.make_async_copy(dy_hbm.at[2 * r + core, :, cols], dy_buf.at[slot, m], load_sem.at[slot, m, 1]),
                       pltpu.make_async_copy(hd_all.at[r], hd_buf.at[slot, m], load_sem.at[slot, m, 2])]
        return copies

    def swap_grads(n):
        return [remote(rows_at(acc, at + (1 - core) * size, size), g_recv.at[n % 2, pl.ds(to, size)],
                       g_send.at[m], g_land.at[n % 2, m], place.sibling()) for m, (at, to, size) in enumerate(segments)]

    for count in range(depth - 1):
        for copy in loads(count):
            copy.start()

    def sum_rows(n):
        acc[...] = jnp.zeros_like(acc)

        def add_pair(i, carry):
            count = n * pairs + i
            slot = count % depth
            for copy in loads(count):
                copy.wait()

            @pl.when(count + depth - 1 < groups * pairs)
            def _():
                for copy in loads(count + depth - 1):
                    copy.start()

            acc[:n_d, :] += dot(hd_buf[slot, 0, :n_d, :], a_buf[slot, 0], NN) + dot(hd_buf[slot, 1, :n_d, :], a_buf[slot, 1], NN)
            acc[n_d:, :] += dot(hd_buf[slot, 0, n_d:, :], dy_buf[slot, 0], NN) + dot(hd_buf[slot, 1, n_d:, :], dy_buf[slot, 1], NN)
            return carry

        lax.fori_loop(0, pairs, add_pair, 0)
        for copy in swap_grads(n):
            copy.start()

    def end_rows(n):
        for copy in swap_grads(n):
            copy.wait()
        for m, (at, to, size) in enumerate(segments):
            total = rows_at(acc, at + core * size, size)[...] + g_recv[n % 2, to:to + size, :]
            if m == 1:
                d_up[n * group:(n + 1) * group, :] = total.T.astype(d_up.dtype)
            else:
                spot = to if m == 0 else to - n_up
                grads[spot:spot + size, n * group:(n + 1) * group] = total.astype(grads.dtype)

    total = dgain_ref[...]
    for n, axis in enumerate(('core', 'x', 'x', 'y', 'y')):
        at = {'core': core, 'x': place.x, 'y': place.y}[axis]
        other = (RING - 1 - at) if n in (2, 4) else at + 1 - 2 * (at % 2)
        device = place.sibling() if axis == 'core' else place.peer(axis, other - at)
        gain_scr[n, 0] = total
        copy = remote(gain_scr.at[n, 0], gain_scr.at[n, 1], dg_send.at[n], dg_recv.at[n], device)
        copy.start()
        copy.wait()
        total = gain_scr[n, 0] + gain_scr[n, 1]
    dgain_out[...] = jnp.sum(total, axis=0).astype(dgain_out.dtype)

    rounds = RING * RING - 1
    assert groups <= rounds
    for n in range(rounds):
        if n < groups:
            sum_rows(n)
        for link in links:
            t, d_1, d_2, piece = issued[link][n]
            axis, way = link
            on_first = axis == axes[t][0]
            d_1, d_2 = (d_1 - way, d_2) if on_first else (d_1, d_2 - way)
            landed(spot_of(t, row_index(t, d_1, d_2), piece), link_sem.at[links.index(link), n])
            along = d_1 if on_first else d_2
            if abs(along) == 1 and piece == (0 if way == 1 else 1):
                issue(link, t, d_1, d_2, piece)
            if on_first:
                for other in (1, -1):
                    issue((axes[t][1], other), t, d_1, d_2, piece)
            pair(t, d_1, d_2, piece)
        if n < groups:
            end_rows(n)

    for t in range(2):
        for piece in range(2):
            theirs = dx_all.at[pl.ds(0, RING * RING), pl.ds(piece * mid, mid)] if t else (y_lo, y_hi)[piece].at[pl.ds(0, RING * RING)]
            landed(theirs, pair_recv.at[t, piece])
    for copy in sends:
        copy.wait_send()
    for copy in locals_:
        copy.wait()


def place_kernel(y_lo, y_hi, dx_all, grads, d_up, dgain, y_out, dx_out, d_wqkv, d_wout, d_wdown, d_wup, dgain_out, bounce, in_sem, out_sem, sem):
    rows, mid, _ = y_lo.shape
    n_qkv, n_o, n_dn = d_wqkv.shape[0], d_wout.shape[0], d_wdown.shape[0]
    bufs, per = bounce.shape[0], bounce.shape[1]
    count = rows // per
    loads = [pltpu.make_async_copy(y_hi.at[pl.ds(n * per, per)], bounce.at[n % bufs], in_sem.at[n % bufs]) for n in range(count)]
    stores = [pltpu.make_async_copy(bounce.at[n % bufs], y_out.at[pl.ds(n * per, per), pl.ds(mid, mid)], out_sem.at[n % bufs]) for n in range(count)]
    for n in range(min(bufs, count)):
        loads[n].start()
    split = 4
    part = rows // split
    direct = []
    for n in range(split):
        at = pl.ds(n * part, part)
        direct += [(dx_all.at[at], dx_out.at[at]), (y_lo.at[at], y_out.at[at, pl.ds(0, mid)])]
    direct += [(grads.at[pl.ds(0, n_qkv)], d_wqkv),
               (grads.at[pl.ds(n_qkv, n_o)], d_wout), (grads.at[pl.ds(n_qkv + n_o, n_dn)], d_wdown), (d_up, d_wup)]
    copies = [pltpu.make_async_copy(src, dst, sem.at[n]) for n, (src, dst) in enumerate(direct)]
    for copy in copies:
        copy.start()
    dgain_out[...] = dgain[...]
    for n in range(count):
        loads[n].wait()
        stores[n].start()
        if n >= 1 and n - 1 + bufs < count:
            stores[n - 1].wait()
            loads[n - 1 + bufs].start()
    for n in range(max(0, count - bufs), count):
        stores[n].wait()
    for copy in copies:
        copy.wait()


def solution(mesh):
    devices = mesh.shape['model']
    assert devices == 2 * RING * RING

    def body(x_in, seg_ids, ln_gain, w_qkv, w_out, w_up, w_down, dy_in):
        rows, seq_len, hidden = x_in.shape
        assert rows == devices
        wqkv = w_qkv.transpose(1, 2, 3, 0).reshape(-1, hidden)
        wo = w_out.reshape(-1, hidden)
        n_parts = (wqkv.shape[0], w_up.shape[1], wo.shape[0], w_down.shape[0])
        n_in, n_out = n_parts[0] + n_parts[1], n_parts[2] + n_parts[3]
        n_all, n_up = n_in + n_out, n_parts[1]
        bf16, f32 = jnp.bfloat16, jnp.float32
        vmem, anywhere = pl.BlockSpec(memory_space=pltpu.VMEM), pl.BlockSpec(memory_space=pl.ANY)
        dma = pltpu.SemaphoreType.DMA
        shape = jax.ShapeDtypeStruct
        chips, mid, group = RING * RING, seq_len // 2, hidden // 8
        fixed = lambda array: pltpu.with_memory_space_constraint(array, pltpu.VMEM)
        y_own, dx_own, d_gain, a_all, hd_all = pl.pallas_call(
            reduce_kernel,
            in_specs=[anywhere, anywhere, vmem, vmem] + [anywhere] * 4,
            out_specs=[anywhere, anywhere, vmem, anywhere, anywhere],
            out_shape=[shape((seq_len, hidden), bf16), shape((seq_len, hidden), bf16), shape((1, hidden), f32),
                       shape((chips, seq_len, hidden), bf16), shape((chips, 2 * n_all, seq_len), bf16)],
            scratch_shapes=[
                pltpu.VMEM((2 * n_in, hidden), bf16), pltpu.VMEM((2 * n_out, hidden), bf16), pltpu.VMEM((hidden, n_up), bf16),
                pltpu.VMEM((2, seq_len, hidden), bf16), pltpu.VMEM((2, seq_len, hidden), bf16),
                pltpu.VMEM((seq_len, hidden), bf16), pltpu.VMEM((2 * n_all, seq_len), bf16),
                pltpu.VMEM((SLOTS, 2, seq_len, hidden), bf16),
                pltpu.VMEM((2, RING + 1, 2, mid, hidden), bf16),
                pltpu.VMEM((2, RING + 1, 2, seq_len, hidden), bf16),
                dma((2, 2)), dma((4,)), dma((4,)), dma((4,)), dma((SLOTS, 2, 2)),
                dma((2, RING + 1, 2)), dma((2, RING + 1, 2, 2)), dma((2, 2)), dma((2,)),
            ],
            compiler_params=pltpu.CompilerParams(collective_id=0, has_side_effects=True, vmem_limit_bytes=VMEM_LIMIT),
            name="rows_reduce",
        )(x_in, dy_in, seg_ids, ln_gain, wqkv, w_up, wo, w_down)

        per_link, depth = chips - 1, 2
        y_lo, y_hi, dx_all, d_gain, grads, d_up = pl.pallas_call(
            lambda *refs: gather_kernel(n_parts, *refs),
            in_specs=[anywhere, anywhere, vmem, anywhere, anywhere, anywhere],
            out_specs=[vmem, anywhere, vmem, vmem, vmem, vmem],
            out_shape=[pltpu.VMEM((rows, mid, hidden), bf16), shape((rows, mid, hidden), bf16), pltpu.VMEM((rows, seq_len, hidden), bf16),
                       pltpu.VMEM((hidden,), bf16), pltpu.VMEM((n_all - n_up, hidden), bf16), pltpu.VMEM((hidden, n_up), bf16)],
            scratch_shapes=[
                pltpu.VMEM((5, 2, 1, hidden), f32), pltpu.VMEM((2 * n_all, group), f32), pltpu.VMEM((2, n_all, group), f32),
                pltpu.VMEM((depth, 2, seq_len, group), bf16), pltpu.VMEM((depth, 2, seq_len, group), bf16),
                pltpu.VMEM((depth, 2, 2 * n_all, seq_len), bf16),
                dma((4, per_link)), dma((4, per_link)), dma((2, 2 * chips)), dma((2, 2)), dma((2, 2)),
                dma((depth, 2, 3)), dma((4,)), dma((2, 4)), dma((5,)), dma((5,)),
            ],
            compiler_params=pltpu.CompilerParams(collective_id=1, has_side_effects=True, vmem_limit_bytes=LANDING_LIMIT),
            name="rows_gather",
        )(y_own, dx_own, d_gain, dy_in, a_all, hd_all)

        bufs = 6
        y_out, dx_out, d_wqkv, d_wout, d_wdown, d_wup, d_gain = pl.pallas_call(
            place_kernel,
            in_specs=[vmem, anywhere, vmem, vmem, vmem, vmem],
            out_specs=[anywhere] * 6 + [vmem],
            out_shape=[shape(x_in.shape, bf16), shape(x_in.shape, bf16), shape(wqkv.shape, bf16), shape(wo.shape, bf16),
                       shape(w_down.shape, bf16), shape(w_up.shape, bf16), shape((hidden,), bf16)],
            scratch_shapes=[pltpu.VMEM((bufs, 2, mid, hidden), bf16), dma((bufs,)), dma((bufs,)), dma((12,))],
            compiler_params=pltpu.CompilerParams(vmem_limit_bytes=LANDING_LIMIT),
            name="rows_place",
        )(fixed(y_lo), pltpu.with_memory_space_constraint(y_hi, pltpu.HBM), fixed(dx_all), fixed(grads), fixed(d_up), fixed(d_gain))
        d_wqkv = d_wqkv.reshape(w_qkv.shape[1:] + (hidden,)).transpose(3, 0, 1, 2)
        return y_out, dx_out, d_gain, d_wqkv, d_wout.reshape(w_out.shape), d_wup, d_wdown

    in_specs = (P('data'), P('data'), P(), P(None, 'model'), P('model'), P(None, 'model'), P('model'), P('data'))
    out_specs = (P('data'), P('data'), P('data'), P('data', 'model'), P(('data', 'model')), P('data', 'model'), P(('data', 'model')))
    return jax.shard_map(body, mesh=mesh, in_specs=in_specs, out_specs=out_specs, check_vma=False)
```

```python
import jax
import jax.numpy as jnp
from jax import lax
from jax.experimental import pallas as pl
from jax.experimental.pallas import tpu as pltpu
from jax.sharding import PartitionSpec as P

LN_EPS = 1e-5
RING = 4
MESH = pl.DeviceIdType.MESH
NT = (((1,), (1,)), ((), ()))
NN = (((1,), (0,)), ((), ()))
TN = (((0,), (0,)), ((), ()))
ORDER = ((2, 2), (1, 2), (2, 3), (3, 2), (1, 1), (3, 3), (2, 1), (2, 0),
         (0, 2), (3, 1), (1, 3), (3, 0), (0, 3), (1, 0), (0, 1), (0, 0))
SLOT = (0, 1, 2, 3, 4, 0, 1, 3, 2, 0, 1, 4, 2, 3, 1, 0)
SLOTS = max(SLOT) + 1
EVENTS = (
    ((0, 0, 0, 1), (0, 0, 1, 1), (0, 1, 0, 1), (0, 1, 1, 1)),
    ((1, 0, 0, 1), (1, 0, 1, 1), (1, 1, 1, 1)),
    ((2, 0, 0, 1), (2, 1, 0, 1), (2, 1, 1, 1)),
    ((3, 0, 0, 1), (3, 0, 1, 1), (3, 1, 0, 1), (1, 1, 0, 1), (2, 0, 1, 1), (3, 1, 1, 1)),
    ((4, 0, 1, 1), (4, 1, 1, 1), (4, 0, 0, 1)),
    ((5, 0, 0, 1), (5, 1, 0, 1), (5, 1, 1, 1)),
    ((6, 0, 1, 1), (6, 1, 0, 1), (6, 1, 1, 1), (6, 0, 0, 1), (5, 0, 1, 1)),
    ((7, 1, 0, 1), (7, 1, 1, 1)),
    ((8, 0, 0, 1), (8, 0, 1, 1), (8, 1, 0, 1), (8, 1, 0, 2), (8, 1, 1, 1), (8, 1, 1, 2), (4, 1, 0, 1), (7, 0, 1, 1), (7, 0, 1, 2)),
    ((9, 0, 1, 1), (9, 1, 0, 1), (9, 0, 0, 1), (7, 0, 0, 1), (7, 0, 0, 2), (9, 1, 1, 1)),
    ((10, 0, 0, 1), (10, 1, 1, 1), (10, 0, 1, 1), (10, 1, 0, 1)),
    ((11, 1, 0, 1), (11, 1, 1, 1)),
    ((12, 0, 0, 1), (12, 0, 1, 1)),
    ((13, 1, 1, 1), (13, 1, 0, 1), (11, 0, 1, 1), (11, 0, 1, 2), (12, 1, 1, 1), (12, 1, 1, 2), (13, 0, 0, 1), (13, 0, 0, 2)),
    ((14, 0, 1, 1), (14, 0, 0, 1), (14, 1, 0, 1), (14, 1, 0, 2), (11, 0, 0, 1), (11, 0, 0, 2), (12, 1, 0, 1), (12, 1, 0, 2), (13, 0, 1, 1), (13, 0, 1, 2), (14, 1, 1, 1), (14, 1, 1, 2)),
    ((15, 0, 1, 1), (15, 1, 0, 1), (15, 1, 1, 1), (15, 0, 0, 1), (15, 0, 1, 2), (15, 1, 0, 2), (15, 0, 0, 2), (15, 1, 1, 2)),
)
VMEM_LIMIT = 60 * 2 ** 20
LANDING_LIMIT = 41 * 2 ** 18


def dot(lhs, rhs, dims):
    return lax.dot_general(lhs, rhs, dims, preferred_element_type=jnp.float32)


def norm_rows(x_f32):
    mean_val = jnp.mean(x_f32, axis=-1, keepdims=True)
    centered = x_f32 - mean_val
    inv_std = lax.rsqrt(jnp.mean(centered * centered, axis=-1, keepdims=True) + LN_EPS)
    return centered * inv_std, inv_std


class Place:
    def __init__(self):
        me = lax.axis_index('model')
        self.core = me % 2
        self.x = (me // 2) % RING
        self.y = me // (2 * RING)
        self.me = me

    def index(self, d_y, d_x, core=None):
        core = self.core if core is None else core
        return (((self.y + d_y) % RING) * RING + (self.x + d_x) % RING) * 2 + core

    def peer(self, axis, offset):
        return self.index(offset % RING, 0) if axis == 'y' else self.index(0, offset % RING)

    def sibling(self):
        return self.index(0, 0, 1 - self.core)


def remote(src, dst, send_sem, recv_sem, device):
    return pltpu.make_async_remote_copy(src_ref=src, dst_ref=dst, send_sem=send_sem, recv_sem=recv_sem,
                                        device_id={'model': device}, device_id_type=MESH)


def greet(peers):
    barrier = pltpu.get_barrier_semaphore()
    for peer in peers:
        pl.semaphore_signal(barrier, inc=1, device_id={'model': peer}, device_id_type=MESH)
    return barrier


def pick(step, values):
    out = jnp.int32(0)
    for n, value in enumerate(values):
        out = jnp.where(step == n, value, out)
    return out


def rows_at(ref, at, count):
    return ref.at[pl.ds(pl.multiple_of(at, 16), count)]


def landed(ref, sem):
    pltpu.make_async_copy(ref, ref, sem).wait()


def add_into(dst, *sources):
    rows = dst.shape[0]
    tile = min(rows, 32)

    def tile_add(n, carry):
        at = pl.ds(pl.multiple_of(n * tile, tile), tile)
        total = dst[at, :].astype(jnp.float32)
        for source in sources:
            total += source[at, :].astype(jnp.float32)
        dst[at, :] = total.astype(dst.dtype)
        return carry

    lax.fori_loop(0, rows // tile, tile_add, 0)


def reduce_kernel(x_hbm, dy_hbm, seg_ref, gain_ref, wqkv_hbm, w1_hbm, wo_hbm, w2_hbm,
                  y_own, dx_own, dgain_ref, a_all, hd_all,
                  w_in, w_out, w1_raw, x_buf, dy_buf, a_scr, hd_scr, stage, half, full,
                  row_sem, w_sem, ws_sem, wr_sem, send_sem, half_sem, full_sem, end_sem, save_sem):
    place = Place()
    core = place.core
    _, seq_len, hidden = x_buf.shape
    mid = seq_len // 2
    n_qkv, n_up, n_o, n_dn = wqkv_hbm.shape[0], w1_hbm.shape[1], wo_hbm.shape[0], w2_hbm.shape[0]
    n_d = 2 * (n_qkv + n_up)
    steps = len(ORDER)

    def row_of(step):
        return place.index(pick(step, [o[0] for o in ORDER]), pick(step, [o[1] for o in ORDER]))

    def row_copy(step, buf, n):
        return pltpu.make_async_copy((x_hbm, dy_hbm)[n].at[row_of(step)], (x_buf, dy_buf)[n].at[buf], row_sem.at[buf, n])

    def save(step, n):
        return pltpu.make_async_copy((a_scr, hd_scr)[n], (a_all, hd_all)[n].at[row_of(step) // 2], save_sem.at[n])

    up_spot = rows_at(w_in, 2 * n_qkv + core * n_up, n_up)
    spots = ((wqkv_hbm, rows_at(w_in, core * n_qkv, n_qkv)), (wo_hbm, rows_at(w_out, core * n_o, n_o)),
             (w2_hbm, rows_at(w_out, 2 * n_o + core * n_dn, n_dn)))

    gain = gain_ref[...].astype(jnp.float32)[None, :]
    sub = min(seq_len, 16)

    def norm_row(buf):
        for t in range(0, seq_len, sub):
            normed, _ = norm_rows(x_buf[buf, t:t + sub, :].astype(jnp.float32))
            a_scr[t:t + sub, :] = (normed * gain).astype(jnp.bfloat16)

    peers = [place.peer('x', 1), place.peer('x', -1), place.peer('y', 1), place.peer('y', -1), place.sibling()]
    barrier = greet(peers)
    raw = pltpu.make_async_copy(w1_hbm, w1_raw, w_sem.at[3])
    raw.start()
    for n in range(2):
        row_copy(0, 0, n).start()
    mine = [pltpu.make_async_copy(src, dst, w_sem.at[n]) for n, (src, dst) in enumerate(spots)]
    for copy in mine:
        copy.start()
    raw.wait()
    turn = min(hidden, 256)
    for h in range(0, hidden, turn):
        up_spot[:, h:h + turn] = w1_raw[h:h + turn, :].T
    pl.semaphore_wait(barrier, len(peers))
    swaps = [remote(src, dst, ws_sem.at[n], wr_sem.at[n], place.sibling()) for n, (src, dst) in enumerate(spots)]
    swaps.append(remote(up_spot, up_spot, ws_sem.at[3], wr_sem.at[3], place.sibling()))
    for n in (0, 3, 1, 2):
        swaps[n].start()
    row_copy(0, 0, 0).wait()
    norm_row(0)
    mine[0].wait()
    for n in (0, 3):
        swaps[n].wait()

    scale = n_o ** -0.5
    cols_step = min(hidden, 512)

    def piece_of(ref, piece):
        return ref.at[pl.ds(piece * mid, mid)]

    def slot_sends(slot):
        return [pltpu.make_async_copy(piece_of(stage.at[slot, t], piece), piece_of(stage.at[slot, t], piece),
                                      send_sem.at[slot, t, piece]) for t in range(2) for piece in range(2)]

    def event(n, t, piece, ring):
        d_y, d_x = ORDER[n]
        first, second = (('x', d_x), ('y', d_y)) if t == 0 else (('y', d_y), ('x', d_x))
        (axis, offset), line = (first, second[1]) if ring == 1 else (second, RING)
        ahead, behind = place.peer(axis, 1), place.peer(axis, -1)
        spot = piece_of(stage.at[SLOT[n], t], piece)

        def send(dst, recv_sem, device):
            remote(spot, dst, send_sem.at[SLOT[n], t, piece], recv_sem, device).start()

        if offset == 2:
            send(half.at[t, line, piece], half_sem.at[t, line, piece], ahead if piece == 0 else behind)
        elif offset in (1, 3):
            side = 0 if offset == 1 else 1
            if side == piece:
                landed(half.at[t, line, piece], half_sem.at[t, line, piece])
                add_into(spot, half.at[t, line, piece])
            send(piece_of(full.at[t, line, side], piece), full_sem.at[t, line, side, piece], ahead if side == 0 else behind)
        else:
            came = [piece_of(full.at[t, line, side], piece) for side in range(2)]
            for side in range(2):
                landed(came[side], full_sem.at[t, line, side, piece])
            add_into(spot, *came)

    def attend(head, qkv, d_attn, allowed):
        at = head * n_qkv
        query, keys, values = qkv[at:at + n_o], qkv[at + n_o:at + 2 * n_o], qkv[at + 2 * n_o:at + 3 * n_o]
        d_o = d_attn[head * n_o:(head + 1) * n_o]
        scores = jnp.where(allowed, dot(keys, query, TN) * scale, -1e30)
        expd = jnp.exp(scores - jnp.max(scores, axis=0, keepdims=True))
        probs = expd / jnp.sum(expd, axis=0, keepdims=True)
        probs_b = probs.astype(jnp.bfloat16)
        hd_scr[n_d + head * n_o:n_d + (head + 1) * n_o, :] = dot(values, probs_b, NN).astype(jnp.bfloat16)
        d_p = dot(values, d_o, TN)
        d_s = (probs * (d_p - jnp.sum(d_p * probs, axis=0, keepdims=True)) * scale).astype(jnp.bfloat16)
        hd_scr[at:at + n_o, :] = dot(keys, d_s, NN).astype(jnp.bfloat16)
        hd_scr[at + n_o:at + 2 * n_o, :] = dot(query, d_s, NT).astype(jnp.bfloat16)
        hd_scr[at + 2 * n_o:at + 3 * n_o, :] = dot(d_o, probs_b, NT).astype(jnp.bfloat16)

    def row_step(step, carry):
        buf = step % 2
        slot = pick(step, SLOT)

        @pl.when(step > 0)
        def _():
            for n in range(2):
                save(step - 1, n).wait()
            row_copy(step, buf, 0).wait()
            norm_row(buf)

        row_copy(step, buf, 1).wait()
        save(step, 0).start()

        @pl.when(step + 1 < steps)
        def _():
            for n in range(2):
                row_copy(step + 1, 1 - buf, n).start()

        @pl.when(step == 0)
        def _():
            for copy in mine[1:] + swaps[1:3]:
                copy.wait()

        proj = dot(w_in[...], a_scr[...], NT)
        d_proj = dot(w_out[...], dy_buf[buf], NT).astype(jnp.bfloat16)
        qkv = proj[:2 * n_qkv].astype(jnp.bfloat16)
        up = proj[2 * n_qkv:].astype(jnp.bfloat16).astype(jnp.float32)
        d_attn = d_proj[:2 * n_o]
        d_hid = d_proj[2 * n_o:].astype(jnp.float32)
        cdf = 0.5 * (1.0 + lax.erf(up * (0.5 ** 0.5)))
        hd_scr[n_d + 2 * n_o:, :] = (up * cdf).astype(jnp.bfloat16)
        slope = cdf + up * (jnp.exp(-0.5 * up * up) * 0.3989422804014327)
        hd_scr[2 * n_qkv:n_d, :] = (d_hid * slope).astype(jnp.bfloat16)

        seg_row = seg_ref[pl.ds(row_of(step), 1), :]
        classes = lax.broadcasted_iota(jnp.int32, (16, seq_len), 0)
        one_hot = (classes == jnp.broadcast_to(seg_row, (16, seq_len))).astype(jnp.bfloat16)
        same = dot(one_hot, one_hot, TN) > 0.5
        key_id = lax.broadcasted_iota(jnp.int32, (seq_len, seq_len), 0)
        query_id = lax.broadcasted_iota(jnp.int32, (seq_len, seq_len), 1)
        allowed = (key_id <= query_id) & same
        for head in range(2):
            attend(head, qkv, d_attn, allowed)
        save(step, 1).start()

        @pl.when(pick(step, [int(SLOT[n] in SLOT[:n]) for n in range(steps)]) == 1)
        def _():
            for copy in slot_sends(slot):
                copy.wait()

        for h in range(0, hidden, cols_step):
            cols = slice(h, h + cols_step)
            stage[slot, 0, :, cols] = dot(hd_scr[n_d:, :], w_out[:, cols], TN).astype(jnp.bfloat16)
            stage[slot, 1, :, cols] = dot(hd_scr[:n_d, :], w_in[:, cols], TN).astype(jnp.bfloat16)

        for n in range(steps - 1):
            @pl.when(step == n)
            def _():
                for work in EVENTS[n]:
                    event(*work)
        return carry

    lax.fori_loop(0, steps, row_step, 0)
    last, buf = SLOT[-1], (steps - 1) % 2
    dgain_ref[...] = jnp.zeros_like(dgain_ref)
    fine = min(mid, 32)

    def finish(piece):
        def tile(n, d_gain):
            at = pl.ds(pl.multiple_of(piece * mid + n * fine, fine), fine)
            x_f32 = x_buf[buf, at, :].astype(jnp.float32)
            normed, inv_std = norm_rows(x_f32)
            grad = stage[last, 1, at, :].astype(jnp.float32)
            stage[last, 0, at, :] = (x_f32 + stage[last, 0, at, :].astype(jnp.float32)).astype(jnp.bfloat16)
            d_hat = grad * gain
            d_x = inv_std * (d_hat - jnp.mean(d_hat, axis=-1, keepdims=True) - normed * jnp.mean(d_hat * normed, axis=-1, keepdims=True))
            stage[last, 1, at, :] = (dy_buf[buf, at, :].astype(jnp.float32) + d_x).astype(jnp.bfloat16)
            return d_gain + jnp.sum(grad * normed, axis=0, keepdims=True)

        dgain_ref[...] += lax.fori_loop(0, mid // fine, tile, jnp.zeros((1, hidden), jnp.float32))
        copies = [pltpu.make_async_copy(piece_of(stage.at[last, t], piece), piece_of(dst, piece), end_sem.at[piece, t])
                  for t, dst in ((0, y_own), (1, dx_own))]
        for copy in copies:
            copy.start()
        return copies

    ends = []
    ended = {0: 0, 1: 0}
    for work in EVENTS[-1]:
        event(*work)
        n, _, piece, ring = work
        if n == steps - 1 and ring == 2:
            ended[piece] += 1
            if ended[piece] == 2:
                ends += finish(piece)
    for slot in range(SLOTS):
        if slot != last:
            for copy in slot_sends(slot):
                copy.wait()
    for copy in ends + [save(steps - 1, n) for n in range(2)]:
        copy.wait()


def gather_kernel(n_parts, y_own, dx_own, dgain_ref, dy_hbm, a_all, hd_all, y_lo, y_hi, dx_all, dgain_out, grads, d_up,
                  gain_scr, acc, g_recv, a_buf, dy_buf, hd_buf, send_sem, link_sem, pair_sem, pair_recv, own_sem,
                  load_sem, g_send, g_land, g_free, dg_send, dg_recv):
    place = Place()
    core = place.core
    _, seq_len, hidden = dx_all.shape
    mid = seq_len // 2
    links = (('x', 1), ('x', -1), ('y', 1), ('y', -1))
    peers = [place.peer(a, o) for a in ('x', 'y') for o in (1, -1)] + [place.sibling()]
    pl.semaphore_wait(greet(peers), len(peers))

    issued = {link: [] for link in links}
    sends = []

    def row_index(t, d_1, d_2):
        return place.index(d_1 % RING, d_2 % RING) if t == 0 else place.index(d_2 % RING, d_1 % RING)

    def spot_of(t, row, piece):
        if t == 1:
            return dx_all.at[row, pl.ds(piece * mid, mid)]
        return (y_lo, y_hi)[piece].at[row]

    def source(t, d_1, d_2, piece):
        if (d_1, d_2) == (0, 0):
            return (y_own, dx_own)[t].at[pl.ds(piece * mid, mid)]
        return spot_of(t, row_index(t, d_1, d_2), piece)

    def issue(link, t, d_1, d_2, piece):
        n = len(issued[link])
        which = links.index(link)
        copy = remote(source(t, d_1, d_2, piece), spot_of(t, row_index(t, d_1, d_2), piece),
                      send_sem.at[which, n], link_sem.at[which, n], place.peer(*link))
        copy.start()
        sends.append(copy)
        issued[link].append((t, d_1, d_2, piece))

    def pair(t, d_1, d_2, piece):
        slot = ((d_1 % RING) * RING + d_2 % RING) * 2 + piece
        copy = remote(source(t, d_1, d_2, piece), spot_of(t, row_index(t, d_1, d_2), piece),
                      pair_sem.at[t, slot], pair_recv.at[t, piece], place.sibling())
        copy.start()
        sends.append(copy)

    axes = (('y', 'x'), ('x', 'y'))
    for ring in range(2):
        for n in range(2):
            for t in range(2):
                for way in (1, -1):
                    issue((axes[t][ring], way), t, 0, 0, n if way == 1 else 1 - n)
    locals_ = []
    for t in range(2):
        for piece in range(2):
            pair(t, 0, 0, piece)
            copy = pltpu.make_async_copy(source(t, 0, 0, piece), spot_of(t, place.me, piece), own_sem.at[t, piece])
            copy.start()
            locals_.append(copy)

    depth, _, group = a_buf.shape
    rows = a_all.shape[0]
    groups = hidden // group
    n_qkv, n_up, n_o, n_dn = n_parts
    n_d = 2 * (n_qkv + n_up)
    segments, at, to = [], 0, 0
    for size in n_parts:
        segments.append((at, to, size))
        at, to = at + 2 * size, to + size

    def loads(count):
        slot, r = count % depth, count % rows
        cols = pl.ds(pl.multiple_of(count // rows * group, group), group)
        return (pltpu.make_async_copy(a_all.at[r, :, cols], a_buf.at[slot], load_sem.at[slot, 0]),
                pltpu.make_async_copy(dy_hbm.at[2 * r + core, :, cols], dy_buf.at[slot], load_sem.at[slot, 1]),
                pltpu.make_async_copy(hd_all.at[r, pl.ds(0, n_d)], hd_buf.at[slot, pl.ds(0, n_d)], load_sem.at[slot, 2]),
                pltpu.make_async_copy(hd_all.at[r, pl.ds(n_d, hd_all.shape[1] - n_d)],
                                      hd_buf.at[slot, pl.ds(n_d, hd_all.shape[1] - n_d)], load_sem.at[slot, 3]))

    def swap_grads(n):
        return [remote(rows_at(acc, at + (1 - core) * size, size), g_recv.at[pl.ds(to, size)],
                       g_send.at[m], g_land.at[m], place.sibling()) for m, (at, to, size) in enumerate(segments)]

    for count in range(depth - 1):
        for copy in loads(count):
            copy.start()

    def sum_rows(n, half):
        if half == 0:
            acc[...] = jnp.zeros_like(acc)

        def add_row(i, carry):
            count = n * rows + i
            slot = count % depth
            for copy in loads(count):
                copy.wait()

            @pl.when(count + depth - 1 < groups * rows)
            def _():
                for copy in loads(count + depth - 1):
                    copy.start()

            acc[:n_d, :] += dot(hd_buf[slot, :n_d, :], a_buf[slot], NN)
            acc[n_d:, :] += dot(hd_buf[slot, n_d:, :], dy_buf[slot], NN)
            return carry

        lax.fori_loop(half * (rows // 2), (half + 1) * (rows // 2), add_row, 0)
        if half == 1:
            if n > 0:
                pl.semaphore_wait(g_free, 1)
            for copy in swap_grads(n):
                copy.start()

    def end_rows(n):
        for copy in swap_grads(n):
            copy.wait()
        for m, (at, to, size) in enumerate(segments):
            total = rows_at(acc, at + core * size, size)[...] + g_recv[to:to + size, :]
            if m == 1:
                d_up[n * group:(n + 1) * group, :] = total.T.astype(d_up.dtype)
            else:
                spot = to if m == 0 else to - n_up
                grads[spot:spot + size, n * group:(n + 1) * group] = total.astype(grads.dtype)
        if n + 1 < groups:
            pl.semaphore_signal(g_free, inc=1, device_id={'model': place.sibling()}, device_id_type=MESH)

    total = dgain_ref[...]
    for n, axis in enumerate(('core', 'x', 'x', 'y', 'y')):
        at = {'core': core, 'x': place.x, 'y': place.y}[axis]
        other = (RING - 1 - at) if n in (2, 4) else at + 1 - 2 * (at % 2)
        device = place.sibling() if axis == 'core' else place.peer(axis, other - at)
        gain_scr[n, 0] = total
        copy = remote(gain_scr.at[n, 0], gain_scr.at[n, 1], dg_send.at[n], dg_recv.at[n], device)
        copy.start()
        copy.wait()
        total = gain_scr[n, 0] + gain_scr[n, 1]
    dgain_out[...] = jnp.sum(total, axis=0).astype(dgain_out.dtype)

    rounds = RING * RING - 1
    assert 2 * groups < rounds
    for n in range(rounds):
        if n > 0 and n % 2 == 0 and n <= 2 * groups:
            end_rows(n // 2 - 1)
        if n < 2 * groups:
            sum_rows(n // 2, n % 2)
        for link in links:
            t, d_1, d_2, piece = issued[link][n]
            axis, way = link
            on_first = axis == axes[t][0]
            d_1, d_2 = (d_1 - way, d_2) if on_first else (d_1, d_2 - way)
            landed(spot_of(t, row_index(t, d_1, d_2), piece), link_sem.at[links.index(link), n])
            along = d_1 if on_first else d_2
            if abs(along) == 1 and piece == (0 if way == 1 else 1):
                issue(link, t, d_1, d_2, piece)
            if on_first:
                for other in (1, -1):
                    issue((axes[t][1], other), t, d_1, d_2, piece)
            pair(t, d_1, d_2, piece)

    for t in range(2):
        for piece in range(2):
            theirs = dx_all.at[pl.ds(0, RING * RING), pl.ds(piece * mid, mid)] if t else (y_lo, y_hi)[piece].at[pl.ds(0, RING * RING)]
            landed(theirs, pair_recv.at[t, piece])
    for copy in sends:
        copy.wait_send()
    for copy in locals_:
        copy.wait()


def place_kernel(y_lo, y_hi, dx_all, grads, d_up, dgain, y_out, dx_out, d_wqkv, d_wout, d_wdown, d_wup, dgain_out, bounce, in_sem, out_sem, sem):
    rows, mid, _ = y_lo.shape
    n_qkv, n_o, n_dn = d_wqkv.shape[0], d_wout.shape[0], d_wdown.shape[0]
    bufs, per = bounce.shape[0], bounce.shape[1]
    count = rows // per
    loads = [pltpu.make_async_copy(y_hi.at[pl.ds(n * per, per)], bounce.at[n % bufs], in_sem.at[n % bufs]) for n in range(count)]
    stores = [pltpu.make_async_copy(bounce.at[n % bufs], y_out.at[pl.ds(n * per, per), pl.ds(mid, mid)], out_sem.at[n % bufs]) for n in range(count)]
    for n in range(min(bufs, count)):
        loads[n].start()
    split = 4
    part = rows // split
    direct = []
    for n in range(split):
        at = pl.ds(n * part, part)
        direct += [(dx_all.at[at], dx_out.at[at]), (y_lo.at[at], y_out.at[at, pl.ds(0, mid)])]
    direct += [(grads.at[pl.ds(0, n_qkv)], d_wqkv),
               (grads.at[pl.ds(n_qkv, n_o)], d_wout), (grads.at[pl.ds(n_qkv + n_o, n_dn)], d_wdown), (d_up, d_wup)]
    copies = [pltpu.make_async_copy(src, dst, sem.at[n]) for n, (src, dst) in enumerate(direct)]
    for copy in copies:
        copy.start()
    dgain_out[...] = dgain[...]
    for n in range(count):
        loads[n].wait()
        stores[n].start()
        if n >= 1 and n - 1 + bufs < count:
            stores[n - 1].wait()
            loads[n - 1 + bufs].start()
    for n in range(max(0, count - bufs), count):
        stores[n].wait()
    for copy in copies:
        copy.wait()


def solution(mesh):
    devices = mesh.shape['model']
    assert devices == 2 * RING * RING

    def body(x_in, seg_ids, ln_gain, w_qkv, w_out, w_up, w_down, dy_in):
        rows, seq_len, hidden = x_in.shape
        assert rows == devices
        wqkv = w_qkv.transpose(1, 2, 3, 0).reshape(-1, hidden)
        wo = w_out.reshape(-1, hidden)
        n_parts = (wqkv.shape[0], w_up.shape[1], wo.shape[0], w_down.shape[0])
        n_in, n_out = n_parts[0] + n_parts[1], n_parts[2] + n_parts[3]
        n_all, n_up = n_in + n_out, n_parts[1]
        bf16, f32 = jnp.bfloat16, jnp.float32
        vmem, anywhere = pl.BlockSpec(memory_space=pltpu.VMEM), pl.BlockSpec(memory_space=pl.ANY)
        dma = pltpu.SemaphoreType.DMA
        shape = jax.ShapeDtypeStruct
        chips, mid, group = RING * RING, seq_len // 2, hidden // 4
        fixed = lambda array: pltpu.with_memory_space_constraint(array, pltpu.VMEM)
        y_own, dx_own, d_gain, a_all, hd_all = pl.pallas_call(
            reduce_kernel,
            in_specs=[anywhere, anywhere, vmem, vmem] + [anywhere] * 4,
            out_specs=[anywhere, anywhere, vmem, anywhere, anywhere],
            out_shape=[shape((seq_len, hidden), bf16), shape((seq_len, hidden), bf16), shape((1, hidden), f32),
                       shape((chips, seq_len, hidden), bf16), shape((chips, 2 * n_all, seq_len), bf16)],
            scratch_shapes=[
                pltpu.VMEM((2 * n_in, hidden), bf16), pltpu.VMEM((2 * n_out, hidden), bf16), pltpu.VMEM((hidden, n_up), bf16),
                pltpu.VMEM((2, seq_len, hidden), bf16), pltpu.VMEM((2, seq_len, hidden), bf16),
                pltpu.VMEM((seq_len, hidden), bf16), pltpu.VMEM((2 * n_all, seq_len), bf16),
                pltpu.VMEM((SLOTS, 2, seq_len, hidden), bf16),
                pltpu.VMEM((2, RING + 1, 2, mid, hidden), bf16),
                pltpu.VMEM((2, RING + 1, 2, seq_len, hidden), bf16),
                dma((2, 2)), dma((4,)), dma((4,)), dma((4,)), dma((SLOTS, 2, 2)),
                dma((2, RING + 1, 2)), dma((2, RING + 1, 2, 2)), dma((2, 2)), dma((2,)),
            ],
            compiler_params=pltpu.CompilerParams(collective_id=0, has_side_effects=True, vmem_limit_bytes=VMEM_LIMIT),
            name="rows_reduce",
        )(x_in, dy_in, seg_ids, ln_gain, wqkv, w_up, wo, w_down)

        per_link, depth = chips - 1, 3
        y_lo, y_hi, dx_all, d_gain, grads, d_up = pl.pallas_call(
            lambda *refs: gather_kernel(n_parts, *refs),
            in_specs=[anywhere, anywhere, vmem, anywhere, anywhere, anywhere],
            out_specs=[vmem, anywhere, vmem, vmem, vmem, vmem],
            out_shape=[pltpu.VMEM((rows, mid, hidden), bf16), shape((rows, mid, hidden), bf16), pltpu.VMEM((rows, seq_len, hidden), bf16),
                       pltpu.VMEM((hidden,), bf16), pltpu.VMEM((n_all - n_up, hidden), bf16), pltpu.VMEM((hidden, n_up), bf16)],
            scratch_shapes=[
                pltpu.VMEM((5, 2, 1, hidden), f32), pltpu.VMEM((2 * n_all, group), f32), pltpu.VMEM((n_all, group), f32),
                pltpu.VMEM((depth, seq_len, group), bf16), pltpu.VMEM((depth, seq_len, group), bf16),
                pltpu.VMEM((depth, 2 * n_all, seq_len), bf16),
                dma((4, per_link)), dma((4, per_link)), dma((2, 2 * chips)), dma((2, 2)), dma((2, 2)),
                dma((depth, 4)), dma((4,)), dma((4,)), pltpu.SemaphoreType.REGULAR, dma((5,)), dma((5,)),
            ],
            compiler_params=pltpu.CompilerParams(collective_id=1, has_side_effects=True, vmem_limit_bytes=LANDING_LIMIT),
            name="rows_gather",
        )(y_own, dx_own, d_gain, dy_in, a_all, hd_all)

        bufs = 6
        y_out, dx_out, d_wqkv, d_wout, d_wdown, d_wup, d_gain = pl.pallas_call(
            place_kernel,
            in_specs=[vmem, anywhere, vmem, vmem, vmem, vmem],
            out_specs=[anywhere] * 6 + [vmem],
            out_shape=[shape(x_in.shape, bf16), shape(x_in.shape, bf16), shape(wqkv.shape, bf16), shape(wo.shape, bf16),
                       shape(w_down.shape, bf16), shape(w_up.shape, bf16), shape((hidden,), bf16)],
            scratch_shapes=[pltpu.VMEM((bufs, 2, mid, hidden), bf16), dma((bufs,)), dma((bufs,)), dma((12,))],
            compiler_params=pltpu.CompilerParams(vmem_limit_bytes=LANDING_LIMIT),
            name="rows_place",
        )(fixed(y_lo), pltpu.with_memory_space_constraint(y_hi, pltpu.HBM), fixed(dx_all), fixed(grads), fixed(d_up), fixed(d_gain))
        d_wqkv = d_wqkv.reshape(w_qkv.shape[1:] + (hidden,)).transpose(3, 0, 1, 2)
        return y_out, dx_out, d_gain, d_wqkv, d_wout.reshape(w_out.shape), d_wup, d_wdown

    in_specs = (P('data'), P('data'), P(), P(None, 'model'), P('model'), P(None, 'model'), P('model'), P('data'))
    out_specs = (P('data'), P('data'), P('data'), P('data', 'model'), P(('data', 'model')), P('data', 'model'), P(('data', 'model')))
    return jax.shard_map(body, mesh=mesh, in_specs=in_specs, out_specs=out_specs, check_vma=False)
```

```python
import functools

import jax
import jax.numpy as jnp
from jax import lax
from jax.experimental import pallas as pl
from jax.experimental.pallas import tpu as pltpu
from jax.sharding import PartitionSpec as P

LN_EPS = 1e-5
RING = 4
MESH = pl.DeviceIdType.MESH
NT = (((1,), (1,)), ((), ()))
NN = (((1,), (0,)), ((), ()))
TN = (((0,), (0,)), ((), ()))
ORDER = ((2, 2), (1, 2), (2, 3), (2, 1), (3, 2), (3, 3), (1, 1), (0, 2),
         (2, 0), (0, 1), (3, 1), (1, 3), (1, 0), (3, 0), (0, 3), (0, 0))
SLOT = (0, 1, 2, 3, 4, 0, 1, 2, 3, 4, 1, 0, 2, 3, 0, 1)
SLOTS = max(SLOT) + 1
PASS, LOAD, ADD = range(3)
EVENTS = (
    (((0, 0, 0, 1, PASS), (0, 0, 1, 1, PASS), (0, 1, 0, 1, PASS), (0, 1, 1, 1, PASS)),
     ()),
    (((1, 0, 0, 1, PASS), (1, 0, 1, 1, PASS), (1, 1, 1, 1, PASS)),
     ()),
    (((2, 0, 0, 1, PASS), (2, 1, 0, 1, PASS), (2, 1, 1, 1, PASS), (1, 1, 0, 1, PASS), (2, 0, 1, 1, PASS)),
     ()),
    (((3, 0, 1, 1, PASS), (3, 1, 0, 1, PASS), (3, 1, 1, 1, PASS), (3, 0, 0, 1, PASS)),
     ()),
    (((4, 0, 0, 1, PASS), (4, 0, 1, 1, PASS), (4, 1, 0, 1, PASS), (4, 1, 1, 1, PASS)),
     ()),
    (((5, 0, 0, 1, PASS), (5, 1, 0, 1, PASS), (5, 1, 1, 1, PASS)),
     ()),
    (((6, 0, 1, 1, PASS), (6, 1, 1, 1, PASS), (6, 0, 0, 1, PASS)),
     ()),
    (((7, 1, 0, 1, LOAD), (7, 0, 0, 1, PASS), (7, 0, 1, 1, PASS), (5, 0, 1, 1, PASS), (6, 1, 0, 1, PASS)),
     ((7, 1, 1, 1, LOAD), (7, 1, 0, 1, ADD), (7, 1, 0, 2, PASS))),
    (((8, 0, 0, 1, LOAD), (8, 1, 0, 1, PASS), (8, 1, 1, 1, PASS), (7, 1, 1, 1, ADD), (8, 0, 1, 1, LOAD), (7, 1, 1, 2, PASS)),
     ((8, 0, 0, 1, ADD), (8, 0, 0, 2, PASS), (8, 0, 1, 1, ADD), (8, 0, 1, 2, PASS))),
    (((9, 0, 1, 1, PASS),),
     ()),
    (((10, 0, 1, 1, PASS), (10, 1, 0, 1, PASS), (10, 1, 1, 1, PASS), (10, 0, 0, 1, PASS)),
     ()),
    (((11, 0, 0, 1, PASS), (11, 1, 1, 1, PASS), (11, 0, 1, 1, PASS), (11, 1, 0, 1, PASS), (9, 0, 0, 1, PASS)),
     ()),
    (((12, 1, 1, 1, PASS), (12, 1, 0, 1, PASS)),
     ()),
    (((12, 0, 0, 1, LOAD), (13, 1, 0, 1, PASS), (13, 1, 1, 1, PASS)),
     ((12, 0, 0, 1, ADD), (9, 1, 0, 1, LOAD), (12, 0, 0, 2, PASS))),
    (((14, 1, 1, 1, LOAD), (14, 0, 0, 1, PASS), (14, 0, 1, 1, PASS), (9, 1, 0, 1, ADD), (14, 1, 0, 1, LOAD), (9, 1, 0, 2, PASS)),
     ((14, 1, 1, 1, ADD), (12, 0, 1, 1, LOAD), (14, 1, 1, 2, PASS), (14, 1, 0, 1, ADD), (14, 1, 0, 2, PASS), (12, 0, 1, 1, ADD), (13, 0, 1, 1, LOAD), (12, 0, 1, 2, PASS), (13, 0, 1, 1, ADD), (9, 1, 1, 1, LOAD), (13, 0, 1, 2, PASS), (9, 1, 1, 1, ADD), (9, 1, 1, 2, PASS))),
    ((),
     ((13, 0, 0, 1, LOAD), (13, 0, 0, 1, ADD), (13, 0, 0, 2, PASS), (15, 1, 0, 1, LOAD), (15, 1, 0, 1, ADD), (15, 0, 0, 1, LOAD), (15, 0, 1, 1, LOAD), (15, 0, 0, 1, ADD), (15, 0, 1, 1, ADD), (15, 1, 1, 1, LOAD), (15, 1, 1, 1, ADD), (15, 0, 1, 2, PASS), (15, 1, 1, 2, PASS), (15, 1, 0, 2, PASS), (15, 0, 0, 2, PASS))),
)
VMEM_LIMIT = 60 * 2 ** 20
LANDING_LIMIT = 8 * 2 ** 20


def dot(lhs, rhs, dims):
    return lax.dot_general(lhs, rhs, dims, preferred_element_type=jnp.float32)


def norm_rows(x_f32):
    mean_val = jnp.mean(x_f32, axis=-1, keepdims=True)
    centered = x_f32 - mean_val
    inv_std = lax.rsqrt(jnp.mean(centered * centered, axis=-1, keepdims=True) + LN_EPS)
    return centered * inv_std, inv_std


class Place:
    def __init__(self):
        me = lax.axis_index('model')
        self.core = me % 2
        self.x = (me // 2) % RING
        self.y = me // (2 * RING)
        self.me = me

    def index(self, d_y, d_x, core=None):
        core = self.core if core is None else core
        return (((self.y + d_y) % RING) * RING + (self.x + d_x) % RING) * 2 + core

    def peer(self, axis, offset):
        return self.index(offset % RING, 0) if axis == 'y' else self.index(0, offset % RING)

    def sibling(self):
        return self.index(0, 0, 1 - self.core)


def remote(src, dst, send_sem, recv_sem, device):
    return pltpu.make_async_remote_copy(src_ref=src, dst_ref=dst, send_sem=send_sem, recv_sem=recv_sem,
                                        device_id={'model': device}, device_id_type=MESH)


def greet(peers):
    barrier = pltpu.get_barrier_semaphore()
    for peer in peers:
        pl.semaphore_signal(barrier, inc=1, device_id={'model': peer}, device_id_type=MESH)
    return barrier


def pick(step, values):
    out = jnp.int32(0)
    for n, value in enumerate(values):
        out = jnp.where(step == n, value, out)
    return out


def rows_at(ref, at, count):
    return ref.at[pl.ds(pl.multiple_of(at, 16), count)]


def landed(ref, sem):
    pltpu.make_async_copy(ref, ref, sem).wait()


def add_into(dst, *sources):
    rows = dst.shape[0]
    tile = min(rows, 32)

    def tile_add(n, carry):
        at = pl.ds(pl.multiple_of(n * tile, tile), tile)
        total = dst[at, :].astype(jnp.float32)
        for source in sources:
            total += source[at, :].astype(jnp.float32)
        dst[at, :] = total.astype(dst.dtype)
        return carry

    lax.fori_loop(0, rows // tile, tile_add, 0)


def reduce_kernel(x_hbm, dy_hbm, seg_ref, gain_ref, wqkv_hbm, w1_hbm, wo_hbm, w2_hbm,
                  y_own, dx_own, dgain_ref, g_own, g_sib, full,
                  w_in, w_out, w1_raw, acc, x_buf, dy_buf, a_scr, hd_scr, stage, half, last_full, tmp,
                  row_sem, w_sem, ws_sem, wr_sem, send_sem, half_sem, full_sem, tmp_sem, end_sem, out_sem):
    place = Place()
    core = place.core
    _, seq_len, hidden = x_buf.shape
    mid = seq_len // 2
    n_qkv, n_up, n_o, n_dn = wqkv_hbm.shape[0], w1_hbm.shape[1], wo_hbm.shape[0], w2_hbm.shape[0]
    n_d = 2 * (n_qkv + n_up)
    steps = len(ORDER)

    def row_of(step):
        return place.index(pick(step, [o[0] for o in ORDER]), pick(step, [o[1] for o in ORDER]))

    def row_copy(row, buf, n):
        return pltpu.make_async_copy((x_hbm, dy_hbm)[n].at[row], (x_buf, dy_buf)[n].at[buf], row_sem.at[buf, n])

    up_spot = rows_at(w_in, 2 * n_qkv + core * n_up, n_up)
    spots = ((wqkv_hbm, rows_at(w_in, core * n_qkv, n_qkv)), (wo_hbm, rows_at(w_out, core * n_o, n_o)),
             (w2_hbm, rows_at(w_out, 2 * n_o + core * n_dn, n_dn)))

    gain = gain_ref[...].astype(jnp.float32)[None, :]
    sub = min(seq_len, 64)

    def norm_row(buf):
        for t in range(0, seq_len, sub):
            normed, _ = norm_rows(x_buf[buf, t:t + sub, :].astype(jnp.float32))
            a_scr[t:t + sub, :] = (normed * gain).astype(jnp.bfloat16)

    peers = [place.peer('x', 1), place.peer('x', -1), place.peer('y', 1), place.peer('y', -1), place.sibling()]
    barrier = greet(peers)
    raw = pltpu.make_async_copy(w1_hbm, w1_raw, w_sem.at[3])
    raw.start()
    for n in range(2):
        row_copy(row_of(0), 0, n).start()
    mine = [pltpu.make_async_copy(src, dst, w_sem.at[n]) for n, (src, dst) in enumerate(spots)]
    for copy in mine:
        copy.start()
    raw.wait()
    turn = min(hidden, 256)
    for h in range(0, hidden, turn):
        up_spot[:, h:h + turn] = w1_raw[h:h + turn, :].T
    pl.semaphore_wait(barrier, len(peers))
    swaps = [remote(src, dst, ws_sem.at[n], wr_sem.at[n], place.sibling()) for n, (src, dst) in enumerate(spots)]
    swaps.append(remote(up_spot, up_spot, ws_sem.at[3], wr_sem.at[3], place.sibling()))
    for n in (0, 3, 1, 2):
        swaps[n].start()
    row_copy(0, 0, 0).wait()
    norm_row(0)
    acc[...] = jnp.zeros_like(acc)
    mine[0].wait()
    for n in (0, 3):
        swaps[n].wait()

    scale = n_o ** -0.5
    cols_step = min(hidden, 512)

    def piece_of(ref, piece):
        return ref.at[pl.ds(piece * mid, mid)]

    def slot_sends(slot):
        return [pltpu.make_async_copy(piece_of(stage.at[slot, t], piece), piece_of(stage.at[slot, t], piece),
                                      send_sem.at[slot, t, piece]) for t in range(2) for piece in range(2)]

    def event(n, t, piece, ring, kind):
        d_y, d_x = ORDER[n]
        first, second = (('x', d_x), ('y', d_y)) if t == 0 else (('y', d_y), ('x', d_x))
        (axis, offset), line = (first, second[1]) if ring == 1 else (second, RING)
        ahead, behind = place.peer(axis, 1), place.peer(axis, -1)
        spot = piece_of(stage.at[SLOT[n], t], piece)

        def send(dst, recv_sem, device):
            remote(spot, dst, send_sem.at[SLOT[n], t, piece], recv_sem, device).start()

        if offset == 2:
            send(half.at[t, line, piece], half_sem.at[t, line, piece], ahead if piece == 0 else behind)
        elif offset in (1, 3):
            side = 0 if offset == 1 else 1
            if side == piece:
                landed(half.at[t, line, piece], half_sem.at[t, line, piece])
                add_into(spot, half.at[t, line, piece])
            dst = last_full.at[t, side] if line == RING else full.at[t, line, side]
            send(piece_of(dst, piece), full_sem.at[t, line, side, piece], ahead if side == 0 else behind)
        elif line == RING:
            came = [piece_of(last_full.at[t, side], piece) for side in range(2)]
            for side in range(2):
                landed(came[side], full_sem.at[t, line, side, piece])
            add_into(spot, *came)
        else:
            loads = [pltpu.make_async_copy(piece_of(full.at[t, line, side], piece), tmp.at[piece, side], tmp_sem.at[piece, side])
                     for side in range(2)]
            if kind == LOAD:
                for side in range(2):
                    landed(piece_of(full.at[t, line, side], piece), full_sem.at[t, line, side, piece])
                    loads[side].start()
            else:
                for load in loads:
                    load.wait()
                add_into(spot, tmp.at[piece, 0], tmp.at[piece, 1])

    def grad_copies():
        copies = []
        for n, (side, dst) in enumerate(((core, g_own), (1 - core, g_sib))):
            at, to = 0, 0
            for m, size in enumerate((n_qkv, n_up, n_o, n_dn)):
                copies.append(pltpu.make_async_copy(rows_at(acc, at + side * size, size), dst.at[pl.ds(to, size)], out_sem.at[4 * n + m]))
                at, to = at + 2 * size, to + size
        return copies

    def attend(qkv, d_attn, allowed):
        heads = range(2)
        parts = [[qkv[head * n_qkv + n * n_o:head * n_qkv + (n + 1) * n_o] for n in range(3)] for head in heads]
        d_o = [d_attn[head * n_o:(head + 1) * n_o] for head in heads]
        raw = [dot(keys, query, TN) for query, keys, _ in parts]
        d_p = [dot(parts[head][2], d_o[head], TN) for head in heads]
        expd = []
        for head in heads:
            scores = jnp.where(allowed, raw[head] * scale, -1e30)
            expd.append(jnp.exp(scores - jnp.max(scores, axis=0, keepdims=True)))
        probs = [e / jnp.sum(e, axis=0, keepdims=True) for e in expd]
        probs_b = [p.astype(jnp.bfloat16) for p in probs]
        d_s = [(probs[head] * (d_p[head] - jnp.sum(d_p[head] * probs[head], axis=0, keepdims=True)) * scale).astype(jnp.bfloat16)
               for head in heads]
        for head in heads:
            at = head * n_qkv
            query, keys, values = parts[head]
            hd_scr[n_d + head * n_o:n_d + (head + 1) * n_o, :] = dot(values, probs_b[head], NN).astype(jnp.bfloat16)
            hd_scr[at + 2 * n_o:at + 3 * n_o, :] = dot(d_o[head], probs_b[head], NT).astype(jnp.bfloat16)
            hd_scr[at:at + n_o, :] = dot(keys, d_s[head], NN).astype(jnp.bfloat16)
            hd_scr[at + n_o:at + 2 * n_o, :] = dot(query, d_s[head], NT).astype(jnp.bfloat16)

    def row_step(step, carry):
        buf = step % 2
        slot = pick(step, SLOT)
        row = row_of(step)

        @pl.when(step > 0)
        def _():
            row_copy(row, buf, 0).wait()
            norm_row(buf)

        row_copy(row, buf, 1).wait()

        @pl.when(step + 1 < steps)
        def _():
            ahead = row_of(step + 1)
            for n in range(2):
                row_copy(ahead, 1 - buf, n).start()

        @pl.when(step == 0)
        def _():
            for copy in mine[1:] + swaps[1:3]:
                copy.wait()

        proj = dot(w_in[...], a_scr[...], NT)
        d_proj = dot(w_out[...], dy_buf[buf], NT).astype(jnp.bfloat16)
        qkv = proj[:2 * n_qkv].astype(jnp.bfloat16)
        up = proj[2 * n_qkv:].astype(jnp.bfloat16).astype(jnp.float32)
        d_attn = d_proj[:2 * n_o]
        d_hid = d_proj[2 * n_o:].astype(jnp.float32)
        cdf = 0.5 * (1.0 + lax.erf(up * (0.5 ** 0.5)))
        hd_scr[n_d + 2 * n_o:, :] = (up * cdf).astype(jnp.bfloat16)
        slope = cdf + up * (jnp.exp(-0.5 * up * up) * 0.3989422804014327)
        hd_scr[2 * n_qkv:n_d, :] = (d_hid * slope).astype(jnp.bfloat16)

        seg_row = seg_ref[pl.ds(row, 1), :]
        classes = lax.broadcasted_iota(jnp.int32, (16, seq_len), 0)
        one_hot = (classes == jnp.broadcast_to(seg_row, (16, seq_len))).astype(jnp.bfloat16)
        same = dot(one_hot, one_hot, TN) > 0.5
        key_id = lax.broadcasted_iota(jnp.int32, (seq_len, seq_len), 0)
        query_id = lax.broadcasted_iota(jnp.int32, (seq_len, seq_len), 1)
        allowed = (key_id <= query_id) & same
        attend(qkv, d_attn, allowed)

        @pl.when(pick(step, [int(SLOT[n] in SLOT[:n]) for n in range(steps)]) == 1)
        def _():
            for copy in slot_sends(slot):
                copy.wait()

        for h in range(0, hidden, cols_step):
            cols = slice(h, h + cols_step)
            stage[slot, 0, :, cols] = dot(hd_scr[n_d:, :], w_out[:, cols], TN).astype(jnp.bfloat16)
            stage[slot, 1, :, cols] = dot(hd_scr[:n_d, :], w_in[:, cols], TN).astype(jnp.bfloat16)

        def pass_on(when):
            for n in range(steps - 1):
                if EVENTS[n][when]:
                    @pl.when(step == n)
                    def _():
                        for work in EVENTS[n][when]:
                            event(*work)

        pass_on(0)
        for h in range(0, hidden, cols_step):
            cols = slice(h, h + cols_step)
            acc[:n_d, cols] += dot(hd_scr[:n_d, :], a_scr[:, cols], NN)
            acc[n_d:, cols] += dot(hd_scr[n_d:, :], dy_buf[buf, :, cols], NN)
        pass_on(1)
        return carry

    lax.fori_loop(0, steps, row_step, 0)
    last, buf = SLOT[-1], (steps - 1) % 2
    for copy in grad_copies():
        copy.start()
    dgain_ref[...] = jnp.zeros_like(dgain_ref)
    fine = min(mid, 32)

    def finish(piece):
        def tile(n, d_gain):
            at = pl.ds(pl.multiple_of(piece * mid + n * fine, fine), fine)
            x_f32 = x_buf[buf, at, :].astype(jnp.float32)
            normed, inv_std = norm_rows(x_f32)
            grad = stage[last, 1, at, :].astype(jnp.float32)
            stage[last, 0, at, :] = (x_f32 + stage[last, 0, at, :].astype(jnp.float32)).astype(jnp.bfloat16)
            d_hat = grad * gain
            d_x = inv_std * (d_hat - jnp.mean(d_hat, axis=-1, keepdims=True) - normed * jnp.mean(d_hat * normed, axis=-1, keepdims=True))
            stage[last, 1, at, :] = (dy_buf[buf, at, :].astype(jnp.float32) + d_x).astype(jnp.bfloat16)
            return d_gain + jnp.sum(grad * normed, axis=0, keepdims=True)

        dgain_ref[...] += lax.fori_loop(0, mid // fine, tile, jnp.zeros((1, hidden), jnp.float32))
        copies = [pltpu.make_async_copy(piece_of(stage.at[last, t], piece), piece_of(dst, piece), end_sem.at[piece, t])
                  for t, dst in ((0, y_own), (1, dx_own))]
        for copy in copies:
            copy.start()
        return copies

    ends = []
    ended = {0: 0, 1: 0}
    for work in EVENTS[-1][1]:
        event(*work)
        n, _, piece, ring, _ = work
        if n == steps - 1 and ring == 2:
            ended[piece] += 1
            if ended[piece] == 2:
                ends += finish(piece)
    for slot in range(SLOTS):
        if slot != last:
            for copy in slot_sends(slot):
                copy.wait()
    for copy in ends + grad_copies():
        copy.wait()


def gather_kernel(y_own, dx_own, dgain_ref, g_own, g_sib, y_lo, y_hi, dx_all, g_recv, dgain_out, grads, d_up,
                  gain_scr, g_buf, t_buf, send_sem, link_sem, pair_sem, pair_recv, own_sem, g_sem, gb_sem, dg_send, dg_recv):
    place = Place()
    core = place.core
    _, seq_len, hidden = dx_all.shape
    mid = seq_len // 2
    links = (('x', 1), ('x', -1), ('y', 1), ('y', -1))
    peers = [place.peer(a, o) for a in ('x', 'y') for o in (1, -1)] + [place.sibling()]
    pl.semaphore_wait(greet(peers), len(peers))

    issued = {link: [] for link in links}
    sends = []

    def row_index(t, d_1, d_2):
        return place.index(d_1 % RING, d_2 % RING) if t == 0 else place.index(d_2 % RING, d_1 % RING)

    def spot_of(t, row, piece):
        if t == 1:
            return dx_all.at[row, pl.ds(piece * mid, mid)]
        return (y_lo, y_hi)[piece].at[row]

    def source(t, d_1, d_2, piece):
        if (d_1, d_2) == (0, 0):
            return (y_own, dx_own)[t].at[pl.ds(piece * mid, mid)]
        return spot_of(t, row_index(t, d_1, d_2), piece)

    def issue(link, t, d_1, d_2, piece):
        n = len(issued[link])
        which = links.index(link)
        copy = remote(source(t, d_1, d_2, piece), spot_of(t, row_index(t, d_1, d_2), piece),
                      send_sem.at[which, n], link_sem.at[which, n], place.peer(*link))
        copy.start()
        sends.append(copy)
        issued[link].append((t, d_1, d_2, piece))

    def pair(t, d_1, d_2, piece):
        slot = ((d_1 % RING) * RING + d_2 % RING) * 2 + piece
        copy = remote(source(t, d_1, d_2, piece), spot_of(t, row_index(t, d_1, d_2), piece),
                      pair_sem.at[t, slot], pair_recv.at[t, piece], place.sibling())
        copy.start()
        sends.append(copy)

    axes = (('y', 'x'), ('x', 'y'))
    for ring in range(2):
        for n in range(2):
            for t in range(2):
                for way in (1, -1):
                    issue((axes[t][ring], way), t, 0, 0, n if way == 1 else 1 - n)
    locals_ = []
    for t in range(2):
        for piece in range(2):
            pair(t, 0, 0, piece)
            copy = pltpu.make_async_copy(source(t, 0, 0, piece), spot_of(t, place.me, piece), own_sem.at[t, piece])
            copy.start()
            locals_.append(copy)

    g_copy = remote(g_sib, g_recv, g_sem.at[0], g_sem.at[1], place.sibling())
    g_copy.start()

    tile, turn = g_buf.shape[1], t_buf.shape[2]
    n_up = d_up.shape[1]
    n_qkv = 3 * tile

    def grad_tile(at, to):
        loads = [pltpu.make_async_copy(g.at[pl.ds(at, tile)], g_buf.at[n], gb_sem.at[n]) for n, g in enumerate((g_own, g_recv))]
        for load in loads:
            load.start()
        for load in loads:
            load.wait()
        grads[to:to + tile, :] = (g_buf[0] + g_buf[1]).astype(grads.dtype)

    def up_tile(h):
        loads = [pltpu.make_async_copy(g.at[pl.ds(n_qkv, n_up), pl.ds(h, turn)], t_buf.at[n], gb_sem.at[n])
                 for n, g in enumerate((g_own, g_recv))]
        for load in loads:
            load.start()
        for load in loads:
            load.wait()
        d_up[h:h + turn, :] = (t_buf[0] + t_buf[1]).T.astype(d_up.dtype)

    jobs = [functools.partial(grad_tile, at, at) for at in range(0, n_qkv, tile)]
    jobs += [functools.partial(grad_tile, at, at - n_up) for at in range(n_qkv + n_up, g_own.shape[0], tile)]
    jobs += [functools.partial(up_tile, h) for h in range(0, hidden, turn)]

    total = dgain_ref[...]
    for n, axis in enumerate(('core', 'x', 'x', 'y', 'y')):
        at = {'core': core, 'x': place.x, 'y': place.y}[axis]
        other = (RING - 1 - at) if n in (2, 4) else at + 1 - 2 * (at % 2)
        device = place.sibling() if axis == 'core' else place.peer(axis, other - at)
        gain_scr[n, 0] = total
        copy = remote(gain_scr.at[n, 0], gain_scr.at[n, 1], dg_send.at[n], dg_recv.at[n], device)
        copy.start()
        copy.wait()
        total = gain_scr[n, 0] + gain_scr[n, 1]
    dgain_out[...] = jnp.sum(total, axis=0).astype(dgain_out.dtype)

    rounds = RING * RING - 1
    for n in range(rounds):
        for link in links:
            t, d_1, d_2, piece = issued[link][n]
            axis, way = link
            on_first = axis == axes[t][0]
            d_1, d_2 = (d_1 - way, d_2) if on_first else (d_1, d_2 - way)
            landed(spot_of(t, row_index(t, d_1, d_2), piece), link_sem.at[links.index(link), n])
            along = d_1 if on_first else d_2
            if abs(along) == 1 and piece == (0 if way == 1 else 1):
                issue(link, t, d_1, d_2, piece)
            if on_first:
                for other in (1, -1):
                    issue((axes[t][1], other), t, d_1, d_2, piece)
            pair(t, d_1, d_2, piece)
        if n == 2:
            g_copy.wait()
        if n >= 2:
            for job in jobs[2 * (n - 2):2 * (n - 1)]:
                job()

    for t in range(2):
        for piece in range(2):
            theirs = dx_all.at[pl.ds(0, RING * RING), pl.ds(piece * mid, mid)] if t else (y_lo, y_hi)[piece].at[pl.ds(0, RING * RING)]
            landed(theirs, pair_recv.at[t, piece])
    for copy in sends:
        copy.wait_send()
    for copy in locals_:
        copy.wait()


def place_kernel(y_lo, y_hi, dx_all, grads, d_up, dgain, y_out, dx_out, d_wqkv, d_wout, d_wdown, d_wup, dgain_out, bounce, in_sem, out_sem, sem):
    rows, mid, _ = y_lo.shape
    n_qkv, n_o, n_dn = d_wqkv.shape[0], d_wout.shape[0], d_wdown.shape[0]
    bufs, per = bounce.shape[0], bounce.shape[1]
    count = rows // per
    loads = [pltpu.make_async_copy(y_hi.at[pl.ds(n * per, per)], bounce.at[n % bufs], in_sem.at[n % bufs]) for n in range(count)]
    stores = [pltpu.make_async_copy(bounce.at[n % bufs], y_out.at[pl.ds(n * per, per), pl.ds(mid, mid)], out_sem.at[n % bufs]) for n in range(count)]
    for n in range(min(bufs, count)):
        loads[n].start()
    split = 4
    part = rows // split
    direct = []
    for n in range(split):
        at = pl.ds(n * part, part)
        direct += [(dx_all.at[at], dx_out.at[at]), (y_lo.at[at], y_out.at[at, pl.ds(0, mid)])]
    direct += [(grads.at[pl.ds(0, n_qkv)], d_wqkv),
               (grads.at[pl.ds(n_qkv, n_o)], d_wout), (grads.at[pl.ds(n_qkv + n_o, n_dn)], d_wdown), (d_up, d_wup)]
    copies = [pltpu.make_async_copy(src, dst, sem.at[n]) for n, (src, dst) in enumerate(direct)]
    for copy in copies:
        copy.start()
    dgain_out[...] = dgain[...]
    for n in range(count):
        loads[n].wait()
        stores[n].start()
        if n >= 1 and n - 1 + bufs < count:
            stores[n - 1].wait()
            loads[n - 1 + bufs].start()
    for n in range(max(0, count - bufs), count):
        stores[n].wait()
    for copy in copies:
        copy.wait()


def solution(mesh):
    devices = mesh.shape['model']
    assert devices == 2 * RING * RING

    def body(x_in, seg_ids, ln_gain, w_qkv, w_out, w_up, w_down, dy_in):
        rows, seq_len, hidden = x_in.shape
        assert rows == devices
        wqkv = w_qkv.transpose(1, 2, 3, 0).reshape(-1, hidden)
        wo = w_out.reshape(-1, hidden)
        n_qkv, n_up, n_o, n_dn = wqkv.shape[0], w_up.shape[1], wo.shape[0], w_down.shape[0]
        n_in, n_out = n_qkv + n_up, n_o + n_dn
        n_all = n_in + n_out
        bf16, f32 = jnp.bfloat16, jnp.float32
        vmem, anywhere = pl.BlockSpec(memory_space=pltpu.VMEM), pl.BlockSpec(memory_space=pl.ANY)
        dma = pltpu.SemaphoreType.DMA
        shape = jax.ShapeDtypeStruct
        chips, mid = RING * RING, seq_len // 2
        fixed = lambda array: pltpu.with_memory_space_constraint(array, pltpu.VMEM)
        y_own, dx_own, d_gain, g_own, g_sib, _ = pl.pallas_call(
            reduce_kernel,
            in_specs=[anywhere, anywhere, vmem, vmem] + [anywhere] * 4,
            out_specs=[anywhere, anywhere, vmem, anywhere, anywhere, anywhere],
            out_shape=[shape((seq_len, hidden), bf16), shape((seq_len, hidden), bf16), shape((1, hidden), f32),
                       shape((n_all, hidden), f32), shape((n_all, hidden), f32), shape((2, RING, 2, seq_len, hidden), bf16)],
            scratch_shapes=[
                pltpu.VMEM((2 * n_in, hidden), bf16), pltpu.VMEM((2 * n_out, hidden), bf16), pltpu.VMEM((hidden, n_up), bf16),
                pltpu.VMEM((2 * n_all, hidden), f32),
                pltpu.VMEM((2, seq_len, hidden), bf16), pltpu.VMEM((2, seq_len, hidden), bf16),
                pltpu.VMEM((seq_len, hidden), bf16), pltpu.VMEM((2 * n_all, seq_len), bf16),
                pltpu.VMEM((SLOTS, 2, seq_len, hidden), bf16),
                pltpu.VMEM((2, RING + 1, 2, mid, hidden), bf16),
                pltpu.VMEM((2, 2, seq_len, hidden), bf16), pltpu.VMEM((2, 2, mid, hidden), bf16),
                dma((2, 2)), dma((4,)), dma((4,)), dma((4,)), dma((SLOTS, 2, 2)),
                dma((2, RING + 1, 2)), dma((2, RING + 1, 2, 2)), dma((2, 2)), dma((2, 2)), dma((8,)),
            ],
            compiler_params=pltpu.CompilerParams(collective_id=0, has_side_effects=True, vmem_limit_bytes=VMEM_LIMIT),
            name="rows_reduce",
        )(x_in, dy_in, seg_ids, ln_gain, wqkv, w_up, wo, w_down)

        per_link = chips - 1
        y_lo, y_hi, dx_all, _, d_gain, grads, d_up = pl.pallas_call(
            gather_kernel,
            in_specs=[anywhere, anywhere, vmem, anywhere, anywhere],
            out_specs=[vmem, anywhere, vmem, anywhere, vmem, vmem, vmem],
            out_shape=[pltpu.VMEM((rows, mid, hidden), bf16), shape((rows, mid, hidden), bf16), pltpu.VMEM((rows, seq_len, hidden), bf16),
                       shape(g_sib.shape, f32), pltpu.VMEM((hidden,), bf16),
                       pltpu.VMEM((n_all - n_up, hidden), bf16), pltpu.VMEM((hidden, n_up), bf16)],
            scratch_shapes=[
                pltpu.VMEM((5, 2, 1, hidden), f32), pltpu.VMEM((2, n_o, hidden), f32), pltpu.VMEM((2, n_up, min(hidden, 256)), f32),
                dma((4, per_link)), dma((4, per_link)), dma((2, 2 * chips)), dma((2, 2)), dma((2, 2)), dma((2,)), dma((2,)),
                dma((5,)), dma((5,)),
            ],
            compiler_params=pltpu.CompilerParams(collective_id=1, has_side_effects=True, vmem_limit_bytes=LANDING_LIMIT),
            name="rows_gather",
        )(y_own, dx_own, d_gain, g_own, g_sib)

        bufs = 6
        y_out, dx_out, d_wqkv, d_wout, d_wdown, d_wup, d_gain = pl.pallas_call(
            place_kernel,
            in_specs=[vmem, anywhere, vmem, vmem, vmem, vmem],
            out_specs=[anywhere] * 6 + [vmem],
            out_shape=[shape(x_in.shape, bf16), shape(x_in.shape, bf16), shape(wqkv.shape, bf16), shape(wo.shape, bf16),
                       shape(w_down.shape, bf16), shape(w_up.shape, bf16), shape((hidden,), bf16)],
            scratch_shapes=[pltpu.VMEM((bufs, 2, mid, hidden), bf16), dma((bufs,)), dma((bufs,)), dma((12,))],
            compiler_params=pltpu.CompilerParams(vmem_limit_bytes=LANDING_LIMIT),
            name="rows_place",
        )(fixed(y_lo), pltpu.with_memory_space_constraint(y_hi, pltpu.HBM), fixed(dx_all), fixed(grads), fixed(d_up), fixed(d_gain))
        d_wqkv = d_wqkv.reshape(w_qkv.shape[1:] + (hidden,)).transpose(3, 0, 1, 2)
        return y_out, dx_out, d_gain, d_wqkv, d_wout.reshape(w_out.shape), d_wup, d_wdown

    in_specs = (P('data'), P('data'), P(), P(None, 'model'), P('model'), P(None, 'model'), P('model'), P('data'))
    out_specs = (P('data'), P('data'), P('data'), P('data', 'model'), P(('data', 'model')), P('data', 'model'), P(('data', 'model')))
    return jax.shard_map(body, mesh=mesh, in_specs=in_specs, out_specs=out_specs, check_vma=False)
```

```python
import functools

import jax
import jax.numpy as jnp
from jax import lax
from jax.experimental import pallas as pl
from jax.experimental.pallas import tpu as pltpu
from jax.sharding import PartitionSpec as P

LN_EPS = 1e-5
RING = 4
MESH = pl.DeviceIdType.MESH
NT = (((1,), (1,)), ((), ()))
NN = (((1,), (0,)), ((), ()))
TN = (((0,), (0,)), ((), ()))
ORDER = ((2, 2), (1, 2), (2, 3), (2, 1), (3, 2), (3, 3), (1, 1), (0, 2),
         (2, 0), (0, 1), (3, 1), (1, 3), (1, 0), (3, 0), (0, 3), (0, 0))
SLOT = (0, 1, 2, 3, 4, 0, 1, 2, 3, 4, 1, 0, 2, 3, 0, 1)
SLOTS = max(SLOT) + 1
PASS, LOAD, ADD = range(3)
EVENTS = (
    (((0, 0, 0, 1, PASS), (0, 0, 1, 1, PASS), (0, 1, 0, 1, PASS), (0, 1, 1, 1, PASS)),
     ()),
    (((1, 0, 0, 1, PASS), (1, 0, 1, 1, PASS), (1, 1, 1, 1, PASS)),
     ()),
    (((2, 0, 0, 1, PASS), (2, 1, 0, 1, PASS), (2, 1, 1, 1, PASS), (1, 1, 0, 1, PASS), (2, 0, 1, 1, PASS)),
     ()),
    (((3, 0, 1, 1, PASS), (3, 1, 0, 1, PASS), (3, 1, 1, 1, PASS), (3, 0, 0, 1, PASS)),
     ()),
    (((4, 0, 0, 1, PASS), (4, 0, 1, 1, PASS), (4, 1, 0, 1, PASS), (4, 1, 1, 1, PASS)),
     ()),
    (((5, 0, 0, 1, PASS), (5, 1, 0, 1, PASS), (5, 1, 1, 1, PASS)),
     ()),
    (((6, 0, 1, 1, PASS), (6, 1, 1, 1, PASS), (6, 0, 0, 1, PASS)),
     ()),
    (((7, 1, 0, 1, LOAD), (7, 0, 0, 1, PASS), (7, 0, 1, 1, PASS), (5, 0, 1, 1, PASS), (6, 1, 0, 1, PASS)),
     ((7, 1, 1, 1, LOAD), (7, 1, 0, 1, ADD), (7, 1, 0, 2, PASS))),
    (((8, 0, 0, 1, LOAD), (8, 1, 0, 1, PASS), (8, 1, 1, 1, PASS), (7, 1, 1, 1, ADD), (8, 0, 1, 1, LOAD), (7, 1, 1, 2, PASS)),
     ((8, 0, 0, 1, ADD), (8, 0, 0, 2, PASS), (8, 0, 1, 1, ADD), (8, 0, 1, 2, PASS))),
    (((9, 0, 1, 1, PASS),),
     ()),
    (((10, 0, 1, 1, PASS), (10, 1, 0, 1, PASS), (10, 1, 1, 1, PASS), (10, 0, 0, 1, PASS)),
     ()),
    (((11, 0, 0, 1, PASS), (11, 1, 1, 1, PASS), (11, 0, 1, 1, PASS), (11, 1, 0, 1, PASS), (9, 0, 0, 1, PASS)),
     ()),
    (((12, 1, 1, 1, PASS), (12, 1, 0, 1, PASS)),
     ()),
    (((12, 0, 0, 1, LOAD), (13, 1, 0, 1, PASS), (13, 1, 1, 1, PASS)),
     ((12, 0, 0, 1, ADD), (9, 1, 0, 1, LOAD), (12, 0, 0, 2, PASS))),
    (((14, 1, 1, 1, LOAD), (14, 0, 0, 1, PASS), (14, 0, 1, 1, PASS), (9, 1, 0, 1, ADD), (14, 1, 0, 1, LOAD), (9, 1, 0, 2, PASS)),
     ((14, 1, 1, 1, ADD), (12, 0, 1, 1, LOAD), (14, 1, 1, 2, PASS), (14, 1, 0, 1, ADD), (14, 1, 0, 2, PASS), (12, 0, 1, 1, ADD), (13, 0, 1, 1, LOAD), (12, 0, 1, 2, PASS), (13, 0, 1, 1, ADD), (9, 1, 1, 1, LOAD), (13, 0, 1, 2, PASS), (9, 1, 1, 1, ADD), (9, 1, 1, 2, PASS))),
    ((),
     ((13, 0, 0, 1, LOAD), (13, 0, 0, 1, ADD), (13, 0, 0, 2, PASS), (15, 1, 0, 1, LOAD), (15, 1, 0, 1, ADD), (15, 0, 0, 1, LOAD), (15, 0, 1, 1, LOAD), (15, 0, 0, 1, ADD), (15, 0, 1, 1, ADD), (15, 1, 1, 1, LOAD), (15, 1, 1, 1, ADD), (15, 0, 1, 2, PASS), (15, 1, 1, 2, PASS), (15, 1, 0, 2, PASS), (15, 0, 0, 2, PASS))),
)
VMEM_LIMIT = 60 * 2 ** 20
LANDING_LIMIT = 8 * 2 ** 20


def dot(lhs, rhs, dims):
    return lax.dot_general(lhs, rhs, dims, preferred_element_type=jnp.float32)


def norm_rows(x_f32):
    mean_val = jnp.mean(x_f32, axis=-1, keepdims=True)
    centered = x_f32 - mean_val
    inv_std = lax.rsqrt(jnp.mean(centered * centered, axis=-1, keepdims=True) + LN_EPS)
    return centered * inv_std, inv_std


class Place:
    def __init__(self):
        me = lax.axis_index('model')
        self.core = me % 2
        self.x = (me // 2) % RING
        self.y = me // (2 * RING)
        self.me = me

    def index(self, d_y, d_x, core=None):
        core = self.core if core is None else core
        return (((self.y + d_y) % RING) * RING + (self.x + d_x) % RING) * 2 + core

    def peer(self, axis, offset):
        return self.index(offset % RING, 0) if axis == 'y' else self.index(0, offset % RING)

    def sibling(self):
        return self.index(0, 0, 1 - self.core)


def remote(src, dst, send_sem, recv_sem, device):
    return pltpu.make_async_remote_copy(src_ref=src, dst_ref=dst, send_sem=send_sem, recv_sem=recv_sem,
                                        device_id={'model': device}, device_id_type=MESH)


def greet(peers):
    barrier = pltpu.get_barrier_semaphore()
    for peer in peers:
        pl.semaphore_signal(barrier, inc=1, device_id={'model': peer}, device_id_type=MESH)
    return barrier


def pick(step, values):
    out = jnp.int32(0)
    for n, value in enumerate(values):
        out = jnp.where(step == n, value, out)
    return out


def rows_at(ref, at, count):
    return ref.at[pl.ds(pl.multiple_of(at, 16), count)]


def landed(ref, sem):
    pltpu.make_async_copy(ref, ref, sem).wait()


def add_into(dst, *sources):
    rows = dst.shape[0]
    tile = min(rows, 32)

    def tile_add(n, carry):
        at = pl.ds(pl.multiple_of(n * tile, tile), tile)
        total = dst[at, :].astype(jnp.float32)
        for source in sources:
            total += source[at, :].astype(jnp.float32)
        dst[at, :] = total.astype(dst.dtype)
        return carry

    lax.fori_loop(0, rows // tile, tile_add, 0)


def reduce_kernel(x_hbm, dy_hbm, seg_ref, gain_ref, wqkv_hbm, w1_hbm, wo_hbm, w2_hbm,
                  y_own, dx_own, dgain_ref, g_own, g_sib, full,
                  w_in, w_out, w1_raw, acc, x_buf, dy_buf, a_scr, hd_scr, stage, half, last_full, tmp,
                  row_sem, w_sem, ws_sem, wr_sem, send_sem, half_sem, full_sem, tmp_sem, end_sem, out_sem):
    place = Place()
    core = place.core
    _, seq_len, hidden = x_buf.shape
    mid = seq_len // 2
    n_qkv, n_up, n_o, n_dn = wqkv_hbm.shape[0], w1_hbm.shape[1], wo_hbm.shape[0], w2_hbm.shape[0]
    n_d = 2 * (n_qkv + n_up)
    steps = len(ORDER)

    def row_of(step):
        return place.index(pick(step, [o[0] for o in ORDER]), pick(step, [o[1] for o in ORDER]))

    def row_copy(row, buf, n):
        return pltpu.make_async_copy((x_hbm, dy_hbm)[n].at[row], (x_buf, dy_buf)[n].at[buf], row_sem.at[buf, n])

    up_spot = rows_at(w_in, 2 * n_qkv + core * n_up, n_up)
    spots = ((wqkv_hbm, rows_at(w_in, core * n_qkv, n_qkv)), (wo_hbm, rows_at(w_out, core * n_o, n_o)),
             (w2_hbm, rows_at(w_out, 2 * n_o + core * n_dn, n_dn)))

    gain = gain_ref[...].astype(jnp.float32)[None, :]
    sub = min(seq_len, 64)

    def norm_row(buf):
        for t in range(0, seq_len, sub):
            normed, _ = norm_rows(x_buf[buf, t:t + sub, :].astype(jnp.float32))
            a_scr[t:t + sub, :] = (normed * gain).astype(jnp.bfloat16)

    peers = [place.peer('x', 1), place.peer('x', -1), place.peer('y', 1), place.peer('y', -1), place.sibling()]
    barrier = greet(peers)
    raw = pltpu.make_async_copy(w1_hbm, w1_raw, w_sem.at[3])
    raw.start()
    for n in range(2):
        row_copy(row_of(0), 0, n).start()
    mine = [pltpu.make_async_copy(src, dst, w_sem.at[n]) for n, (src, dst) in enumerate(spots)]
    for copy in mine:
        copy.start()
    raw.wait()
    turn = min(hidden, 256)
    for h in range(0, hidden, turn):
        up_spot[:, h:h + turn] = w1_raw[h:h + turn, :].T
    pl.semaphore_wait(barrier, len(peers))
    swaps = [remote(src, dst, ws_sem.at[n], wr_sem.at[n], place.sibling()) for n, (src, dst) in enumerate(spots)]
    swaps.append(remote(up_spot, up_spot, ws_sem.at[3], wr_sem.at[3], place.sibling()))
    for n in (0, 3, 1, 2):
        swaps[n].start()
    row_copy(0, 0, 0).wait()
    norm_row(0)
    acc[...] = jnp.zeros_like(acc)
    mine[0].wait()
    for n in (0, 3):
        swaps[n].wait()

    scale = n_o ** -0.5
    cols_step = min(hidden, 512)

    def piece_of(ref, piece):
        return ref.at[pl.ds(piece * mid, mid)]

    def slot_sends(slot):
        return [pltpu.make_async_copy(piece_of(stage.at[slot, t], piece), piece_of(stage.at[slot, t], piece),
                                      send_sem.at[slot, t, piece]) for t in range(2) for piece in range(2)]

    def event(n, t, piece, ring, kind):
        d_y, d_x = ORDER[n]
        first, second = (('x', d_x), ('y', d_y)) if t == 0 else (('y', d_y), ('x', d_x))
        (axis, offset), line = (first, second[1]) if ring == 1 else (second, RING)
        ahead, behind = place.peer(axis, 1), place.peer(axis, -1)
        spot = piece_of(stage.at[SLOT[n], t], piece)

        def send(dst, recv_sem, device):
            remote(spot, dst, send_sem.at[SLOT[n], t, piece], recv_sem, device).start()

        if offset == 2:
            send(half.at[t, line, piece], half_sem.at[t, line, piece], ahead if piece == 0 else behind)
        elif offset in (1, 3):
            side = 0 if offset == 1 else 1
            if side == piece:
                landed(half.at[t, line, piece], half_sem.at[t, line, piece])
                add_into(spot, half.at[t, line, piece])
            dst = last_full.at[t, side] if line == RING else full.at[t, line, side]
            send(piece_of(dst, piece), full_sem.at[t, line, side, piece], ahead if side == 0 else behind)
        elif line == RING:
            came = [piece_of(last_full.at[t, side], piece) for side in range(2)]
            for side in range(2):
                landed(came[side], full_sem.at[t, line, side, piece])
            add_into(spot, *came)
        else:
            loads = [pltpu.make_async_copy(piece_of(full.at[t, line, side], piece), tmp.at[piece, side], tmp_sem.at[piece, side])
                     for side in range(2)]
            if kind == LOAD:
                for side in range(2):
                    landed(piece_of(full.at[t, line, side], piece), full_sem.at[t, line, side, piece])
                    loads[side].start()
            else:
                for load in loads:
                    load.wait()
                add_into(spot, tmp.at[piece, 0], tmp.at[piece, 1])

    def grad_copies():
        copies = []
        for n, (side, dst) in enumerate(((core, g_own), (1 - core, g_sib))):
            at, to = 0, 0
            for m, size in enumerate((n_qkv, n_up, n_o, n_dn)):
                copies.append(pltpu.make_async_copy(rows_at(acc, at + side * size, size), dst.at[pl.ds(to, size)], out_sem.at[4 * n + m]))
                at, to = at + 2 * size, to + size
        return copies

    def attend(qkv, d_attn, allowed):
        heads = range(2)
        parts = [[qkv[head * n_qkv + n * n_o:head * n_qkv + (n + 1) * n_o] for n in range(3)] for head in heads]
        d_o = [d_attn[head * n_o:(head + 1) * n_o] for head in heads]
        raw = [dot(keys, query, TN) for query, keys, _ in parts]
        d_p = [dot(parts[head][2], d_o[head], TN) for head in heads]
        expd = []
        for head in heads:
            scores = jnp.where(allowed, raw[head] * scale, -1e30)
            expd.append(jnp.exp(scores - jnp.max(scores, axis=0, keepdims=True)))
        probs = [e / jnp.sum(e, axis=0, keepdims=True) for e in expd]
        probs_b = [p.astype(jnp.bfloat16) for p in probs]
        d_s = [(probs[head] * (d_p[head] - jnp.sum(d_p[head] * probs[head], axis=0, keepdims=True)) * scale).astype(jnp.bfloat16)
               for head in heads]
        for head in heads:
            at = head * n_qkv
            query, keys, values = parts[head]
            hd_scr[n_d + head * n_o:n_d + (head + 1) * n_o, :] = dot(values, probs_b[head], NN).astype(jnp.bfloat16)
            hd_scr[at + 2 * n_o:at + 3 * n_o, :] = dot(d_o[head], probs_b[head], NT).astype(jnp.bfloat16)
            hd_scr[at:at + n_o, :] = dot(keys, d_s[head], NN).astype(jnp.bfloat16)
            hd_scr[at + n_o:at + 2 * n_o, :] = dot(query, d_s[head], NT).astype(jnp.bfloat16)

    def row_step(step, carry):
        buf = step % 2
        slot = pick(step, SLOT)
        row = row_of(step)

        @pl.when(step > 0)
        def _():
            row_copy(row, buf, 0).wait()
            norm_row(buf)

        row_copy(row, buf, 1).wait()

        @pl.when(step + 1 < steps)
        def _():
            ahead = row_of(step + 1)
            for n in range(2):
                row_copy(ahead, 1 - buf, n).start()

        @pl.when(step == 0)
        def _():
            for copy in mine[1:] + swaps[1:3]:
                copy.wait()

        proj = dot(w_in[...], a_scr[...], NT)
        d_proj = dot(w_out[...], dy_buf[buf], NT).astype(jnp.bfloat16)
        qkv = proj[:2 * n_qkv].astype(jnp.bfloat16)
        up = proj[2 * n_qkv:].astype(jnp.bfloat16).astype(jnp.float32)
        d_attn = d_proj[:2 * n_o]
        d_hid = d_proj[2 * n_o:].astype(jnp.float32)
        cdf = 0.5 * (1.0 + lax.erf(up * (0.5 ** 0.5)))
        hd_scr[n_d + 2 * n_o:, :] = (up * cdf).astype(jnp.bfloat16)
        slope = cdf + up * (jnp.exp(-0.5 * up * up) * 0.3989422804014327)
        hd_scr[2 * n_qkv:n_d, :] = (d_hid * slope).astype(jnp.bfloat16)

        seg_row = seg_ref[pl.ds(row, 1), :]
        classes = lax.broadcasted_iota(jnp.int32, (16, seq_len), 0)
        one_hot = (classes == jnp.broadcast_to(seg_row, (16, seq_len))).astype(jnp.bfloat16)
        same = dot(one_hot, one_hot, TN) > 0.5
        key_id = lax.broadcasted_iota(jnp.int32, (seq_len, seq_len), 0)
        query_id = lax.broadcasted_iota(jnp.int32, (seq_len, seq_len), 1)
        allowed = (key_id <= query_id) & same
        attend(qkv, d_attn, allowed)

        @pl.when(pick(step, [int(SLOT[n] in SLOT[:n]) for n in range(steps)]) == 1)
        def _():
            for copy in slot_sends(slot):
                copy.wait()

        for h in range(0, hidden, cols_step):
            cols = slice(h, h + cols_step)
            stage[slot, 0, :, cols] = dot(hd_scr[n_d:, :], w_out[:, cols], TN).astype(jnp.bfloat16)
            stage[slot, 1, :, cols] = dot(hd_scr[:n_d, :], w_in[:, cols], TN).astype(jnp.bfloat16)

        def pass_on(when):
            for n in range(steps - 1):
                if EVENTS[n][when]:
                    @pl.when(step == n)
                    def _():
                        for work in EVENTS[n][when]:
                            event(*work)

        pass_on(0)
        for h in range(0, hidden, cols_step):
            cols = slice(h, h + cols_step)
            acc[:n_d, cols] += dot(hd_scr[:n_d, :], a_scr[:, cols], NN)
            acc[n_d:, cols] += dot(hd_scr[n_d:, :], dy_buf[buf, :, cols], NN)
        pass_on(1)
        return carry

    lax.fori_loop(0, steps, row_step, 0)
    last, buf = SLOT[-1], (steps - 1) % 2
    for copy in grad_copies():
        copy.start()
    dgain_ref[...] = jnp.zeros_like(dgain_ref)
    fine = min(mid, 32)

    def finish(piece):
        def tile(n, d_gain):
            at = pl.ds(pl.multiple_of(piece * mid + n * fine, fine), fine)
            x_f32 = x_buf[buf, at, :].astype(jnp.float32)
            normed, inv_std = norm_rows(x_f32)
            grad = stage[last, 1, at, :].astype(jnp.float32)
            stage[last, 0, at, :] = (x_f32 + stage[last, 0, at, :].astype(jnp.float32)).astype(jnp.bfloat16)
            d_hat = grad * gain
            d_x = inv_std * (d_hat - jnp.mean(d_hat, axis=-1, keepdims=True) - normed * jnp.mean(d_hat * normed, axis=-1, keepdims=True))
            stage[last, 1, at, :] = (dy_buf[buf, at, :].astype(jnp.float32) + d_x).astype(jnp.bfloat16)
            return d_gain + jnp.sum(grad * normed, axis=0, keepdims=True)

        dgain_ref[...] += lax.fori_loop(0, mid // fine, tile, jnp.zeros((1, hidden), jnp.float32))
        copies = [pltpu.make_async_copy(piece_of(stage.at[last, t], piece), piece_of(dst, piece), end_sem.at[piece, t])
                  for t, dst in ((0, y_own), (1, dx_own))]
        for copy in copies:
            copy.start()
        return copies

    ends = []
    ended = {0: 0, 1: 0}
    for work in EVENTS[-1][1]:
        event(*work)
        n, _, piece, ring, _ = work
        if n == steps - 1 and ring == 2:
            ended[piece] += 1
            if ended[piece] == 2:
                ends += finish(piece)
    for slot in range(SLOTS):
        if slot != last:
            for copy in slot_sends(slot):
                copy.wait()
    for copy in ends + grad_copies():
        copy.wait()


def gather_kernel(y_own, dx_own, dgain_ref, g_own, g_sib, y_lo, y_hi, dx_all, g_recv, dgain_out, grads, d_up,
                  gain_scr, g_buf, t_buf, send_sem, link_sem, pair_sem, pair_recv, own_sem, g_sem, gb_sem, dg_send, dg_recv):
    place = Place()
    core = place.core
    _, seq_len, hidden = dx_all.shape
    mid = seq_len // 2
    links = (('x', 1), ('x', -1), ('y', 1), ('y', -1))
    peers = [place.peer(a, o) for a in ('x', 'y') for o in (1, 2, 3)] + [place.sibling()]
    pl.semaphore_wait(greet(peers), len(peers))

    issued = {link: [] for link in links}
    sends = []

    def row_index(t, d_1, d_2):
        return place.index(d_1 % RING, d_2 % RING) if t == 0 else place.index(d_2 % RING, d_1 % RING)

    def spot_of(t, row, piece):
        if t == 1:
            return dx_all.at[row, pl.ds(piece * mid, mid)]
        return (y_lo, y_hi)[piece].at[row]

    def source(t, d_1, d_2, piece):
        if (d_1, d_2) == (0, 0):
            return (y_own, dx_own)[t].at[pl.ds(piece * mid, mid)]
        return spot_of(t, row_index(t, d_1, d_2), piece)

    def issue(link, t, d_1, d_2, piece):
        n = len(issued[link])
        which = links.index(link)
        copy = remote(source(t, d_1, d_2, piece), spot_of(t, row_index(t, d_1, d_2), piece),
                      send_sem.at[which, n], link_sem.at[which, n], place.peer(*link))
        copy.start()
        sends.append(copy)
        issued[link].append((t, d_1, d_2, piece))

    def pair(t, d_1, d_2, piece):
        slot = ((d_1 % RING) * RING + d_2 % RING) * 2 + piece
        copy = remote(source(t, d_1, d_2, piece), spot_of(t, row_index(t, d_1, d_2), piece),
                      pair_sem.at[t, slot], pair_recv.at[t, piece], place.sibling())
        copy.start()
        sends.append(copy)

    axes = (('y', 'x'), ('x', 'y'))
    def gain_swap(n):
        axis = ('x', 'core', 'y')[n]
        at = {'core': place.core, 'x': place.x, 'y': place.y}[axis]
        devices = [place.sibling()] if axis == 'core' else [place.peer(axis, offset) for offset in (1, 2, 3)]
        return at, [remote(gain_scr.at[n, at], gain_scr.at[n, at], dg_send.at[n, m], dg_recv.at[n, m], device)
                    for m, device in enumerate(devices)]

    def gain_start(n, value):
        at, copies = gain_swap(n)
        gain_scr[n, at] = value
        for copy in copies:
            copy.start()

    def gain_end(n):
        _, copies = gain_swap(n)
        for copy in copies:
            copy.wait()
        total = gain_scr[n, 0]
        for m in range(1, len(copies) + 1):
            total = total + gain_scr[n, m]
        return total

    gain_start(0, dgain_ref[...])
    for ring in range(2):
        for n in range(2):
            for t in range(2):
                for way in (1, -1):
                    issue((axes[t][ring], way), t, 0, 0, n if way == 1 else 1 - n)
    locals_ = []
    for t in range(2):
        for piece in range(2):
            pair(t, 0, 0, piece)
            copy = pltpu.make_async_copy(source(t, 0, 0, piece), spot_of(t, place.me, piece), own_sem.at[t, piece])
            copy.start()
            locals_.append(copy)

    g_copy = remote(g_sib, g_recv, g_sem.at[0], g_sem.at[1], place.sibling())
    g_copy.start()

    tile, turn = g_buf.shape[1], t_buf.shape[2]
    n_up = d_up.shape[1]
    n_qkv = 3 * tile

    def grad_tile(at, to):
        loads = [pltpu.make_async_copy(g.at[pl.ds(at, tile)], g_buf.at[n], gb_sem.at[n]) for n, g in enumerate((g_own, g_recv))]
        for load in loads:
            load.start()
        for load in loads:
            load.wait()
        grads[to:to + tile, :] = (g_buf[0] + g_buf[1]).astype(grads.dtype)

    def up_tile(h):
        loads = [pltpu.make_async_copy(g.at[pl.ds(n_qkv, n_up), pl.ds(h, turn)], t_buf.at[n], gb_sem.at[n])
                 for n, g in enumerate((g_own, g_recv))]
        for load in loads:
            load.start()
        for load in loads:
            load.wait()
        d_up[h:h + turn, :] = (t_buf[0] + t_buf[1]).T.astype(d_up.dtype)

    jobs = [functools.partial(grad_tile, at, at) for at in range(0, n_qkv, tile)]
    jobs += [functools.partial(grad_tile, at, at - n_up) for at in range(n_qkv + n_up, g_own.shape[0], tile)]
    jobs += [functools.partial(up_tile, h) for h in range(0, hidden, turn)]

    gain_start(1, gain_end(0))
    rounds = RING * RING - 1
    for n in range(rounds):
        for link in links:
            t, d_1, d_2, piece = issued[link][n]
            axis, way = link
            on_first = axis == axes[t][0]
            d_1, d_2 = (d_1 - way, d_2) if on_first else (d_1, d_2 - way)
            landed(spot_of(t, row_index(t, d_1, d_2), piece), link_sem.at[links.index(link), n])
            along = d_1 if on_first else d_2
            if abs(along) == 1 and piece == (0 if way == 1 else 1):
                issue(link, t, d_1, d_2, piece)
            if on_first:
                for other in (1, -1):
                    issue((axes[t][1], other), t, d_1, d_2, piece)
            pair(t, d_1, d_2, piece)
        if n == 0:
            gain_start(2, gain_end(1))
        if n == 10:
            dgain_out[...] = jnp.sum(gain_end(2), axis=0).astype(dgain_out.dtype)
        if n == 2:
            g_copy.wait()
        if n >= 2:
            for job in jobs[2 * (n - 2):2 * (n - 1)]:
                job()

    for t in range(2):
        for piece in range(2):
            theirs = dx_all.at[pl.ds(0, RING * RING), pl.ds(piece * mid, mid)] if t else (y_lo, y_hi)[piece].at[pl.ds(0, RING * RING)]
            landed(theirs, pair_recv.at[t, piece])
    for copy in sends:
        copy.wait_send()
    for copy in locals_:
        copy.wait()


def place_kernel(y_lo, y_hi, dx_all, grads, d_up, dgain, y_out, dx_out, d_wqkv, d_wout, d_wdown, d_wup, dgain_out, bounce, in_sem, out_sem, sem):
    rows, mid, _ = y_lo.shape
    n_qkv, n_o, n_dn = d_wqkv.shape[0], d_wout.shape[0], d_wdown.shape[0]
    bufs, per = bounce.shape[0], bounce.shape[1]
    count = rows // per
    loads = [pltpu.make_async_copy(y_hi.at[pl.ds(n * per, per)], bounce.at[n % bufs], in_sem.at[n % bufs]) for n in range(count)]
    stores = [pltpu.make_async_copy(bounce.at[n % bufs], y_out.at[pl.ds(n * per, per), pl.ds(mid, mid)], out_sem.at[n % bufs]) for n in range(count)]
    for n in range(min(bufs, count)):
        loads[n].start()
    split = 4
    part = rows // split
    direct = []
    for n in range(split):
        at = pl.ds(n * part, part)
        direct += [(dx_all.at[at], dx_out.at[at]), (y_lo.at[at], y_out.at[at, pl.ds(0, mid)])]
    direct += [(grads.at[pl.ds(0, n_qkv)], d_wqkv),
               (grads.at[pl.ds(n_qkv, n_o)], d_wout), (grads.at[pl.ds(n_qkv + n_o, n_dn)], d_wdown), (d_up, d_wup)]
    copies = [pltpu.make_async_copy(src, dst, sem.at[n]) for n, (src, dst) in enumerate(direct)]
    for copy in copies:
        copy.start()
    dgain_out[...] = dgain[...]
    for n in range(count):
        loads[n].wait()
        stores[n].start()
        if n >= 1 and n - 1 + bufs < count:
            stores[n - 1].wait()
            loads[n - 1 + bufs].start()
    for n in range(max(0, count - bufs), count):
        stores[n].wait()
    for copy in copies:
        copy.wait()


def solution(mesh):
    devices = mesh.shape['model']
    assert devices == 2 * RING * RING

    def body(x_in, seg_ids, ln_gain, w_qkv, w_out, w_up, w_down, dy_in):
        rows, seq_len, hidden = x_in.shape
        assert rows == devices
        wqkv = w_qkv.transpose(1, 2, 3, 0).reshape(-1, hidden)
        wo = w_out.reshape(-1, hidden)
        n_qkv, n_up, n_o, n_dn = wqkv.shape[0], w_up.shape[1], wo.shape[0], w_down.shape[0]
        n_in, n_out = n_qkv + n_up, n_o + n_dn
        n_all = n_in + n_out
        bf16, f32 = jnp.bfloat16, jnp.float32
        vmem, anywhere = pl.BlockSpec(memory_space=pltpu.VMEM), pl.BlockSpec(memory_space=pl.ANY)
        dma = pltpu.SemaphoreType.DMA
        shape = jax.ShapeDtypeStruct
        chips, mid = RING * RING, seq_len // 2
        fixed = lambda array: pltpu.with_memory_space_constraint(array, pltpu.VMEM)
        y_own, dx_own, d_gain, g_own, g_sib, _ = pl.pallas_call(
            reduce_kernel,
            in_specs=[anywhere, anywhere, vmem, vmem] + [anywhere] * 4,
            out_specs=[anywhere, anywhere, vmem, anywhere, anywhere, anywhere],
            out_shape=[shape((seq_len, hidden), bf16), shape((seq_len, hidden), bf16), shape((1, hidden), f32),
                       shape((n_all, hidden), f32), shape((n_all, hidden), f32), shape((2, RING, 2, seq_len, hidden), bf16)],
            scratch_shapes=[
                pltpu.VMEM((2 * n_in, hidden), bf16), pltpu.VMEM((2 * n_out, hidden), bf16), pltpu.VMEM((hidden, n_up), bf16),
                pltpu.VMEM((2 * n_all, hidden), f32),
                pltpu.VMEM((2, seq_len, hidden), bf16), pltpu.VMEM((2, seq_len, hidden), bf16),
                pltpu.VMEM((seq_len, hidden), bf16), pltpu.VMEM((2 * n_all, seq_len), bf16),
                pltpu.VMEM((SLOTS, 2, seq_len, hidden), bf16),
                pltpu.VMEM((2, RING + 1, 2, mid, hidden), bf16),
                pltpu.VMEM((2, 2, seq_len, hidden), bf16), pltpu.VMEM((2, 2, mid, hidden), bf16),
                dma((2, 2)), dma((4,)), dma((4,)), dma((4,)), dma((SLOTS, 2, 2)),
                dma((2, RING + 1, 2)), dma((2, RING + 1, 2, 2)), dma((2, 2)), dma((2, 2)), dma((8,)),
            ],
            compiler_params=pltpu.CompilerParams(collective_id=0, has_side_effects=True, vmem_limit_bytes=VMEM_LIMIT),
            name="rows_reduce",
        )(x_in, dy_in, seg_ids, ln_gain, wqkv, w_up, wo, w_down)

        per_link = chips - 1
        y_lo, y_hi, dx_all, _, d_gain, grads, d_up = pl.pallas_call(
            gather_kernel,
            in_specs=[anywhere, anywhere, vmem, anywhere, anywhere],
            out_specs=[vmem, anywhere, vmem, anywhere, vmem, vmem, vmem],
            out_shape=[pltpu.VMEM((rows, mid, hidden), bf16), shape((rows, mid, hidden), bf16), pltpu.VMEM((rows, seq_len, hidden), bf16),
                       shape(g_sib.shape, f32), pltpu.VMEM((hidden,), bf16),
                       pltpu.VMEM((n_all - n_up, hidden), bf16), pltpu.VMEM((hidden, n_up), bf16)],
            scratch_shapes=[
                pltpu.VMEM((3, RING, 1, hidden), f32), pltpu.VMEM((2, n_o, hidden), f32), pltpu.VMEM((2, n_up, min(hidden, 256)), f32),
                dma((4, per_link)), dma((4, per_link)), dma((2, 2 * chips)), dma((2, 2)), dma((2, 2)), dma((2,)), dma((2,)),
                dma((3, 3)), dma((3, 3)),
            ],
            compiler_params=pltpu.CompilerParams(collective_id=1, has_side_effects=True, vmem_limit_bytes=LANDING_LIMIT),
            name="rows_gather",
        )(y_own, dx_own, d_gain, g_own, g_sib)

        bufs = 6
        y_out, dx_out, d_wqkv, d_wout, d_wdown, d_wup, d_gain = pl.pallas_call(
            place_kernel,
            in_specs=[vmem, anywhere, vmem, vmem, vmem, vmem],
            out_specs=[anywhere] * 6 + [vmem],
            out_shape=[shape(x_in.shape, bf16), shape(x_in.shape, bf16), shape(wqkv.shape, bf16), shape(wo.shape, bf16),
                       shape(w_down.shape, bf16), shape(w_up.shape, bf16), shape((hidden,), bf16)],
            scratch_shapes=[pltpu.VMEM((bufs, 2, mid, hidden), bf16), dma((bufs,)), dma((bufs,)), dma((12,))],
            compiler_params=pltpu.CompilerParams(vmem_limit_bytes=LANDING_LIMIT),
            name="rows_place",
        )(fixed(y_lo), pltpu.with_memory_space_constraint(y_hi, pltpu.HBM), fixed(dx_all), fixed(grads), fixed(d_up), fixed(d_gain))
        d_wqkv = d_wqkv.reshape(w_qkv.shape[1:] + (hidden,)).transpose(3, 0, 1, 2)
        return y_out, dx_out, d_gain, d_wqkv, d_wout.reshape(w_out.shape), d_wup, d_wdown

    in_specs = (P('data'), P('data'), P(), P(None, 'model'), P('model'), P(None, 'model'), P('model'), P('data'))
    out_specs = (P('data'), P('data'), P('data'), P('data', 'model'), P(('data', 'model')), P('data', 'model'), P(('data', 'model')))
    return jax.shard_map(body, mesh=mesh, in_specs=in_specs, out_specs=out_specs, check_vma=False)
```

```python
import functools

import jax
import jax.numpy as jnp
from jax import lax
from jax.experimental import pallas as pl
from jax.experimental.pallas import tpu as pltpu
from jax.sharding import PartitionSpec as P

LN_EPS = 1e-5
RING = 4
MESH = pl.DeviceIdType.MESH
NT = (((1,), (1,)), ((), ()))
NN = (((1,), (0,)), ((), ()))
TN = (((0,), (0,)), ((), ()))
ORDER = ((2, 2), (1, 2), (2, 3), (2, 1), (3, 2), (3, 3), (1, 1), (0, 2),
         (2, 0), (0, 1), (3, 1), (1, 3), (1, 0), (3, 0), (0, 3), (0, 0))
SLOT = (0, 1, 2, 3, 4, 0, 1, 2, 3, 4, 1, 0, 2, 3, 0, 1)
SLOTS = max(SLOT) + 1
PASS, LOAD, ADD = range(3)
EVENTS = (
    (((0, 0, 0, 1, PASS), (0, 0, 1, 1, PASS), (0, 1, 0, 1, PASS), (0, 1, 1, 1, PASS)),
     ()),
    (((1, 0, 0, 1, PASS), (1, 0, 1, 1, PASS), (1, 1, 1, 1, PASS)),
     ()),
    (((2, 0, 0, 1, PASS), (2, 1, 0, 1, PASS), (2, 1, 1, 1, PASS), (1, 1, 0, 1, PASS), (2, 0, 1, 1, PASS)),
     ()),
    (((3, 0, 1, 1, PASS), (3, 1, 0, 1, PASS), (3, 1, 1, 1, PASS), (3, 0, 0, 1, PASS)),
     ()),
    (((4, 0, 0, 1, PASS), (4, 0, 1, 1, PASS), (4, 1, 0, 1, PASS), (4, 1, 1, 1, PASS)),
     ()),
    (((5, 0, 0, 1, PASS), (5, 1, 0, 1, PASS), (5, 1, 1, 1, PASS)),
     ()),
    (((6, 0, 1, 1, PASS), (6, 1, 1, 1, PASS), (6, 0, 0, 1, PASS)),
     ()),
    (((7, 1, 0, 1, LOAD), (7, 0, 0, 1, PASS), (7, 0, 1, 1, PASS), (5, 0, 1, 1, PASS), (6, 1, 0, 1, PASS)),
     ((7, 1, 1, 1, LOAD), (7, 1, 0, 1, ADD), (7, 1, 0, 2, PASS))),
    (((8, 0, 0, 1, LOAD), (8, 1, 0, 1, PASS), (8, 1, 1, 1, PASS), (7, 1, 1, 1, ADD), (8, 0, 1, 1, LOAD), (7, 1, 1, 2, PASS)),
     ((8, 0, 0, 1, ADD), (8, 0, 0, 2, PASS), (8, 0, 1, 1, ADD), (8, 0, 1, 2, PASS))),
    (((9, 0, 1, 1, PASS),),
     ()),
    (((10, 0, 1, 1, PASS), (10, 1, 0, 1, PASS), (10, 1, 1, 1, PASS), (10, 0, 0, 1, PASS)),
     ()),
    (((11, 0, 0, 1, PASS), (11, 1, 1, 1, PASS), (11, 0, 1, 1, PASS), (11, 1, 0, 1, PASS), (9, 0, 0, 1, PASS)),
     ()),
    (((12, 1, 1, 1, PASS), (12, 1, 0, 1, PASS)),
     ()),
    (((12, 0, 0, 1, LOAD), (13, 1, 0, 1, PASS), (13, 1, 1, 1, PASS)),
     ((12, 0, 0, 1, ADD), (9, 1, 0, 1, LOAD), (12, 0, 0, 2, PASS))),
    (((14, 1, 1, 1, LOAD), (14, 0, 0, 1, PASS), (14, 0, 1, 1, PASS), (9, 1, 0, 1, ADD), (14, 1, 0, 1, LOAD), (9, 1, 0, 2, PASS)),
     ((14, 1, 1, 1, ADD), (12, 0, 1, 1, LOAD), (14, 1, 1, 2, PASS), (14, 1, 0, 1, ADD), (14, 1, 0, 2, PASS), (12, 0, 1, 1, ADD), (13, 0, 1, 1, LOAD), (12, 0, 1, 2, PASS), (13, 0, 1, 1, ADD), (9, 1, 1, 1, LOAD), (13, 0, 1, 2, PASS), (9, 1, 1, 1, ADD), (9, 1, 1, 2, PASS))),
    ((),
     ((13, 0, 0, 1, LOAD), (13, 0, 0, 1, ADD), (13, 0, 0, 2, PASS), (15, 1, 0, 1, LOAD), (15, 1, 0, 1, ADD), (15, 0, 0, 1, LOAD), (15, 0, 1, 1, LOAD), (15, 0, 0, 1, ADD), (15, 0, 1, 1, ADD), (15, 1, 1, 1, LOAD), (15, 1, 1, 1, ADD), (15, 0, 1, 2, PASS), (15, 1, 1, 2, PASS), (15, 1, 0, 2, PASS), (15, 0, 0, 2, PASS))),
)
VMEM_LIMIT = 60 * 2 ** 20
LANDING_LIMIT = 5 * 2 ** 20


def dot(lhs, rhs, dims):
    return lax.dot_general(lhs, rhs, dims, preferred_element_type=jnp.float32)


def norm_rows(x_f32):
    mean_val = jnp.mean(x_f32, axis=-1, keepdims=True)
    centered = x_f32 - mean_val
    inv_std = lax.rsqrt(jnp.mean(centered * centered, axis=-1, keepdims=True) + LN_EPS)
    return centered * inv_std, inv_std


class Place:
    def __init__(self):
        me = lax.axis_index('model')
        self.core = me % 2
        self.x = (me // 2) % RING
        self.y = me // (2 * RING)
        self.me = me

    def index(self, d_y, d_x, core=None):
        core = self.core if core is None else core
        return (((self.y + d_y) % RING) * RING + (self.x + d_x) % RING) * 2 + core

    def peer(self, axis, offset):
        return self.index(offset % RING, 0) if axis == 'y' else self.index(0, offset % RING)

    def sibling(self):
        return self.index(0, 0, 1 - self.core)


def remote(src, dst, send_sem, recv_sem, device):
    return pltpu.make_async_remote_copy(src_ref=src, dst_ref=dst, send_sem=send_sem, recv_sem=recv_sem,
                                        device_id={'model': device}, device_id_type=MESH)


def greet(peers):
    barrier = pltpu.get_barrier_semaphore()
    for peer in peers:
        pl.semaphore_signal(barrier, inc=1, device_id={'model': peer}, device_id_type=MESH)
    return barrier


def pick(step, values):
    out = jnp.int32(0)
    for n, value in enumerate(values):
        out = jnp.where(step == n, value, out)
    return out


def rows_at(ref, at, count):
    return ref.at[pl.ds(pl.multiple_of(at, 16), count)]


def landed(ref, sem):
    pltpu.make_async_copy(ref, ref, sem).wait()


def add_into(dst, *sources):
    rows = dst.shape[0]
    tile = min(rows, 32)

    def tile_add(n, carry):
        at = pl.ds(pl.multiple_of(n * tile, tile), tile)
        total = dst[at, :].astype(jnp.float32)
        for source in sources:
            total += source[at, :].astype(jnp.float32)
        dst[at, :] = total.astype(dst.dtype)
        return carry

    lax.fori_loop(0, rows // tile, tile_add, 0)


def reduce_kernel(x_hbm, dy_hbm, seg_ref, gain_ref, wqkv_hbm, w1_hbm, wo_hbm, w2_hbm,
                  y_own, dx_own, dgain_ref, g_own, g_sib, full,
                  w_in, w_out, w1_raw, acc, x_buf, dy_buf, a_scr, hd_scr, stage, half, last_full, tmp,
                  row_sem, w_sem, ws_sem, wr_sem, send_sem, half_sem, full_sem, tmp_sem, out_sem):
    place = Place()
    core = place.core
    _, seq_len, hidden = x_buf.shape
    mid = seq_len // 2
    n_qkv, n_up, n_o, n_dn = wqkv_hbm.shape[0], w1_hbm.shape[1], wo_hbm.shape[0], w2_hbm.shape[0]
    n_d = 2 * (n_qkv + n_up)
    steps = len(ORDER)

    def row_of(step):
        return place.index(pick(step, [o[0] for o in ORDER]), pick(step, [o[1] for o in ORDER]))

    def row_copy(row, buf, n):
        return pltpu.make_async_copy((x_hbm, dy_hbm)[n].at[row], (x_buf, dy_buf)[n].at[buf], row_sem.at[buf, n])

    up_spot = rows_at(w_in, 2 * n_qkv + core * n_up, n_up)
    spots = ((wqkv_hbm, rows_at(w_in, core * n_qkv, n_qkv)), (wo_hbm, rows_at(w_out, core * n_o, n_o)),
             (w2_hbm, rows_at(w_out, 2 * n_o + core * n_dn, n_dn)))

    gain = gain_ref[...].astype(jnp.float32)[None, :]
    sub = min(seq_len, 64)

    def norm_row(buf):
        for t in range(0, seq_len, sub):
            normed, _ = norm_rows(x_buf[buf, t:t + sub, :].astype(jnp.float32))
            a_scr[t:t + sub, :] = (normed * gain).astype(jnp.bfloat16)

    peers = [place.peer('x', 1), place.peer('x', -1), place.peer('y', 1), place.peer('y', -1), place.sibling()]
    barrier = greet(peers)
    raw = pltpu.make_async_copy(w1_hbm, w1_raw, w_sem.at[3])
    raw.start()
    for n in range(2):
        row_copy(row_of(0), 0, n).start()
    mine = [pltpu.make_async_copy(src, dst, w_sem.at[n]) for n, (src, dst) in enumerate(spots)]
    for copy in mine:
        copy.start()
    raw.wait()
    turn = min(hidden, 256)
    for h in range(0, hidden, turn):
        up_spot[:, h:h + turn] = w1_raw[h:h + turn, :].T
    pl.semaphore_wait(barrier, len(peers))
    swaps = [remote(dst, dst, ws_sem.at[n], wr_sem.at[n], place.sibling()) for n, (_, dst) in enumerate(spots)]
    swaps.append(remote(up_spot, up_spot, ws_sem.at[3], wr_sem.at[3], place.sibling()))
    for n in (0, 3, 1, 2):
        if n < 3:
            mine[n].wait()
        swaps[n].start()
    row_copy(0, 0, 0).wait()
    norm_row(0)
    acc[...] = jnp.zeros_like(acc)
    for n in (0, 3):
        swaps[n].wait()

    scale = n_o ** -0.5
    cols_step = min(hidden, 512)

    def piece_of(ref, piece):
        return ref.at[pl.ds(piece * mid, mid)]

    def slot_sends(slot):
        return [pltpu.make_async_copy(piece_of(stage.at[slot, t], piece), piece_of(stage.at[slot, t], piece),
                                      send_sem.at[slot, t, piece]) for t in range(2) for piece in range(2)]

    def event(n, t, piece, ring, kind):
        d_y, d_x = ORDER[n]
        first, second = (('x', d_x), ('y', d_y)) if t == 0 else (('y', d_y), ('x', d_x))
        (axis, offset), line = (first, second[1]) if ring == 1 else (second, RING)
        ahead, behind = place.peer(axis, 1), place.peer(axis, -1)
        spot = piece_of(stage.at[SLOT[n], t], piece)

        def send(dst, recv_sem, device):
            remote(spot, dst, send_sem.at[SLOT[n], t, piece], recv_sem, device).start()

        if offset == 2:
            send(half.at[t, line, piece], half_sem.at[t, line, piece], ahead if piece == 0 else behind)
        elif offset in (1, 3):
            side = 0 if offset == 1 else 1
            if side == piece:
                landed(half.at[t, line, piece], half_sem.at[t, line, piece])
                add_into(spot, half.at[t, line, piece])
            dst = last_full.at[t, side] if line == RING else full.at[t, line, side]
            send(piece_of(dst, piece), full_sem.at[t, line, side, piece], ahead if side == 0 else behind)
        elif line == RING:
            came = [piece_of(last_full.at[t, side], piece) for side in range(2)]
            for side in range(2):
                landed(came[side], full_sem.at[t, line, side, piece])
            add_into(spot, *came)
        else:
            loads = [pltpu.make_async_copy(piece_of(full.at[t, line, side], piece), tmp.at[piece, side], tmp_sem.at[piece, side])
                     for side in range(2)]
            if kind == LOAD:
                for side in range(2):
                    landed(piece_of(full.at[t, line, side], piece), full_sem.at[t, line, side, piece])
                    loads[side].start()
            else:
                for load in loads:
                    load.wait()
                add_into(spot, tmp.at[piece, 0], tmp.at[piece, 1])

    def grad_copies():
        copies = []
        for n, (side, dst) in enumerate(((core, g_own), (1 - core, g_sib))):
            at, to = 0, 0
            for m, size in enumerate((n_qkv, n_up, n_o, n_dn)):
                copies.append(pltpu.make_async_copy(rows_at(acc, at + side * size, size), dst.at[pl.ds(to, size)], out_sem.at[4 * n + m]))
                at, to = at + 2 * size, to + size
        return copies

    def attend(qkv, d_attn, allowed):
        heads = range(2)
        parts = [[qkv[head * n_qkv + n * n_o:head * n_qkv + (n + 1) * n_o] for n in range(3)] for head in heads]
        d_o = [d_attn[head * n_o:(head + 1) * n_o] for head in heads]
        raw = [dot(keys, query, TN) for query, keys, _ in parts]
        d_p = [dot(parts[head][2], d_o[head], TN) for head in heads]
        expd = []
        for head in heads:
            scores = jnp.where(allowed, raw[head] * scale, -1e30)
            expd.append(jnp.exp(scores - jnp.max(scores, axis=0, keepdims=True)))
        probs = [e / jnp.sum(e, axis=0, keepdims=True) for e in expd]
        probs_b = [p.astype(jnp.bfloat16) for p in probs]
        d_s = [(probs[head] * (d_p[head] - jnp.sum(d_p[head] * probs[head], axis=0, keepdims=True)) * scale).astype(jnp.bfloat16)
               for head in heads]
        for head in heads:
            at = head * n_qkv
            query, keys, values = parts[head]
            hd_scr[n_d + head * n_o:n_d + (head + 1) * n_o, :] = dot(values, probs_b[head], NN).astype(jnp.bfloat16)
            hd_scr[at + 2 * n_o:at + 3 * n_o, :] = dot(d_o[head], probs_b[head], NT).astype(jnp.bfloat16)
            hd_scr[at:at + n_o, :] = dot(keys, d_s[head], NN).astype(jnp.bfloat16)
            hd_scr[at + n_o:at + 2 * n_o, :] = dot(query, d_s[head], NT).astype(jnp.bfloat16)

    def row_step(step, carry):
        buf = step % 2
        slot = pick(step, SLOT)
        row = row_of(step)

        @pl.when(step > 0)
        def _():
            row_copy(row, buf, 0).wait()
            norm_row(buf)

        row_copy(row, buf, 1).wait()

        @pl.when(step + 1 < steps)
        def _():
            ahead = row_of(step + 1)
            for n in range(2):
                row_copy(ahead, 1 - buf, n).start()

        @pl.when(step == 0)
        def _():
            for copy in swaps[1:3]:
                copy.wait()

        proj = dot(w_in[...], a_scr[...], NT)
        d_proj = dot(w_out[...], dy_buf[buf], NT).astype(jnp.bfloat16)
        qkv = proj[:2 * n_qkv].astype(jnp.bfloat16)
        up = proj[2 * n_qkv:].astype(jnp.bfloat16).astype(jnp.float32)
        d_attn = d_proj[:2 * n_o]
        d_hid = d_proj[2 * n_o:].astype(jnp.float32)
        cdf = 0.5 * (1.0 + lax.erf(up * (0.5 ** 0.5)))
        hd_scr[n_d + 2 * n_o:, :] = (up * cdf).astype(jnp.bfloat16)
        slope = cdf + up * (jnp.exp(-0.5 * up * up) * 0.3989422804014327)
        hd_scr[2 * n_qkv:n_d, :] = (d_hid * slope).astype(jnp.bfloat16)

        seg_row = seg_ref[pl.ds(row, 1), :]
        classes = lax.broadcasted_iota(jnp.int32, (16, seq_len), 0)
        one_hot = (classes == jnp.broadcast_to(seg_row, (16, seq_len))).astype(jnp.bfloat16)
        same = dot(one_hot, one_hot, TN) > 0.5
        key_id = lax.broadcasted_iota(jnp.int32, (seq_len, seq_len), 0)
        query_id = lax.broadcasted_iota(jnp.int32, (seq_len, seq_len), 1)
        allowed = (key_id <= query_id) & same
        attend(qkv, d_attn, allowed)

        @pl.when(pick(step, [int(SLOT[n] in SLOT[:n]) for n in range(steps)]) == 1)
        def _():
            for copy in slot_sends(slot):
                copy.wait()

        for h in range(0, hidden, cols_step):
            cols = slice(h, h + cols_step)
            stage[slot, 0, :, cols] = dot(hd_scr[n_d:, :], w_out[:, cols], TN).astype(jnp.bfloat16)
            stage[slot, 1, :, cols] = dot(hd_scr[:n_d, :], w_in[:, cols], TN).astype(jnp.bfloat16)

        def pass_on(when):
            for n in range(steps - 1):
                if EVENTS[n][when]:
                    @pl.when(step == n)
                    def _():
                        for work in EVENTS[n][when]:
                            event(*work)

        pass_on(0)
        for h in range(0, hidden, cols_step):
            cols = slice(h, h + cols_step)
            acc[:n_d, cols] += dot(hd_scr[:n_d, :], a_scr[:, cols], NN)
            acc[n_d:, cols] += dot(hd_scr[n_d:, :], dy_buf[buf, :, cols], NN)
        pass_on(1)
        return carry

    lax.fori_loop(0, steps, row_step, 0)
    last, buf = SLOT[-1], (steps - 1) % 2
    for copy in grad_copies():
        copy.start()
    dgain_ref[...] = jnp.zeros_like(dgain_ref)
    fine = min(mid, 32)

    def finish(piece):
        def tile(n, d_gain):
            at = pl.ds(pl.multiple_of(piece * mid + n * fine, fine), fine)
            x_f32 = x_buf[buf, at, :].astype(jnp.float32)
            normed, inv_std = norm_rows(x_f32)
            grad = stage[last, 1, at, :].astype(jnp.float32)
            y_own[at, :] = (x_f32 + stage[last, 0, at, :].astype(jnp.float32)).astype(jnp.bfloat16)
            d_hat = grad * gain
            d_x = inv_std * (d_hat - jnp.mean(d_hat, axis=-1, keepdims=True) - normed * jnp.mean(d_hat * normed, axis=-1, keepdims=True))
            dx_own[at, :] = (dy_buf[buf, at, :].astype(jnp.float32) + d_x).astype(jnp.bfloat16)
            return d_gain + jnp.sum(grad * normed, axis=0, keepdims=True)

        dgain_ref[...] += lax.fori_loop(0, mid // fine, tile, jnp.zeros((1, hidden), jnp.float32))

    ended = {0: 0, 1: 0}
    for work in EVENTS[-1][1]:
        event(*work)
        n, _, piece, ring, _ = work
        if n == steps - 1 and ring == 2:
            ended[piece] += 1
            if ended[piece] == 2:
                finish(piece)
    for slot in range(SLOTS):
        if slot != last:
            for copy in slot_sends(slot):
                copy.wait()
    for copy in grad_copies():
        copy.wait()


def gather_kernel(y_own, dx_own, dgain_ref, g_own, g_sib, y_lo, y_hi, dx_all, g_recv, dgain_out, grads, d_up,
                  gain_scr, g_buf, t_buf, send_sem, link_sem, pair_sem, pair_recv, own_sem, g_sem, gb_sem, dg_send, dg_recv):
    place = Place()
    core = place.core
    _, seq_len, hidden = dx_all.shape
    mid = seq_len // 2
    links = (('x', 1), ('x', -1), ('y', 1), ('y', -1))
    peers = [place.peer(a, o) for a in ('x', 'y') for o in (1, 2, 3)] + [place.sibling()]
    pl.semaphore_wait(greet(peers), len(peers))

    issued = {link: [] for link in links}
    sends = []

    def row_index(t, d_1, d_2):
        return place.index(d_1 % RING, d_2 % RING) if t == 0 else place.index(d_2 % RING, d_1 % RING)

    def spot_of(t, row, piece):
        if t == 1:
            return dx_all.at[row, pl.ds(piece * mid, mid)]
        return (y_lo, y_hi)[piece].at[row]

    def source(t, d_1, d_2, piece):
        if (d_1, d_2) == (0, 0):
            return (y_own, dx_own)[t].at[pl.ds(piece * mid, mid)]
        return spot_of(t, row_index(t, d_1, d_2), piece)

    def issue(link, t, d_1, d_2, piece):
        n = len(issued[link])
        which = links.index(link)
        copy = remote(source(t, d_1, d_2, piece), spot_of(t, row_index(t, d_1, d_2), piece),
                      send_sem.at[which, n], link_sem.at[which, n], place.peer(*link))
        copy.start()
        sends.append(copy)
        issued[link].append((t, d_1, d_2, piece))

    def pair(t, d_1, d_2, piece):
        slot = ((d_1 % RING) * RING + d_2 % RING) * 2 + piece
        copy = remote(source(t, d_1, d_2, piece), spot_of(t, row_index(t, d_1, d_2), piece),
                      pair_sem.at[t, slot], pair_recv.at[t, piece], place.sibling())
        copy.start()
        sends.append(copy)

    axes = (('y', 'x'), ('x', 'y'))
    def gain_swap(n):
        axis = ('x', 'core', 'y')[n]
        at = {'core': place.core, 'x': place.x, 'y': place.y}[axis]
        devices = [place.sibling()] if axis == 'core' else [place.peer(axis, offset) for offset in (1, 2, 3)]
        return at, [remote(gain_scr.at[n, at], gain_scr.at[n, at], dg_send.at[n, m], dg_recv.at[n, m], device)
                    for m, device in enumerate(devices)]

    def gain_start(n, value):
        at, copies = gain_swap(n)
        gain_scr[n, at] = value
        for copy in copies:
            copy.start()

    def gain_end(n):
        _, copies = gain_swap(n)
        for copy in copies:
            copy.wait()
        total = gain_scr[n, 0]
        for m in range(1, len(copies) + 1):
            total = total + gain_scr[n, m]
        return total

    gain_start(0, dgain_ref[...])
    for ring in range(2):
        for n in range(2):
            for t in range(2):
                for way in (1, -1):
                    issue((axes[t][ring], way), t, 0, 0, n if way == 1 else 1 - n)
    for t in range(2):
        for piece in range(2):
            pair(t, 0, 0, piece)
    own_copy = pltpu.make_async_copy(y_own.at[pl.ds(mid, mid)], y_hi.at[place.me], own_sem)
    own_copy.start()
    g_copy = remote(g_sib, g_recv, g_sem.at[0], g_sem.at[1], place.sibling())
    g_copy.start()

    tile, turn = g_buf.shape[1], t_buf.shape[2]
    n_up = d_up.shape[1]
    n_qkv = 3 * tile

    def grad_tile(at, to):
        loads = [pltpu.make_async_copy(g.at[pl.ds(at, tile)], g_buf.at[n], gb_sem.at[n]) for n, g in enumerate((g_own, g_recv))]
        for load in loads:
            load.start()
        for load in loads:
            load.wait()
        grads[to:to + tile, :] = (g_buf[0] + g_buf[1]).astype(grads.dtype)

    def up_tile(h):
        loads = [pltpu.make_async_copy(g.at[pl.ds(n_qkv, n_up), pl.ds(h, turn)], t_buf.at[n], gb_sem.at[n])
                 for n, g in enumerate((g_own, g_recv))]
        for load in loads:
            load.start()
        for load in loads:
            load.wait()
        d_up[h:h + turn, :] = (t_buf[0] + t_buf[1]).T.astype(d_up.dtype)

    jobs = [functools.partial(grad_tile, at, at) for at in range(0, n_qkv, tile)]
    jobs += [functools.partial(grad_tile, at, at - n_up) for at in range(n_qkv + n_up, g_own.shape[0], tile)]
    jobs += [functools.partial(up_tile, h) for h in range(0, hidden, turn)]

    gain_start(1, gain_end(0))
    rounds = RING * RING - 1
    for n in range(rounds):
        for link in links:
            t, d_1, d_2, piece = issued[link][n]
            axis, way = link
            on_first = axis == axes[t][0]
            d_1, d_2 = (d_1 - way, d_2) if on_first else (d_1, d_2 - way)
            landed(spot_of(t, row_index(t, d_1, d_2), piece), link_sem.at[links.index(link), n])
            along = d_1 if on_first else d_2
            if abs(along) == 1 and piece == (0 if way == 1 else 1):
                issue(link, t, d_1, d_2, piece)
            if on_first:
                for other in (1, -1):
                    issue((axes[t][1], other), t, d_1, d_2, piece)
            pair(t, d_1, d_2, piece)
        if n == 0:
            gain_start(2, gain_end(1))
            y_lo[place.me] = y_own[0:mid, :]
            dx_all[place.me] = dx_own[...]
        if n == 10:
            dgain_out[...] = jnp.sum(gain_end(2), axis=0).astype(dgain_out.dtype)
        if n == 2:
            g_copy.wait()
        if n >= 2:
            for job in jobs[2 * (n - 2):2 * (n - 1)]:
                job()

    for t in range(2):
        for piece in range(2):
            theirs = dx_all.at[pl.ds(0, RING * RING), pl.ds(piece * mid, mid)] if t else (y_lo, y_hi)[piece].at[pl.ds(0, RING * RING)]
            landed(theirs, pair_recv.at[t, piece])
    for copy in sends:
        copy.wait_send()
    own_copy.wait()


def place_kernel(y_lo, y_hi, dx_all, grads, d_up, dgain, _y_own, _dx_own, y_out, dx_out, d_wqkv, d_wout, d_wdown, d_wup, dgain_out, bounce, in_sem, out_sem, sem):
    rows, mid, _ = y_lo.shape
    n_qkv, n_o, n_dn = d_wqkv.shape[0], d_wout.shape[0], d_wdown.shape[0]
    bufs, per = bounce.shape[0], bounce.shape[1]
    count = rows // per
    loads = [pltpu.make_async_copy(y_hi.at[pl.ds(n * per, per)], bounce.at[n % bufs], in_sem.at[n % bufs]) for n in range(count)]
    stores = [pltpu.make_async_copy(bounce.at[n % bufs], y_out.at[pl.ds(n * per, per), pl.ds(mid, mid)], out_sem.at[n % bufs]) for n in range(count)]
    for n in range(min(bufs, count)):
        loads[n].start()
    split = 4
    part = rows // split
    direct = []
    for n in range(split):
        at = pl.ds(n * part, part)
        direct += [(dx_all.at[at], dx_out.at[at]), (y_lo.at[at], y_out.at[at, pl.ds(0, mid)])]
    direct += [(grads.at[pl.ds(0, n_qkv)], d_wqkv),
               (grads.at[pl.ds(n_qkv, n_o)], d_wout), (grads.at[pl.ds(n_qkv + n_o, n_dn)], d_wdown), (d_up, d_wup)]
    copies = [pltpu.make_async_copy(src, dst, sem.at[n]) for n, (src, dst) in enumerate(direct)]
    for copy in copies:
        copy.start()
    dgain_out[...] = dgain[...]
    for n in range(count):
        loads[n].wait()
        stores[n].start()
        if n >= 1 and n - 1 + bufs < count:
            stores[n - 1].wait()
            loads[n - 1 + bufs].start()
    for n in range(max(0, count - bufs), count):
        stores[n].wait()
    for copy in copies:
        copy.wait()


def solution(mesh):
    devices = mesh.shape['model']
    assert devices == 2 * RING * RING

    def body(x_in, seg_ids, ln_gain, w_qkv, w_out, w_up, w_down, dy_in):
        rows, seq_len, hidden = x_in.shape
        assert rows == devices
        wqkv = w_qkv.transpose(1, 2, 3, 0).reshape(-1, hidden)
        wo = w_out.reshape(-1, hidden)
        n_qkv, n_up, n_o, n_dn = wqkv.shape[0], w_up.shape[1], wo.shape[0], w_down.shape[0]
        n_in, n_out = n_qkv + n_up, n_o + n_dn
        n_all = n_in + n_out
        bf16, f32 = jnp.bfloat16, jnp.float32
        vmem, anywhere = pl.BlockSpec(memory_space=pltpu.VMEM), pl.BlockSpec(memory_space=pl.ANY)
        dma = pltpu.SemaphoreType.DMA
        shape = jax.ShapeDtypeStruct
        chips, mid = RING * RING, seq_len // 2
        fixed = lambda array: pltpu.with_memory_space_constraint(array, pltpu.VMEM)
        y_own, dx_own, d_gain, g_own, g_sib, _ = pl.pallas_call(
            reduce_kernel,
            in_specs=[anywhere, anywhere, vmem, vmem] + [anywhere] * 4,
            out_specs=[vmem, vmem, vmem, anywhere, anywhere, anywhere],
            out_shape=[pltpu.VMEM((seq_len, hidden), bf16), pltpu.VMEM((seq_len, hidden), bf16), shape((1, hidden), f32),
                       shape((n_all, hidden), f32), shape((n_all, hidden), f32), shape((2, RING, 2, seq_len, hidden), bf16)],
            scratch_shapes=[
                pltpu.VMEM((2 * n_in, hidden), bf16), pltpu.VMEM((2 * n_out, hidden), bf16), pltpu.VMEM((hidden, n_up), bf16),
                pltpu.VMEM((2 * n_all, hidden), f32),
                pltpu.VMEM((2, seq_len, hidden), bf16), pltpu.VMEM((2, seq_len, hidden), bf16),
                pltpu.VMEM((seq_len, hidden), bf16), pltpu.VMEM((2 * n_all, seq_len), bf16),
                pltpu.VMEM((SLOTS, 2, seq_len, hidden), bf16),
                pltpu.VMEM((2, RING + 1, 2, mid, hidden), bf16),
                pltpu.VMEM((2, 2, seq_len, hidden), bf16), pltpu.VMEM((2, 2, mid, hidden), bf16),
                dma((2, 2)), dma((4,)), dma((4,)), dma((4,)), dma((SLOTS, 2, 2)),
                dma((2, RING + 1, 2)), dma((2, RING + 1, 2, 2)), dma((2, 2)), dma((8,)),
            ],
            compiler_params=pltpu.CompilerParams(collective_id=0, has_side_effects=True, vmem_limit_bytes=VMEM_LIMIT),
            name="rows_reduce",
        )(x_in, dy_in, seg_ids, ln_gain, wqkv, w_up, wo, w_down)

        per_link = chips - 1
        y_lo, y_hi, dx_all, _, d_gain, grads, d_up = pl.pallas_call(
            gather_kernel,
            in_specs=[vmem, vmem, vmem, anywhere, anywhere],
            out_specs=[vmem, anywhere, vmem, anywhere, vmem, vmem, vmem],
            out_shape=[pltpu.VMEM((rows, mid, hidden), bf16), shape((rows, mid, hidden), bf16), pltpu.VMEM((rows, seq_len, hidden), bf16),
                       shape(g_sib.shape, f32), pltpu.VMEM((hidden,), bf16),
                       pltpu.VMEM((n_all - n_up, hidden), bf16), pltpu.VMEM((hidden, n_up), bf16)],
            scratch_shapes=[
                pltpu.VMEM((3, RING, 1, hidden), f32), pltpu.VMEM((2, n_o, hidden), f32), pltpu.VMEM((2, n_up, min(hidden, 256)), f32),
                dma((4, per_link)), dma((4, per_link)), dma((2, 2 * chips)), dma((2, 2)), dma, dma((2,)), dma((2,)),
                dma((3, 3)), dma((3, 3)),
            ],
            compiler_params=pltpu.CompilerParams(collective_id=1, has_side_effects=True, vmem_limit_bytes=LANDING_LIMIT),
            name="rows_gather",
        )(fixed(y_own), fixed(dx_own), d_gain, g_own, g_sib)

        bufs = 4
        y_out, dx_out, d_wqkv, d_wout, d_wdown, d_wup, d_gain = pl.pallas_call(
            place_kernel,
            in_specs=[vmem, anywhere] + [vmem] * 6,
            out_specs=[anywhere] * 6 + [vmem],
            out_shape=[shape(x_in.shape, bf16), shape(x_in.shape, bf16), shape(wqkv.shape, bf16), shape(wo.shape, bf16),
                       shape(w_down.shape, bf16), shape(w_up.shape, bf16), shape((hidden,), bf16)],
            scratch_shapes=[pltpu.VMEM((bufs, 2, mid, hidden), bf16), dma((bufs,)), dma((bufs,)), dma((12,))],
            compiler_params=pltpu.CompilerParams(vmem_limit_bytes=LANDING_LIMIT),
            name="rows_place",
        )(fixed(y_lo), pltpu.with_memory_space_constraint(y_hi, pltpu.HBM), fixed(dx_all), fixed(grads), fixed(d_up), fixed(d_gain),
          fixed(y_own), fixed(dx_own))
        d_wqkv = d_wqkv.reshape(w_qkv.shape[1:] + (hidden,)).transpose(3, 0, 1, 2)
        return y_out, dx_out, d_gain, d_wqkv, d_wout.reshape(w_out.shape), d_wup, d_wdown

    in_specs = (P('data'), P('data'), P(), P(None, 'model'), P('model'), P(None, 'model'), P('model'), P('data'))
    out_specs = (P('data'), P('data'), P('data'), P('data', 'model'), P(('data', 'model')), P('data', 'model'), P(('data', 'model')))
    return jax.shard_map(body, mesh=mesh, in_specs=in_specs, out_specs=out_specs, check_vma=False)
```
